8 devices in a mesh: dp: 1 (over z), tp: 2 (over y), sp: 4 (over x, core).
Axes of the slice: x: 2, y: 2, z: 1, core: 2. Of those that a mesh axis runs over, the one named last changes fastest.
Arguments:
- x_in: bfloat16 [65536, 1536], P(('dp', 'sp'))
- grad_y: bfloat16 [65536, 1536], P(('dp', 'sp'))
- w_qkv: bfloat16 [1536, 3, 1536], P(None, None, 'tp')
- w_out: bfloat16 [1536, 1536], P('tp')
- ln_gamma: float32 [1536], replicated
- ln_beta: float32 [1536], replicated
- temperature: float32 [48], replicated
Outputs:
- output 1: bfloat16 [65536, 1536], P(('dp', 'sp'))
- output 2: bfloat16 [65536, 1536], P(('dp', 'sp'))
- output 3: float32 [1536, 3, 1536], P(('dp', 'sp'), None, 'tp')
- output 4: float32 [1536, 1536], P(('dp', 'tp', 'sp'))
- output 5: float32 [1536], P('dp')
- output 6: float32 [1536], P('dp')
- output 7: float32 [48], P('dp')
All inputs are finite; a program needn't handle non-finite values.
Results may differ from the reference program's by a relative error of at most 0.001.
Values are sent between devices in bfloat16 or wider.
A program may use at most 1 GiB of HBM per device.

```python
import jax
import jax.numpy as jnp
from jax import lax

MODEL_DIM = 1536
NUM_HEADS = 48
NUM_TOKENS = 65536
NUM_REGIONS = 8
HEAD_DIM = MODEL_DIM // NUM_HEADS
LN_EPS = 1e-6


def setup_inputs(seed: int = 0, part: int = 0) -> dict:
    part_key = jax.random.fold_in(jax.random.key(seed), part)
    key_noise, key_offset, key_grad, key_goffset = jax.random.split(part_key, 4)
    key_wqkv, key_wout, key_gamma, key_beta, key_temp = jax.random.split(jax.random.key(seed + 1), 5)
    rows_per_region = NUM_TOKENS // NUM_REGIONS
    w_scale = MODEL_DIM ** -0.5
    offsets = jax.random.normal(key_offset, (NUM_REGIONS, MODEL_DIM), jnp.float32)
    x_vals = jax.random.normal(key_noise, (NUM_TOKENS, MODEL_DIM), jnp.float32) + jnp.repeat(offsets, rows_per_region, axis=0)
    grad_offsets = 0.5 * jax.random.normal(key_goffset, (NUM_REGIONS, MODEL_DIM), jnp.float32)
    grad_vals = jax.random.normal(key_grad, (NUM_TOKENS, MODEL_DIM), jnp.float32) + jnp.repeat(grad_offsets, rows_per_region, axis=0)
    w_qkv = jax.random.normal(key_wqkv, (MODEL_DIM, 3, MODEL_DIM), jnp.float32) * w_scale
    w_out = jax.random.normal(key_wout, (MODEL_DIM, MODEL_DIM), jnp.float32) * w_scale
    ln_gamma = 1.0 + 0.3 * jax.random.normal(key_gamma, (MODEL_DIM,), jnp.float32)
    ln_beta = 0.3 * jax.random.normal(key_beta, (MODEL_DIM,), jnp.float32)
    temperature = jax.random.uniform(key_temp, (NUM_HEADS,), jnp.float32, 2.0, 4.0)
    return {"x_in": x_vals.astype(jnp.bfloat16), "grad_y": grad_vals.astype(jnp.bfloat16), "w_qkv": w_qkv.astype(jnp.bfloat16), "w_out": w_out.astype(jnp.bfloat16), "ln_gamma": ln_gamma, "ln_beta": ln_beta, "temperature": temperature}


def head_pass(operands):
    q_head, k_head, v_head, dout_head, temp_one = operands
    gram_mat = jnp.dot(q_head.T, k_head, preferred_element_type=jnp.float32)
    q_sq = jnp.sum(jnp.square(q_head.astype(jnp.float32)), axis=0)
    k_sq = jnp.sum(jnp.square(k_head.astype(jnp.float32)), axis=0)
    norm_prod = jnp.sqrt(q_sq)[:, None] * jnp.sqrt(k_sq)[None, :]
    gram_n = gram_mat / norm_prod
    attn_prob = jax.nn.softmax(temp_one * gram_n, axis=-1)
    attn_bf = attn_prob.astype(jnp.bfloat16)
    out_head = jnp.dot(v_head, attn_bf.T, preferred_element_type=jnp.float32).astype(jnp.bfloat16)
    d_attn = jnp.dot(dout_head.T, v_head, preferred_element_type=jnp.float32)
    dv_head = jnp.dot(dout_head, attn_bf, preferred_element_type=jnp.float32).astype(jnp.bfloat16)
    d_logit = attn_prob * (d_attn - jnp.sum(attn_prob * d_attn, axis=-1, keepdims=True))
    temp_grad = jnp.sum(d_logit * gram_n)
    grad_sn = temp_one * d_logit
    d_gram = (grad_sn / norm_prod).astype(jnp.bfloat16)
    prod_sn = grad_sn * gram_n
    q_coef = -jnp.sum(prod_sn, axis=1) / q_sq
    k_coef = -jnp.sum(prod_sn, axis=0) / k_sq
    dq_head = (jnp.dot(k_head, d_gram.T, preferred_element_type=jnp.float32) + q_head.astype(jnp.float32) * q_coef[None, :]).astype(jnp.bfloat16)
    dk_head = (jnp.dot(q_head, d_gram, preferred_element_type=jnp.float32) + k_head.astype(jnp.float32) * k_coef[None, :]).astype(jnp.bfloat16)
    return out_head, dq_head, dk_head, dv_head, temp_grad


def reference(x_in, grad_y, w_qkv, w_out, ln_gamma, ln_beta, temperature):
    x_float = x_in.astype(jnp.float32)
    centered = x_float - jnp.mean(x_float, axis=1, keepdims=True)
    inv_std = lax.rsqrt(jnp.mean(centered * centered, axis=1, keepdims=True) + LN_EPS)
    x_hat = centered * inv_std
    u_act = (x_hat * ln_gamma + ln_beta).astype(jnp.bfloat16)
    w_flat = w_qkv.reshape(MODEL_DIM, 3 * MODEL_DIM)
    qkv_act = jnp.dot(u_act, w_flat, preferred_element_type=jnp.float32).astype(jnp.bfloat16)
    qkv_heads = qkv_act.reshape(NUM_TOKENS, 3, NUM_HEADS, HEAD_DIM).transpose(1, 2, 0, 3)
    dout_act = jnp.dot(grad_y, w_out.T, preferred_element_type=jnp.float32).astype(jnp.bfloat16)
    dout_heads = dout_act.reshape(NUM_TOKENS, NUM_HEADS, HEAD_DIM).transpose(1, 0, 2)
    out_heads, dq_heads, dk_heads, dv_heads, grad_temp = lax.map(head_pass, (qkv_heads[0], qkv_heads[1], qkv_heads[2], dout_heads, temperature))
    out_act = out_heads.transpose(1, 0, 2).reshape(NUM_TOKENS, MODEL_DIM)
    y_out = (x_float + jnp.dot(out_act, w_out, preferred_element_type=jnp.float32)).astype(jnp.bfloat16)
    grad_wout = jnp.dot(out_act.T, grad_y, preferred_element_type=jnp.float32)
    dqkv_act = jnp.stack([dq_heads, dk_heads, dv_heads], axis=0).transpose(2, 0, 1, 3).reshape(NUM_TOKENS, 3 * MODEL_DIM)
    grad_wqkv = jnp.dot(u_act.T, dqkv_act, preferred_element_type=jnp.float32).reshape(MODEL_DIM, 3, MODEL_DIM)
    grad_u = jnp.dot(dqkv_act, w_flat.T, preferred_element_type=jnp.float32)
    grad_gamma = jnp.sum(grad_u * x_hat, axis=0)
    grad_beta = jnp.sum(grad_u, axis=0)
    grad_xhat = grad_u * ln_gamma
    grad_ln = inv_std * (grad_xhat - jnp.mean(grad_xhat, axis=1, keepdims=True) - x_hat * jnp.mean(grad_xhat * x_hat, axis=1, keepdims=True))
    grad_x = (grad_y.astype(jnp.float32) + grad_ln).astype(jnp.bfloat16)
    return y_out, grad_x, grad_wqkv, grad_wout, grad_gamma, grad_beta, grad_temp
```

```python
import jax
import jax.numpy as jnp
from jax import lax
from jax.sharding import PartitionSpec as P

LN_EPS = 1e-6
GROUP = 256
F32 = jnp.float32
BF16 = jnp.bfloat16


def layer_norm_fwd(x_rows, ln_gamma, ln_beta):
    x_float = x_rows.astype(F32)
    centered = x_float - jnp.mean(x_float, axis=-1, keepdims=True)
    inv_std = lax.rsqrt(jnp.mean(centered * centered, axis=-1, keepdims=True) + LN_EPS)
    x_hat = centered * inv_std
    return x_hat, inv_std, (x_hat * ln_gamma + ln_beta).astype(BF16)


def layer_norm_bwd(grad_u, x_hat, inv_std, ln_gamma):
    gh = grad_u * ln_gamma
    return inv_std * (gh - jnp.mean(gh, axis=-1, keepdims=True) - x_hat * jnp.mean(gh * x_hat, axis=-1, keepdims=True))


def state_forward(gram_mat, q_sq, k_sq, temp_heads):
    norm_prod = jnp.sqrt(q_sq)[:, :, None] * jnp.sqrt(k_sq)[:, None, :]
    gram_n = gram_mat / norm_prod
    attn_prob = jax.nn.softmax(temp_heads[:, None, None] * gram_n, axis=-1)
    return gram_n, norm_prod, attn_prob


def state_backward(d_attn, attn_prob, gram_n, norm_prod, q_sq, k_sq, temp_heads):
    d_logit = attn_prob * (d_attn - jnp.sum(attn_prob * d_attn, axis=-1, keepdims=True))
    temp_grad = jnp.sum(d_logit * gram_n, axis=(1, 2))
    grad_sn = temp_heads[:, None, None] * d_logit
    d_gram = (grad_sn / norm_prod).astype(BF16)
    prod_sn = grad_sn * gram_n
    q_coef = -jnp.sum(prod_sn, axis=2) / q_sq
    k_coef = -jnp.sum(prod_sn, axis=1) / k_sq
    return d_gram, q_coef, k_coef, temp_grad


def block_diag(mat):
    heads, dim, _ = mat.shape
    per = GROUP // dim
    m = mat.reshape(heads // per, per, dim, dim)
    eye = jnp.eye(per, dtype=mat.dtype)
    out = m[:, :, :, None, :] * eye[None, :, None, :, None]
    return out.reshape(heads // per, GROUP, GROUP)


def diag_blocks(mat, dim):
    groups = mat.shape[0]
    per = GROUP // dim
    m = mat.reshape(groups, per, dim, per, dim)
    return jnp.stack([m[:, i, :, i, :] for i in range(per)], axis=1).reshape(groups * per, dim, dim)


def mix(act, bd):
    n, cols = act.shape
    out = [jnp.dot(act[:, g * GROUP:(g + 1) * GROUP], bd[g], preferred_element_type=F32) for g in range(cols // GROUP)]
    return jnp.concatenate(out, axis=1)


def gram(lhs, rhs):
    cols = lhs.shape[1]
    sl = lambda t, g: t[:, g * GROUP:(g + 1) * GROUP]
    return jnp.stack([lax.dot_general(sl(lhs, g), sl(rhs, g), (((0,), (0,)), ((), ())), preferred_element_type=F32) for g in range(cols // GROUP)])


def solution(mesh):
    tp_size = mesh.shape["tp"]
    row_spec = P(("dp", "sp"), None)
    swap = [(0, 1), (1, 0)]

    def local_step(x_blk, grad_blk, w_qkv, w_out, ln_gamma, ln_beta, temps):
        tokens, model_width = x_blk.shape
        local_cols = w_qkv.shape[2]
        heads_loc = temps.shape[0] // tp_size
        head_dim = local_cols // heads_loc
        temp_heads = lax.dynamic_slice_in_dim(temps, lax.axis_index("tp") * heads_loc, heads_loc)
        w_far = lax.ppermute(w_qkv, "tp", swap)
        wo_far = lax.ppermute(w_out, "tp", swap)
        x_hat, inv_std, u_act = layer_norm_fwd(x_blk, ln_gamma, ln_beta)

        def project(w3, wo):
            q, k, v = [jnp.dot(u_act, w3[:, e], preferred_element_type=F32).astype(BF16) for e in range(3)]
            do = lax.dot_general(grad_blk, wo, (((1,), (1,)), ((), ())), preferred_element_type=F32).astype(BF16)
            return q, k, v, do

        near = project(w_qkv, w_out)
        q, k, v, do = near
        sq = lambda t: jnp.sum(jnp.square(t.astype(F32)), axis=0).reshape(heads_loc, head_dim)
        gram_mat, d_attn, q_sq, k_sq = lax.psum(
            (diag_blocks(gram(q, k), head_dim), diag_blocks(gram(do, v), head_dim), sq(q), sq(k)), "sp")
        gram_n, norm_prod, attn_prob = state_forward(gram_mat, q_sq, k_sq, temp_heads)
        d_gram, q_coef, k_coef, temp_grad = state_backward(d_attn, attn_prob, gram_n, norm_prod, q_sq, k_sq, temp_heads)
        state = (attn_prob.astype(BF16), d_gram, q_coef, k_coef)
        far_state = lax.ppermute(state, "tp", swap)
        far = project(w_far, wo_far)

        def backward(acts, st):
            q, k, v, do = acts
            attn_bf, d_gram, q_coef, k_coef = st
            tr = lambda m: jnp.swapaxes(m, 1, 2)
            o = mix(v, block_diag(tr(attn_bf))).astype(BF16)
            dv = mix(do, block_diag(attn_bf)).astype(BF16)
            dq = (mix(k, block_diag(tr(d_gram))) + q.astype(F32) * q_coef.reshape(1, -1)).astype(BF16)
            dk = (mix(q, block_diag(d_gram)) + k.astype(F32) * k_coef.reshape(1, -1)).astype(BF16)
            return o, jnp.concatenate([dq, dk, dv], axis=1)

        o_n, r_n = backward(near, state)
        wout_part = lax.dot_general(o_n, grad_blk, (((0,), (0,)), ((), ())), preferred_element_type=F32)
        grad_wout = lax.psum_scatter(wout_part, "sp", scatter_dimension=0, tiled=True)
        wqkv_part = lax.dot_general(u_act, r_n, (((0,), (0,)), ((), ())), preferred_element_type=F32).reshape(model_width, 3, local_cols)
        grad_wqkv = lax.psum_scatter(wqkv_part, "sp", scatter_dimension=0, tiled=True)
        o_f, r_f = backward(far, far_state)
        y_out = (x_blk.astype(F32) + jnp.dot(jnp.concatenate([o_n, o_f], axis=1), jnp.concatenate([w_out, wo_far], axis=0), preferred_element_type=F32)).astype(BF16)
        w_all = jnp.concatenate([w_qkv.reshape(model_width, -1), w_far.reshape(model_width, -1)], axis=1)
        grad_u = lax.dot_general(jnp.concatenate([r_n, r_f], axis=1), w_all, (((1,), (1,)), ((), ())), preferred_element_type=F32)
        grad_gamma, grad_beta = lax.psum((jnp.sum(grad_u * x_hat, axis=0), jnp.sum(grad_u, axis=0)), "sp")
        grad_x = (grad_blk.astype(F32) + layer_norm_bwd(grad_u, x_hat, inv_std, ln_gamma)).astype(BF16)
        grad_temp = lax.all_gather(temp_grad, "tp", tiled=True)
        return y_out, grad_x, grad_wqkv, grad_wout, grad_gamma, grad_beta, grad_temp

    in_specs = (row_spec, row_spec, P(None, None, "tp"), P("tp", None), P(None), P(None), P(None))
    out_specs = (row_spec, row_spec, P(("dp", "sp"), None, "tp"), P(("dp", "tp", "sp"), None), P("dp"), P("dp"), P("dp"))
    return jax.shard_map(local_step, mesh=mesh, in_specs=in_specs, out_specs=out_specs, check_vma=False)
```

```python
import functools

import jax
import jax.numpy as jnp
from jax import lax
from jax.experimental import pallas as pl
from jax.experimental.pallas import tpu as pltpu
from jax.sharding import PartitionSpec as P


LN_EPS = 1e-6
GROUP = 256
HEAD = 32
F32 = jnp.float32
BF16 = jnp.bfloat16
NN = (((1,), (0,)), ((), ()))
NT = (((1,), (1,)), ((), ()))
TN = (((0,), (0,)), ((), ()))
PROJ_ROWS = 512
ROWS = 256
OWN_CHUNKS = (4, 6, 8, 6)


def dot(a, b, dims=NN):
    return lax.dot_general(a, b, dims, preferred_element_type=F32)


def normalize(x):
    cen = x - jnp.mean(x, axis=-1, keepdims=True)
    inv = lax.rsqrt(jnp.mean(cen * cen, axis=-1, keepdims=True) + LN_EPS)
    return cen * inv, inv


def row_spec(rows, cols, index):
    return pl.BlockSpec((rows, cols), lambda *a: (index(*a), 0))


def whole(shape):
    return pl.BlockSpec(shape, lambda *a: (0,) * len(shape), pipeline_mode=pl.Buffered(1))


def sds(shape, dtype):
    return jax.ShapeDtypeStruct(shape, dtype)


def params(**kw):
    return pltpu.CompilerParams(vmem_limit_bytes=64_000_000, **kw)


def cost(flops, nbytes):
    return pl.CostEstimate(flops=int(flops), bytes_accessed=int(nbytes), transcendentals=0)


def project_body(x_ref, g_ref, w_ref, wo_ref, gm_ref, bt_ref, u_ref, q_ref, k_ref, v_ref, do_ref, part_ref, gr, da, qs, ks):
    i = pl.program_id(0)
    rows, cols = q_ref.shape
    groups = cols // GROUP
    do_ref[...] = dot(g_ref[...], wo_ref[...], NT).astype(BF16)
    xh, _ = normalize(x_ref[...].astype(F32))
    u_ref[...] = (xh * gm_ref[...] + bt_ref[...]).astype(BF16)
    u = u_ref[...]
    for e, out in enumerate((q_ref, k_ref, v_ref)):
        out[...] = dot(u, w_ref[e]).astype(BF16)

    def add(acc, s, val):
        acc[s] = jnp.where(i == 0, val, acc[s] + val)

    for s in range(groups):
        c = slice(s * GROUP, (s + 1) * GROUP)
        add(gr, s, dot(q_ref[:, c], k_ref[:, c], TN))
        add(da, s, dot(do_ref[:, c], v_ref[:, c], TN))
    for acc, t in ((qs, q_ref), (ks, k_ref)):
        f = t[...].astype(F32)
        val = jnp.sum((f * f).reshape(rows // 8, 8, cols), axis=0)
        acc[...] = jnp.where(i == 0, val, acc[...] + val)

    @pl.when(i == pl.num_programs(0) - 1)
    def _():
        col_head = lax.broadcasted_iota(jnp.int32, (HEAD, GROUP), 1) // HEAD
        for a, acc in enumerate((gr, da)):
            for s in range(groups):
                tot = jnp.zeros((HEAD, GROUP), F32)
                for h in range(GROUP // HEAD):
                    tot += jnp.where(col_head == h, acc[s, h * HEAD:(h + 1) * HEAD, :], 0.0)
                part_ref[(a * groups + s) * HEAD:(a * groups + s + 1) * HEAD, :] = tot
        base = 2 * groups * HEAD
        for a, acc in enumerate((qs, ks)):
            tot = jnp.sum(acc[...], axis=0, keepdims=True)
            for s in range(groups):
                part_ref[base + 8 * (a * groups + s):base + 8 * (a * groups + s + 1), :] = jnp.broadcast_to(
                    tot[:, s * GROUP:(s + 1) * GROUP], (8, GROUP))


def project(x, g, w3, wo, gamma, beta):
    tokens, width = x.shape
    cols = wo.shape[0]
    groups = cols // GROUP
    part_rows = 2 * groups * (HEAD + 8)
    row = lambda c: row_spec(PROJ_ROWS, c, lambda i: i)
    return pl.pallas_call(
        project_body,
        grid=(tokens // PROJ_ROWS,),
        in_specs=[row(width), row(width), whole(w3.shape), whole(wo.shape), whole((1, width)), whole((1, width))],
        out_specs=[row(width)] + [row(cols)] * 4 + [pl.BlockSpec((part_rows, GROUP), lambda i: (0, 0))],
        out_shape=[sds((tokens, width), BF16)] + [sds((tokens, cols), BF16)] * 4 + [sds((part_rows, GROUP), F32)],
        scratch_shapes=[pltpu.VMEM((groups, GROUP, GROUP), F32)] * 2 + [pltpu.VMEM((8, cols), F32)] * 2,
        name="project",
        compiler_params=params(),
        cost_estimate=cost(2 * tokens * width * cols * 4.4, 2 * tokens * (3 * width + 4 * cols)),
    )(x, g, w3, wo, gamma, beta)


def far_v_body(off_ref, u_ref, w_ref, v_ref):
    v_ref[...] = dot(u_ref[...], w_ref[...]).astype(BF16)


def far_v(off, u, w, blocks):
    width, cols = w.shape
    rows = 2 * ROWS
    return pl.pallas_call(
        far_v_body,
        grid_spec=pltpu.PrefetchScalarGridSpec(
            num_scalar_prefetch=1,
            grid=(blocks // 2,),
            in_specs=[row_spec(rows, width, lambda j, off: off[1] // 2 + j), whole(w.shape)],
            out_specs=row_spec(rows, cols, lambda j, off: j),
        ),
        out_shape=sds((blocks * ROWS, cols), BF16),
        name="far_v",
        compiler_params=params(),
        cost_estimate=cost(2 * blocks * ROWS * width * cols, 2 * blocks * ROWS * (width + cols)),
    )(off, u, w)


def state_body(near_ref, far_ref, tau_ref, attn_ref, dgram_ref, coef_ref, dtau_ref, *, groups):
    r_head = lax.broadcasted_iota(jnp.int32, (GROUP, GROUP), 0)
    c_head = lax.broadcasted_iota(jnp.int32, (GROUP, GROUP), 1)
    eye = r_head == c_head
    mask = (r_head // HEAD) == (c_head // HEAD)
    spread = lambda t: jnp.concatenate([t] * (GROUP // HEAD), axis=0)
    to_col = lambda t: jnp.sum(jnp.where(eye, t, 0.0), axis=1, keepdims=True)
    to_row = lambda t: jnp.sum(jnp.where(eye, t, 0.0), axis=0, keepdims=True)
    base = 2 * groups * HEAD
    coef_ref[...] = jnp.zeros_like(coef_ref)
    dtau_ref[...] = jnp.zeros_like(dtau_ref)
    for side, ref in enumerate((near_ref, far_ref)):
        for s in range(groups):
            gram_mat = spread(ref[s * HEAD:(s + 1) * HEAD, :])
            d_attn = spread(ref[(groups + s) * HEAD:(groups + s + 1) * HEAD, :])
            b_row = ref[base + 8 * (groups + s):base + 8 * (groups + s) + 1, :]
            a_col = to_col(ref[base + 8 * s:base + 8 * s + 1, :])
            g = side * groups + s
            tau = to_col(tau_ref[g:g + 1, :])
            norm_prod = jnp.sqrt(a_col) * jnp.sqrt(b_row)
            gram_n = gram_mat / norm_prod
            logit = jnp.where(mask, tau * gram_n, -jnp.inf)
            e = jnp.exp(logit - jnp.max(logit, axis=1, keepdims=True))
            attn = e / jnp.sum(e, axis=1, keepdims=True)
            d_attn = jnp.where(mask, d_attn, 0.0)
            d_logit = jnp.where(mask, attn * (d_attn - jnp.sum(attn * d_attn, axis=1, keepdims=True)), 0.0)
            gram_n = jnp.where(mask, gram_n, 0.0)
            grad_sn = tau * d_logit
            prod = grad_sn * gram_n
            attn_ref[g] = attn.astype(BF16)
            dgram_ref[g] = jnp.where(mask, grad_sn / norm_prod, 0.0).astype(BF16)
            coef_ref[2 * side:2 * side + 1, s * GROUP:(s + 1) * GROUP] = to_row(-jnp.sum(prod, axis=1, keepdims=True) / a_col)
            coef_ref[2 * side + 1:2 * side + 2, s * GROUP:(s + 1) * GROUP] = -jnp.sum(prod, axis=0, keepdims=True) / b_row
            if side == 0:
                dtau_ref[s:s + 1, :] = to_row(jnp.sum(d_logit * gram_n, axis=1, keepdims=True))


def head_state(near, far, tau_rows):
    groups = tau_rows.shape[0] // 2
    vm = pl.BlockSpec(memory_space=pltpu.VMEM)
    return pl.pallas_call(
        functools.partial(state_body, groups=groups),
        in_specs=[vm] * 3,
        out_specs=[vm] * 4,
        out_shape=[sds((2 * groups, GROUP, GROUP), BF16)] * 2 + [sds((8, groups * GROUP), F32), sds((8, GROUP), F32)],
        name="head_state",
        cost_estimate=cost(10**9, 2 * 10**6),
    )(near, far, tau_rows)


def mix_block(q, k, v, do, attn_ref, dgram_ref, coef_ref, side, s):
    groups = attn_ref.shape[0] // 2
    am, gm = attn_ref[side * groups + s], dgram_ref[side * groups + s]
    c = slice(s * GROUP, (s + 1) * GROUP)
    dq = dot(k, gm, NT) + q.astype(F32) * coef_ref[2 * side:2 * side + 1, c]
    dk = dot(q, gm, NN) + k.astype(F32) * coef_ref[2 * side + 1:2 * side + 2, c]
    return dot(v, am, NT).astype(BF16), dq.astype(BF16), dk.astype(BF16), dot(do, am, NN).astype(BF16)


def finish_rows(j, x_ref, g_ref, du, gm_ref, dx_refs, dsum_ref):
    rows, width = x_ref.shape
    xh, inv = normalize(x_ref[...].astype(F32))
    fold = lambda t: jnp.sum(t.reshape(rows // 8, 8, width), axis=0)
    for a, val in enumerate((fold(du * xh), fold(du))):
        dsum_ref[a] = jnp.where(j == 0, val, dsum_ref[a] + val)
    gh = du * gm_ref[...]
    m1 = jnp.mean(gh, axis=-1, keepdims=True)
    m2 = jnp.mean(gh * xh, axis=-1, keepdims=True)
    dx = (g_ref[...].astype(F32) + inv * (gh - m1 - xh * m2)).astype(BF16)
    for ref in dx_refs:
        ref[...] = dx


def rows_body(*refs, near_ready, n_alias, send):
    it = iter(refs)
    nxt = lambda n: [next(it) for _ in range(n)]
    _, x_ref, g_ref, u_ref = nxt(4)
    if near_ready:
        o_in, r_in = nxt(2)
    else:
        q_ref, k_ref, v_ref, do_ref = nxt(4)
    attn_ref, dgram_ref, coef_ref, wn_ref, wf_ref, won_ref, wof_ref, gm_ref = nxt(8)
    nxt(n_alias)
    y_ref, gx_ref = nxt(2)
    if not near_ready:
        o_ref, r_ref = nxt(2)
    send_ref = nxt(1) if send else []
    (dsum_ref,) = nxt(1)
    of_s, rf_s, qf_s, kf_s, vf_s, dof_s = nxt(6)
    j = pl.program_id(0)
    groups = attn_ref.shape[0] // 2
    u = u_ref[...]
    for e, t in enumerate((qf_s, kf_s, vf_s)):
        t[...] = dot(u, wf_ref[e]).astype(BF16)
    dof_s[...] = dot(g_ref[...], wof_ref[...], NT).astype(BF16)
    if near_ready:
        o_ref, r_ref = o_in, r_in
    else:
        for s in range(groups):
            c = slice(s * GROUP, (s + 1) * GROUP)
            o_ref[:, c], r_ref[0, :, c], r_ref[1, :, c], r_ref[2, :, c] = mix_block(
                q_ref[:, c], k_ref[:, c], v_ref[:, c], do_ref[:, c], attn_ref, dgram_ref, coef_ref, 0, s)
    for s in range(groups):
        c = slice(s * GROUP, (s + 1) * GROUP)
        of_s[:, c], rf_s[0, :, c], rf_s[1, :, c], rf_s[2, :, c] = mix_block(
            qf_s[:, c], kf_s[:, c], vf_s[:, c], dof_s[:, c], attn_ref, dgram_ref, coef_ref, 1, s)
    du = dot(r_ref[0], wn_ref[0], NT)
    for e in range(1, 3):
        du += dot(r_ref[e], wn_ref[e], NT)
    for e in range(3):
        du += dot(rf_s[e], wf_ref[e], NT)
    y_ref[...] = (x_ref[...].astype(F32) + (dot(o_ref[...], won_ref[...]) + dot(of_s[...], wof_ref[...]))).astype(BF16)
    finish_rows(j, x_ref, g_ref, du, gm_ref, [gx_ref] + send_ref, dsum_ref)


def rows_call(off, sel, start, blocks, acts, state, weights, prev, *, near_ready, send):
    x = acts[0]
    tokens, width = x.shape
    cols = weights[2].shape[0]
    at = lambda j, off: off[sel] + start + j
    row = lambda c: row_spec(ROWS, c, at)
    row3 = pl.BlockSpec((3, ROWS, cols), lambda j, off: (0, at(j, off), 0))
    any_ = pl.BlockSpec(memory_space=pl.ANY)
    act_specs = [row(width)] * 3 + ([row(cols), row3] if near_ready else [row(cols)] * 4)
    consts = list(state) + list(weights)
    out_specs = [row(width)] * 2
    out_shape = [sds((tokens, width), BF16)] * 2
    if not near_ready:
        out_specs += [row(cols), row3]
        out_shape += [sds((tokens, cols), BF16), sds((3, tokens, cols), BF16)]
    n_alias = 0 if prev is None else len(prev)
    first = 1 + len(acts) + len(consts)
    aliases = {first + a: a for a in range(n_alias)}
    if send:
        out_specs.append(row_spec(ROWS, width, lambda j, off: j))
        out_shape.append(sds((blocks * ROWS, width), BF16))
    out_specs.append(pl.BlockSpec((2, 8, width), lambda j, off: (0, 0, 0)))
    out_shape.append(sds((2, 8, width), F32))
    return pl.pallas_call(
        functools.partial(rows_body, near_ready=near_ready, n_alias=n_alias, send=send),
        grid_spec=pltpu.PrefetchScalarGridSpec(
            num_scalar_prefetch=1,
            grid=(blocks,),
            in_specs=act_specs + [whole(t.shape) for t in consts] + [any_] * n_alias,
            out_specs=out_specs,
            scratch_shapes=[pltpu.VMEM((ROWS, cols), BF16), pltpu.VMEM((3, ROWS, cols), BF16)] + [pltpu.VMEM((ROWS, cols), BF16)] * 4,
        ),
        out_shape=out_shape,
        input_output_aliases=aliases,
        name="rows",
        compiler_params=params(),
        cost_estimate=cost(2 * blocks * ROWS * width * cols * 13, 2 * blocks * ROWS * (5 * width + 8 * cols)),
    )(off, *acts, *consts, *(prev or ()))


def local_body(*refs, with_y):
    it = iter(refs)
    nxt = lambda n: [next(it) for _ in range(n)]
    _, q_ref, k_ref, v_ref, do_ref = nxt(5)
    if with_y:
        x_ref, vf_ref = nxt(2)
    attn_ref, dgram_ref, coef_ref = nxt(3)
    if with_y:
        won_ref, wof_ref = nxt(2)
        nxt(3)
        y_ref, o_ref, r_ref, of_s = nxt(4)
    else:
        nxt(2)
        o_ref, r_ref = nxt(2)
    groups = attn_ref.shape[0] // 2
    for s in range(groups):
        c = slice(s * GROUP, (s + 1) * GROUP)
        if with_y:
            of_s[:, c] = dot(vf_ref[:, c], attn_ref[groups + s], NT).astype(BF16)
        o_ref[:, c], r_ref[0, :, c], r_ref[1, :, c], r_ref[2, :, c] = mix_block(
            q_ref[:, c], k_ref[:, c], v_ref[:, c], do_ref[:, c], attn_ref, dgram_ref, coef_ref, 0, s)
    if with_y:
        y_ref[...] = (x_ref[...].astype(F32) + (dot(o_ref[...], won_ref[...]) + dot(of_s[...], wof_ref[...]))).astype(BF16)


def local_call(off, sel, blocks, near, state, prev, x=None, vf=None, weights=()):
    with_y = x is not None
    cols = near[0].shape[1]
    at = lambda j, off: off[sel] + j
    row = lambda c: row_spec(ROWS, c, at)
    row3 = pl.BlockSpec((3, ROWS, cols), lambda j, off: (0, at(j, off), 0))
    any_ = pl.BlockSpec(memory_space=pl.ANY)
    acts, act_specs = list(near), [row(cols)] * 4
    if with_y:
        acts += [x, vf]
        act_specs += [row(x.shape[1]), row_spec(ROWS, cols, lambda j, off: j)]
    consts = list(state) + list(weights)
    out_specs = ([row(x.shape[1])] if with_y else []) + [row(cols), row3]
    first = 1 + len(acts) + len(consts)
    return pl.pallas_call(
        functools.partial(local_body, with_y=with_y),
        grid_spec=pltpu.PrefetchScalarGridSpec(
            num_scalar_prefetch=1,
            grid=(blocks,),
            in_specs=act_specs + [whole(t.shape) for t in consts] + [any_] * len(prev),
            out_specs=out_specs,
            scratch_shapes=[pltpu.VMEM((ROWS, cols), BF16)] if with_y else [],
        ),
        out_shape=[sds(t.shape, t.dtype) for t in prev],
        input_output_aliases={first + a: a for a in range(len(prev))},
        name="local_y" if with_y else "local",
        compiler_params=params(),
        cost_estimate=cost(2 * blocks * ROWS * cols * (1536 * 2.8 if with_y else 1024), 2 * blocks * ROWS * cols * (13 if with_y else 8)),
    )(off, *acts, *consts, *prev)


def solution(mesh):
    tp_size = mesh.shape["tp"]
    sp_size = mesh.shape["sp"]
    in_rows = P(("dp", "sp"), None)
    swap = [(0, 1), (1, 0)]

    def exchange(t):
        return lax.ppermute(t, "tp", swap)

    def step(x, g, w_qkv, w_out, ln_gamma, ln_beta, temps):
        tokens, width = x.shape
        cols = w_qkv.shape[2]
        groups = cols // GROUP
        me = lax.axis_index("tp")
        w_near = jnp.transpose(w_qkv, (1, 0, 2))
        w_far = exchange(w_near)
        wo_far = exchange(w_out)
        gamma, beta = ln_gamma.reshape(1, width), ln_beta.reshape(1, width)
        own = sum(OWN_CHUNKS)
        rest = tokens // ROWS - 2 * own
        off = jnp.stack([me * own, (1 - me) * own, jnp.full_like(me, 2 * own)]).astype(jnp.int32)

        u, q, k, v, do, part = project(x, g, w_near, w_out, gamma, beta)
        near = (q, k, v, do)
        peers = [lax.ppermute(part, "sp", [(s, s ^ d) for s in range(sp_size)]) for d in (1, 2, 3)]
        part = (part + peers[0]) + (peers[1] + peers[2])
        part_far = exchange(part)
        vf = far_v(off, u, w_far[2], own)
        tau = jnp.repeat(temps, HEAD).reshape(tp_size, groups, GROUP)
        tau = jnp.where(me == 0, tau, tau[::-1]).reshape(2 * groups, GROUP)
        attn, dgram, coef, dtau = head_state(part, part_far, tau)
        state = (attn, dgram, coef)
        weights = (w_near, w_far, w_out, wo_far, gamma)

        prev, dsum, recv, start = None, None, [], 0
        for blocks in OWN_CHUNKS:
            *prev, sent, ds = rows_call(off, 0, start, blocks, (x, g, u) + near, state, weights, prev, near_ready=False, send=True)
            recv.append((start, exchange(sent)))
            dsum = ds if dsum is None else dsum + ds
            start += blocks
        y, gx, o, r = prev
        y, o, r = local_call(off, 1, own, near, state, (y, o, r), x, vf, (w_out, wo_far))
        o, r = local_call(off, 2, rest, near, state, (o, r))
        wqkv_part = lax.dot_general(u, r, (((0,), (1,)), ((), ())), preferred_element_type=F32)
        o, wqkv_part = lax.optimization_barrier((o, wqkv_part))
        grad_wqkv = lax.psum_scatter(wqkv_part, "sp", scatter_dimension=0, tiled=True)
        wout_part = dot(o, g, TN)
        gx, wout_part = lax.optimization_barrier((gx, wout_part))
        grad_wout = lax.psum_scatter(wout_part, "sp", scatter_dimension=0, tiled=True)
        y, gx, ds = rows_call(off, 2, 0, rest, (x, g, u, o, r), state, weights, (y, gx), near_ready=True, send=False)
        sums = lax.psum(jnp.sum(dsum + 0.5 * ds, axis=1), ("tp", "sp"))
        for start, blk in recv:
            gx = lax.dynamic_update_slice(gx, blk, ((off[1] + start) * ROWS, 0))
        dtau = jnp.sum(dtau[:groups].reshape(groups * GROUP // HEAD, HEAD), axis=1)
        dtau_far = lax.ppermute(dtau, "tp", swap)
        grad_temp = jnp.where(me == 0, jnp.concatenate([dtau, dtau_far]), jnp.concatenate([dtau_far, dtau]))
        return y, gx, grad_wqkv, grad_wout, sums[0], sums[1], grad_temp

    in_specs = (in_rows, in_rows, P(None, None, "tp"), P("tp", None), P(None), P(None), P(None))
    out_specs = (in_rows, in_rows, P(("dp", "sp"), None, "tp"), P(("dp", "tp", "sp"), None), P("dp"), P("dp"), P("dp"))
    return jax.shard_map(step, mesh=mesh, in_specs=in_specs, out_specs=out_specs, check_vma=False)
```

```python
import functools

import jax
import jax.numpy as jnp
from jax import lax
from jax.experimental import pallas as pl
from jax.experimental.pallas import tpu as pltpu
from jax.sharding import PartitionSpec as P


LN_EPS = 1e-6
GROUP = 256
HEAD = 32
F32 = jnp.float32
BF16 = jnp.bfloat16
NN = (((1,), (0,)), ((), ()))
NT = (((1,), (1,)), ((), ()))
TN = (((0,), (0,)), ((), ()))
PROJ_ROWS = 512
ROWS = 256
OWN_CHUNKS = (4, 6, 9, 13)
EARLY_V = 12


def dot(a, b, dims=NN):
    return lax.dot_general(a, b, dims, preferred_element_type=F32)


def normalize(x):
    cen = x - jnp.mean(x, axis=-1, keepdims=True)
    inv = lax.rsqrt(jnp.mean(cen * cen, axis=-1, keepdims=True) + LN_EPS)
    return cen * inv, inv


def row_spec(rows, cols, index):
    return pl.BlockSpec((rows, cols), lambda *a: (index(*a), 0))


def half_spec(rows, cols, which, start):
    return pl.BlockSpec((1, rows, cols), lambda j, off: (off[which], start + j, 0))


def both_spec(lead, rows, cols, start):
    zeros = (0,) * len(lead)
    return pl.BlockSpec((*lead, 2, rows, cols), lambda j, off: (*zeros, 0, start + j, 0))


def whole(shape):
    return pl.BlockSpec(shape, lambda *a: (0,) * len(shape), pipeline_mode=pl.Buffered(1))


def sds(shape, dtype):
    return jax.ShapeDtypeStruct(shape, dtype)


def params(**kw):
    return pltpu.CompilerParams(vmem_limit_bytes=64_000_000, **kw)


def cost(flops, nbytes):
    return pl.CostEstimate(flops=int(flops), bytes_accessed=int(nbytes), transcendentals=0)


def project_body(x_ref, g_ref, w_ref, wo_ref, gm_ref, bt_ref, u_ref, q_ref, k_ref, v_ref, do_ref, part_ref, gr, da, qs, ks):
    i = pl.program_id(0)
    rows, cols = q_ref.shape
    groups = cols // GROUP
    do_ref[...] = dot(g_ref[...], wo_ref[...], NT).astype(BF16)
    xh, _ = normalize(x_ref[...].astype(F32))
    u_ref[...] = (xh * gm_ref[...] + bt_ref[...]).astype(BF16)
    u = u_ref[...]
    for e, out in enumerate((q_ref, k_ref, v_ref)):
        out[...] = dot(u, w_ref[e]).astype(BF16)

    def add(acc, s, val):
        acc[s] = jnp.where(i == 0, val, acc[s] + val)

    for s in range(groups):
        c = slice(s * GROUP, (s + 1) * GROUP)
        add(gr, s, dot(q_ref[:, c], k_ref[:, c], TN))
        add(da, s, dot(do_ref[:, c], v_ref[:, c], TN))
    for acc, t in ((qs, q_ref), (ks, k_ref)):
        f = t[...].astype(F32)
        val = jnp.sum((f * f).reshape(rows // 8, 8, cols), axis=0)
        acc[...] = jnp.where(i == 0, val, acc[...] + val)

    @pl.when(i == pl.num_programs(0) - 1)
    def _():
        col_head = lax.broadcasted_iota(jnp.int32, (HEAD, GROUP), 1) // HEAD
        for a, acc in enumerate((gr, da)):
            for s in range(groups):
                tot = jnp.zeros((HEAD, GROUP), F32)
                for h in range(GROUP // HEAD):
                    tot += jnp.where(col_head == h, acc[s, h * HEAD:(h + 1) * HEAD, :], 0.0)
                part_ref[(a * groups + s) * HEAD:(a * groups + s + 1) * HEAD, :] = tot
        base = 2 * groups * HEAD
        for a, acc in enumerate((qs, ks)):
            tot = jnp.sum(acc[...], axis=0, keepdims=True)
            for s in range(groups):
                part_ref[base + 8 * (a * groups + s):base + 8 * (a * groups + s + 1), :] = jnp.broadcast_to(
                    tot[:, s * GROUP:(s + 1) * GROUP], (8, GROUP))


def project(x, g, w3, wo, gamma, beta):
    tokens, width = x.shape
    cols = wo.shape[0]
    groups = cols // GROUP
    part_rows = 2 * groups * (HEAD + 8)
    row = lambda c: row_spec(PROJ_ROWS, c, lambda i: i)
    return pl.pallas_call(
        project_body,
        grid=(tokens // PROJ_ROWS,),
        in_specs=[row(width), row(width), whole(w3.shape), whole(wo.shape), whole((1, width)), whole((1, width))],
        out_specs=[row(width)] + [row(cols)] * 4 + [pl.BlockSpec((part_rows, GROUP), lambda i: (0, 0))],
        out_shape=[sds((tokens, width), BF16)] + [sds((tokens, cols), BF16)] * 4 + [sds((part_rows, GROUP), F32)],
        scratch_shapes=[pltpu.VMEM((groups, GROUP, GROUP), F32)] * 2 + [pltpu.VMEM((8, cols), F32)] * 2,
        name="project",
        compiler_params=params(),
        cost_estimate=cost(2 * tokens * width * cols * 4.4, 2 * tokens * (3 * width + 4 * cols)),
    )(x, g, w3, wo, gamma, beta)


def far_v_body(off_ref, u_ref, w_ref, v_ref):
    v_ref[...] = dot(u_ref[0], w_ref[0]).astype(BF16)


def far_v(off, u2, w3, blocks):
    width, cols = w3.shape[1:]
    rows = 2 * ROWS
    return pl.pallas_call(
        far_v_body,
        grid_spec=pltpu.PrefetchScalarGridSpec(
            num_scalar_prefetch=1,
            grid=(blocks // 2,),
            in_specs=[half_spec(rows, width, 1, 0),
                      pl.BlockSpec((1, width, cols), lambda j, off: (2, 0, 0), pipeline_mode=pl.Buffered(1))],
            out_specs=pl.BlockSpec((rows, cols), lambda j, off: (j, 0)),
        ),
        out_shape=sds((blocks * ROWS, cols), BF16),
        name="far_v",
        compiler_params=params(),
        cost_estimate=cost(2 * blocks * ROWS * width * cols, 2 * blocks * ROWS * (width + cols)),
    )(off, u2, w3)


def state_body(near_ref, far_ref, tau_ref, attn_ref, dgram_ref, coef_ref, dtau_ref, *, groups):
    r_head = lax.broadcasted_iota(jnp.int32, (GROUP, GROUP), 0)
    c_head = lax.broadcasted_iota(jnp.int32, (GROUP, GROUP), 1)
    eye = r_head == c_head
    mask = (r_head // HEAD) == (c_head // HEAD)
    spread = lambda t: jnp.concatenate([t] * (GROUP // HEAD), axis=0)
    to_col = lambda t: jnp.sum(jnp.where(eye, t, 0.0), axis=1, keepdims=True)
    to_row = lambda t: jnp.sum(jnp.where(eye, t, 0.0), axis=0, keepdims=True)
    base = 2 * groups * HEAD
    coef_ref[...] = jnp.zeros_like(coef_ref)
    dtau_ref[...] = jnp.zeros_like(dtau_ref)
    for side, ref in enumerate((near_ref, far_ref)):
        for s in range(groups):
            gram_mat = spread(ref[s * HEAD:(s + 1) * HEAD, :])
            d_attn = spread(ref[(groups + s) * HEAD:(groups + s + 1) * HEAD, :])
            b_row = ref[base + 8 * (groups + s):base + 8 * (groups + s) + 1, :]
            a_col = to_col(ref[base + 8 * s:base + 8 * s + 1, :])
            g = side * groups + s
            tau = to_col(tau_ref[g:g + 1, :])
            norm_prod = jnp.sqrt(a_col) * jnp.sqrt(b_row)
            gram_n = gram_mat / norm_prod
            logit = jnp.where(mask, tau * gram_n, -jnp.inf)
            e = jnp.exp(logit - jnp.max(logit, axis=1, keepdims=True))
            attn = e / jnp.sum(e, axis=1, keepdims=True)
            d_attn = jnp.where(mask, d_attn, 0.0)
            d_logit = jnp.where(mask, attn * (d_attn - jnp.sum(attn * d_attn, axis=1, keepdims=True)), 0.0)
            gram_n = jnp.where(mask, gram_n, 0.0)
            grad_sn = tau * d_logit
            prod = grad_sn * gram_n
            attn_ref[g] = attn.astype(BF16)
            dgram_ref[g] = jnp.where(mask, grad_sn / norm_prod, 0.0).astype(BF16)
            coef_ref[2 * side:2 * side + 1, s * GROUP:(s + 1) * GROUP] = to_row(-jnp.sum(prod, axis=1, keepdims=True) / a_col)
            coef_ref[2 * side + 1:2 * side + 2, s * GROUP:(s + 1) * GROUP] = -jnp.sum(prod, axis=0, keepdims=True) / b_row
            if side == 0:
                dtau_ref[s:s + 1, :] = to_row(jnp.sum(d_logit * gram_n, axis=1, keepdims=True))


def head_state(near, far, tau_rows):
    groups = tau_rows.shape[0] // 2
    vm = pl.BlockSpec(memory_space=pltpu.VMEM)
    return pl.pallas_call(
        functools.partial(state_body, groups=groups),
        in_specs=[vm] * 3,
        out_specs=[vm] * 4,
        out_shape=[sds((2 * groups, GROUP, GROUP), BF16)] * 2 + [sds((8, groups * GROUP), F32), sds((8, GROUP), F32)],
        name="head_state",
        cost_estimate=cost(10**9, 2 * 10**6),
    )(near, far, tau_rows)


def mix_block(q, k, v, do, attn_ref, dgram_ref, coef_ref, side, s):
    groups = attn_ref.shape[0] // 2
    am, gm = attn_ref[side * groups + s], dgram_ref[side * groups + s]
    c = slice(s * GROUP, (s + 1) * GROUP)
    dq = dot(k, gm, NT) + q.astype(F32) * coef_ref[2 * side:2 * side + 1, c]
    dk = dot(q, gm, NN) + k.astype(F32) * coef_ref[2 * side + 1:2 * side + 2, c]
    return dot(v, am, NT).astype(BF16), dq.astype(BF16), dk.astype(BF16), dot(do, am, NN).astype(BF16)


def finish_rows(j, x_ref, g_ref, du, gm_ref, dx_refs, dsum_ref):
    rows, width = x_ref.shape[1:]
    xh, inv = normalize(x_ref[0].astype(F32))
    fold = lambda t: jnp.sum(t.reshape(rows // 8, 8, width), axis=0)
    for a, val in enumerate((fold(du * xh), fold(du))):
        dsum_ref[a] = jnp.where(j == 0, val, dsum_ref[a] + val)
    gh = du * gm_ref[...]
    m1 = jnp.mean(gh, axis=-1, keepdims=True)
    m2 = jnp.mean(gh * xh, axis=-1, keepdims=True)
    dx = (g_ref[0].astype(F32) + inv * (gh - m1 - xh * m2)).astype(BF16)
    for ref in dx_refs:
        ref[0] = dx


def rows_body(*refs, n_alias):
    it = iter(refs)
    nxt = lambda n: [next(it) for _ in range(n)]
    off_ref, x_ref, g_ref, u_ref, q_ref, k_ref, v_ref, do_ref = nxt(8)
    attn_ref, dgram_ref, coef_ref, wn_ref, wf_ref, won_ref, wof_ref, gm_ref = nxt(8)
    nxt(n_alias)
    y_ref, gx_ref, o_ref, rqk_ref, rv_ref, send_ref, dsum_ref = nxt(7)
    on_s, rn_s, of_s, rf_s, qf_s, kf_s, vf_s, dof_s = nxt(8)
    j = pl.program_id(0)
    own, other = off_ref[0], off_ref[1]
    groups = attn_ref.shape[0] // 2
    u = u_ref[0]
    for e, t in enumerate((qf_s, kf_s, vf_s)):
        t[...] = dot(u, wf_ref[e]).astype(BF16)
    dof_s[...] = dot(g_ref[0], wof_ref[...], NT).astype(BF16)
    state = (attn_ref, dgram_ref, coef_ref)
    for s in range(groups):
        c = slice(s * GROUP, (s + 1) * GROUP)
        for half in (own, other):
            o, dq, dk, dv = mix_block(q_ref[half, :, c], k_ref[half, :, c], v_ref[half, :, c], do_ref[half, :, c], *state, 0, s)
            o_ref[half, :, c], rqk_ref[0, half, :, c], rqk_ref[1, half, :, c], rv_ref[half, :, c] = o, dq, dk, dv
            if half is own:
                on_s[:, c], rn_s[0, :, c], rn_s[1, :, c], rn_s[2, :, c] = o, dq, dk, dv
    for s in range(groups):
        c = slice(s * GROUP, (s + 1) * GROUP)
        of_s[:, c], rf_s[0, :, c], rf_s[1, :, c], rf_s[2, :, c] = mix_block(
            qf_s[:, c], kf_s[:, c], vf_s[:, c], dof_s[:, c], *state, 1, s)
    du = dot(rn_s[0], wn_ref[0], NT)
    for e in range(1, 3):
        du += dot(rn_s[e], wn_ref[e], NT)
    for e in range(3):
        du += dot(rf_s[e], wf_ref[e], NT)
    y_ref[0] = (x_ref[0].astype(F32) + (dot(on_s[...], won_ref[...]) + dot(of_s[...], wof_ref[...]))).astype(BF16)
    finish_rows(j, x_ref, g_ref, du, gm_ref, [gx_ref, send_ref], dsum_ref)


def rows_call(off, start, blocks, acts, state, weights, prev):
    _, half, width = acts[0].shape
    cols = weights[2].shape[0]
    row = half_spec(ROWS, width, 0, start)
    both = lambda *lead: both_spec(lead, ROWS, cols, start)
    consts = list(state) + list(weights)
    first = 1 + len(acts) + len(consts)
    return pl.pallas_call(
        functools.partial(rows_body, n_alias=len(prev)),
        grid_spec=pltpu.PrefetchScalarGridSpec(
            num_scalar_prefetch=1,
            grid=(blocks,),
            in_specs=[row] * 3 + [both()] * 4 + [whole(t.shape) for t in consts] + [pl.BlockSpec(memory_space=pl.ANY)] * len(prev),
            out_specs=[row, row, both(), both(2), both(),
                       pl.BlockSpec((1, ROWS, width), lambda j, off: (0, j, 0)),
                       pl.BlockSpec((2, 8, width), lambda j, off: (0, 0, 0))],
            scratch_shapes=[pltpu.VMEM((ROWS, cols), BF16), pltpu.VMEM((3, ROWS, cols), BF16)] * 2 + [pltpu.VMEM((ROWS, cols), BF16)] * 4,
        ),
        out_shape=[sds((2, half, width), BF16)] * 2 + [sds((2, half, cols), BF16), sds((2, 2, half, cols), BF16), sds((2, half, cols), BF16),
                                                       sds((1, blocks * ROWS, width), BF16), sds((2, 8, width), F32)],
        input_output_aliases={first + a: a for a in range(len(prev))},
        name="rows",
        compiler_params=params(),
        cost_estimate=cost(2 * blocks * ROWS * width * cols * 13, 2 * blocks * ROWS * (6 * width + 16 * cols)),
    )(off, *acts, *consts, *prev)


def far_y_body(off_ref, x_ref, o_ref, vu_ref, *refs, fused):
    it = iter(refs)
    nxt = lambda n: [next(it) for _ in range(n)]
    attn_ref, won_ref, wof_ref = nxt(3)
    if fused:
        (wv_ref,) = nxt(1)
    _, y_ref, of_s = nxt(3)
    if fused:
        vf_ref = nxt(1)[0]
        vf_ref[...] = dot(vu_ref[0], wv_ref[0]).astype(BF16)
    else:
        vf_ref = vu_ref
    groups = attn_ref.shape[0] // 2
    for s in range(groups):
        c = slice(s * GROUP, (s + 1) * GROUP)
        of_s[:, c] = dot(vf_ref[:, c], attn_ref[groups + s], NT).astype(BF16)
    y_ref[0] = (x_ref[0].astype(F32) + (dot(o_ref[0], won_ref[...]) + dot(of_s[...], wof_ref[...]))).astype(BF16)


def far_y(off, start, blocks, x2, o2, vu, attn, wo_near, wo_far, w_far, y2):
    fused = vu.ndim == 3
    width, cols = x2.shape[2], o2.shape[2]
    row = lambda c: half_spec(ROWS, c, 1, start)
    args = [x2, o2, vu, attn, wo_near, wo_far]
    specs = [row(width), row(cols), row(width) if fused else pl.BlockSpec((ROWS, cols), lambda j, off: (start + j, 0)),
             whole(attn.shape), whole(wo_near.shape), whole(wo_far.shape)]
    if fused:
        args.append(w_far)
        specs.append(pl.BlockSpec((1, width, cols), lambda j, off: (2, 0, 0), pipeline_mode=pl.Buffered(1)))
    return pl.pallas_call(
        functools.partial(far_y_body, fused=fused),
        grid_spec=pltpu.PrefetchScalarGridSpec(
            num_scalar_prefetch=1,
            grid=(blocks,),
            in_specs=specs + [pl.BlockSpec(memory_space=pl.ANY)],
            out_specs=row(width),
            scratch_shapes=[pltpu.VMEM((ROWS, cols), BF16)] * (2 if fused else 1),
        ),
        out_shape=sds(y2.shape, y2.dtype),
        input_output_aliases={len(args) + 1: 0},
        name="far_y",
        compiler_params=params(),
        cost_estimate=cost(2 * blocks * ROWS * width * cols * (3.2 if fused else 2.2), 2 * blocks * ROWS * (2 * width + 2 * cols)),
    )(off, *args, y2)


def solution(mesh):
    tp_size = mesh.shape["tp"]
    sp_size = mesh.shape["sp"]
    in_rows = P(("dp", "sp"), None)
    swap = [(0, 1), (1, 0)]

    def exchange(t):
        return lax.ppermute(t, "tp", swap)

    def step(x, g, w_qkv, w_out, ln_gamma, ln_beta, temps):
        tokens, width = x.shape
        cols = w_qkv.shape[2]
        groups = cols // GROUP
        me = lax.axis_index("tp")
        w_near = jnp.transpose(w_qkv, (1, 0, 2))
        w_far = exchange(w_near)
        wo_far = exchange(w_out)
        gamma, beta = ln_gamma.reshape(1, width), ln_beta.reshape(1, width)
        half = tokens // 2
        off = jnp.stack([me, 1 - me]).astype(jnp.int32)
        halves = lambda t: t.reshape(2, half, t.shape[-1])

        u, q, k, v, do, part = project(x, g, w_near, w_out, gamma, beta)
        x2, g2, u2 = halves(x), halves(g), halves(u)
        near = tuple(halves(t) for t in (q, k, v, do))
        peers = [lax.ppermute(part, "sp", [(s, s ^ d) for s in range(sp_size)]) for d in (1, 2, 3)]
        part = (part + peers[0]) + (peers[1] + peers[2])
        part_far = exchange(part)
        vf0 = far_v(off, u2, w_far, EARLY_V)
        tau = jnp.repeat(temps, HEAD).reshape(tp_size, groups, GROUP)
        tau = jnp.where(me == 0, tau, tau[::-1]).reshape(2 * groups, GROUP)
        attn, dgram, coef, dtau = head_state(part, part_far, tau)
        state = (attn, dgram, coef)
        dtau = jnp.sum(dtau[:groups].reshape(groups * GROUP // HEAD, HEAD), axis=1)
        dtau_far = exchange(dtau)
        grad_temp = jnp.where(me == 0, jnp.concatenate([dtau, dtau_far]), jnp.concatenate([dtau_far, dtau]))

        prev, dsum, recv, start = (), None, [], 0
        for blocks in OWN_CHUNKS:
            *prev, sent, ds = rows_call(off, start, blocks, (x2, g2, u2) + near, state, (w_near, w_far, w_out, wo_far, gamma), prev)
            recv.append((start, exchange(sent)))
            dsum = ds if dsum is None else dsum + ds
            start += blocks
        y2, gx2, o2, rqk, rv = prev

        dw_qk = lax.dot_general(u, rqk.reshape(2, tokens, cols), (((0,), (1,)), ((), ())), preferred_element_type=F32)
        o2, dw_qk = lax.optimization_barrier((o2, dw_qk))
        dw_qk = lax.psum_scatter(dw_qk, "sp", scatter_dimension=0, tiled=True)
        dw_o = dot(o2.reshape(tokens, cols), g, TN)
        rv, dw_o = lax.optimization_barrier((rv, dw_o))
        grad_wout = lax.psum_scatter(dw_o, "sp", scatter_dimension=0, tiled=True)
        dw_v = dot(u, rv.reshape(tokens, cols), TN)
        y2, dw_v = lax.optimization_barrier((y2, dw_v))
        dw_v = lax.psum_scatter(dw_v, "sp", scatter_dimension=0, tiled=True)
        y2 = far_y(off, 0, EARLY_V, x2, o2, vf0, attn, w_out, wo_far, w_far, y2)
        y2 = far_y(off, EARLY_V, half // ROWS - EARLY_V, x2, o2, u2, attn, w_out, wo_far, w_far, y2)
        grad_wqkv = jnp.concatenate([dw_qk, dw_v[:, None]], axis=1)

        sums = jnp.sum(dsum, axis=1)
        for axis, perm in (("tp", swap), ("sp", [(s, s ^ 1) for s in range(sp_size)]), ("sp", [(s, s ^ 2) for s in range(sp_size)])):
            sums = sums + lax.ppermute(sums, axis, perm)
        for start, blk in recv:
            gx2 = lax.dynamic_update_slice(gx2, blk, (off[1], start * ROWS, 0))
        return y2.reshape(tokens, width), gx2.reshape(tokens, width), grad_wqkv, grad_wout, sums[0], sums[1], grad_temp

    in_specs = (in_rows, in_rows, P(None, None, "tp"), P("tp", None), P(None), P(None), P(None))
    out_specs = (in_rows, in_rows, P(("dp", "sp"), None, "tp"), P(("dp", "tp", "sp"), None), P("dp"), P("dp"), P("dp"))
    return jax.shard_map(step, mesh=mesh, in_specs=in_specs, out_specs=out_specs, check_vma=False)
```

```python
import functools

import jax
import jax.numpy as jnp
from jax import lax
from jax.experimental import pallas as pl
from jax.experimental.pallas import tpu as pltpu
from jax.sharding import PartitionSpec as P


LN_EPS = 1e-6
GROUP = 256
HEAD = 32
LANES = 128
F32 = jnp.float32
BF16 = jnp.bfloat16
NN = (((1,), (0,)), ((), ()))
NT = (((1,), (1,)), ((), ()))
TN = (((0,), (0,)), ((), ()))
PROJ_ROWS = 512
ROWS = 256
SUM_ROWS = 1024
OWN_CHUNKS = ((4,), (6,), (10,), (8, 4))
EARLY_V = 12


def dot(a, b, dims=NN):
    return lax.dot_general(a, b, dims, preferred_element_type=F32)


def normalize(x):
    mean = jnp.mean(x, axis=-1, keepdims=True)
    cen = x - mean
    inv = lax.rsqrt(jnp.mean(cen * cen, axis=-1, keepdims=True) + LN_EPS)
    return cen * inv, mean, inv


def row_spec(rows, cols, index):
    return pl.BlockSpec((rows, cols), lambda *a: (index(*a), 0))


def half_spec(rows, cols, which, start):
    return pl.BlockSpec((1, rows, cols), lambda j, off: (off[which], start + j, 0))


def both_spec(lead, rows, cols, start):
    zeros = (0,) * len(lead)
    return pl.BlockSpec((*lead, 2, rows, cols), lambda j, off: (*zeros, 0, start + j, 0))


def whole(shape):
    return pl.BlockSpec(shape, lambda *a: (0,) * len(shape), pipeline_mode=pl.Buffered(1))


def sds(shape, dtype):
    return jax.ShapeDtypeStruct(shape, dtype)


def params(**kw):
    return pltpu.CompilerParams(vmem_limit_bytes=64_000_000, **kw)


def cost(flops, nbytes):
    return pl.CostEstimate(flops=int(flops), bytes_accessed=int(nbytes), transcendentals=0)


def project_body(x_ref, g_ref, w_ref, wo_ref, gm_ref, bt_ref, u_ref, q_ref, k_ref, v_ref, do_ref, st_ref, part_ref, gr, da, qs, ks):
    i = pl.program_id(0)
    rows, cols = q_ref.shape
    groups = cols // GROUP
    do_ref[...] = dot(g_ref[...], wo_ref[...], NT).astype(BF16)
    xh, mean, inv = normalize(x_ref[...].astype(F32))
    u_ref[...] = (xh * gm_ref[...] + bt_ref[...]).astype(BF16)
    st_ref[...] = jnp.where(lax.broadcasted_iota(jnp.int32, st_ref.shape, 1) < LANES // 2, mean, inv)
    u = u_ref[...]
    for e, out in enumerate((q_ref, k_ref, v_ref)):
        out[...] = dot(u, w_ref[e]).astype(BF16)

    def add(acc, s, val):
        acc[s] = jnp.where(i == 0, val, acc[s] + val)

    for s in range(groups):
        c = slice(s * GROUP, (s + 1) * GROUP)
        add(gr, s, dot(q_ref[:, c], k_ref[:, c], TN))
        add(da, s, dot(do_ref[:, c], v_ref[:, c], TN))
    for acc, t in ((qs, q_ref), (ks, k_ref)):
        f = t[...].astype(F32)
        val = jnp.sum((f * f).reshape(rows // 8, 8, cols), axis=0)
        acc[...] = jnp.where(i == 0, val, acc[...] + val)

    @pl.when(i == pl.num_programs(0) - 1)
    def _():
        col_head = lax.broadcasted_iota(jnp.int32, (HEAD, GROUP), 1) // HEAD
        for a, acc in enumerate((gr, da)):
            for s in range(groups):
                tot = jnp.zeros((HEAD, GROUP), F32)
                for h in range(GROUP // HEAD):
                    tot += jnp.where(col_head == h, acc[s, h * HEAD:(h + 1) * HEAD, :], 0.0)
                part_ref[(a * groups + s) * HEAD:(a * groups + s + 1) * HEAD, :] = tot
        base = 2 * groups * HEAD
        for a, acc in enumerate((qs, ks)):
            tot = jnp.sum(acc[...], axis=0, keepdims=True)
            for s in range(groups):
                part_ref[base + 8 * (a * groups + s):base + 8 * (a * groups + s + 1), :] = jnp.broadcast_to(
                    tot[:, s * GROUP:(s + 1) * GROUP], (8, GROUP))


def project(x, g, w3, wo, gamma, beta):
    tokens, width = x.shape
    cols = wo.shape[0]
    groups = cols // GROUP
    part_rows = 2 * groups * (HEAD + 8)
    row = lambda c: row_spec(PROJ_ROWS, c, lambda i: i)
    return pl.pallas_call(
        project_body,
        grid=(tokens // PROJ_ROWS,),
        in_specs=[row(width), row(width), whole(w3.shape), whole(wo.shape), whole((1, width)), whole((1, width))],
        out_specs=[row(width)] + [row(cols)] * 4 + [row(LANES), pl.BlockSpec((part_rows, GROUP), lambda i: (0, 0))],
        out_shape=[sds((tokens, width), BF16)] + [sds((tokens, cols), BF16)] * 4 + [sds((tokens, LANES), F32), sds((part_rows, GROUP), F32)],
        scratch_shapes=[pltpu.VMEM((groups, GROUP, GROUP), F32)] * 2 + [pltpu.VMEM((8, cols), F32)] * 2,
        name="project",
        compiler_params=params(),
        cost_estimate=cost(2 * tokens * width * cols * 4.4, 2 * tokens * (3 * width + 4 * cols)),
    )(x, g, w3, wo, gamma, beta)


def far_v_body(off_ref, u_ref, w_ref, *refs):
    refs[-1][...] = dot(u_ref[0], w_ref[0]).astype(BF16)


def far_v(off, u2, w3, blocks, part, parts, prev=()):
    width, cols = w3.shape[1:]
    rows = 2 * ROWS
    steps = blocks * ROWS // rows // parts
    return pl.pallas_call(
        far_v_body,
        grid_spec=pltpu.PrefetchScalarGridSpec(
            num_scalar_prefetch=1,
            grid=(steps,),
            in_specs=[half_spec(rows, width, 1, part * steps),
                      pl.BlockSpec((1, width, cols), lambda j, off: (2, 0, 0), pipeline_mode=pl.Buffered(1))]
            + [pl.BlockSpec(memory_space=pl.ANY)] * len(prev),
            out_specs=pl.BlockSpec((rows, cols), lambda j, off: (part * steps + j, 0)),
        ),
        out_shape=sds((blocks * ROWS, cols), BF16),
        input_output_aliases={3: 0} if prev else {},
        name="far_v",
        compiler_params=params(),
        cost_estimate=cost(2 * steps * rows * width * cols, 2 * steps * rows * (width + cols)),
    )(off, u2, w3, *prev)


def state_body(near_ref, far_ref, tau_ref, attn_ref, dgram_ref, coef_ref, dtau_ref, *, groups):
    r_head = lax.broadcasted_iota(jnp.int32, (GROUP, GROUP), 0)
    c_head = lax.broadcasted_iota(jnp.int32, (GROUP, GROUP), 1)
    eye = r_head == c_head
    mask = (r_head // HEAD) == (c_head // HEAD)
    spread = lambda t: jnp.concatenate([t] * (GROUP // HEAD), axis=0)
    to_col = lambda t: jnp.sum(jnp.where(eye, t, 0.0), axis=1, keepdims=True)
    to_row = lambda t: jnp.sum(jnp.where(eye, t, 0.0), axis=0, keepdims=True)
    base = 2 * groups * HEAD
    coef_ref[...] = jnp.zeros_like(coef_ref)
    dtau_ref[...] = jnp.zeros_like(dtau_ref)
    for side, ref in enumerate((near_ref, far_ref)):
        for s in range(groups):
            gram_mat = spread(ref[s * HEAD:(s + 1) * HEAD, :])
            d_attn = spread(ref[(groups + s) * HEAD:(groups + s + 1) * HEAD, :])
            b_row = ref[base + 8 * (groups + s):base + 8 * (groups + s) + 1, :]
            a_col = to_col(ref[base + 8 * s:base + 8 * s + 1, :])
            g = side * groups + s
            tau = to_col(tau_ref[g:g + 1, :])
            norm_prod = jnp.sqrt(a_col) * jnp.sqrt(b_row)
            gram_n = gram_mat / norm_prod
            logit = jnp.where(mask, tau * gram_n, -jnp.inf)
            e = jnp.exp(logit - jnp.max(logit, axis=1, keepdims=True))
            attn = e / jnp.sum(e, axis=1, keepdims=True)
            d_attn = jnp.where(mask, d_attn, 0.0)
            d_logit = jnp.where(mask, attn * (d_attn - jnp.sum(attn * d_attn, axis=1, keepdims=True)), 0.0)
            gram_n = jnp.where(mask, gram_n, 0.0)
            grad_sn = tau * d_logit
            prod = grad_sn * gram_n
            attn_ref[g] = attn.astype(BF16)
            dgram_ref[g] = jnp.where(mask, grad_sn / norm_prod, 0.0).astype(BF16)
            coef_ref[2 * side:2 * side + 1, s * GROUP:(s + 1) * GROUP] = to_row(-jnp.sum(prod, axis=1, keepdims=True) / a_col)
            coef_ref[2 * side + 1:2 * side + 2, s * GROUP:(s + 1) * GROUP] = -jnp.sum(prod, axis=0, keepdims=True) / b_row
            dtau_ref[g:g + 1, :] = to_row(jnp.sum(d_logit * gram_n, axis=1, keepdims=True))


def head_state(near, far, tau_rows):
    groups = tau_rows.shape[0] // 2
    vm = pl.BlockSpec(memory_space=pltpu.VMEM)
    return pl.pallas_call(
        functools.partial(state_body, groups=groups),
        in_specs=[vm] * 3,
        out_specs=[vm] * 4,
        out_shape=[sds((2 * groups, GROUP, GROUP), BF16)] * 2 + [sds((8, groups * GROUP), F32), sds((8, GROUP), F32)],
        name="head_state",
        cost_estimate=cost(10**9, 2 * 10**6),
    )(near, far, tau_rows)


def mix_block(q, k, v, do, attn_ref, dgram_ref, coef_ref, side, s):
    groups = attn_ref.shape[0] // 2
    am, gm = attn_ref[side * groups + s], dgram_ref[side * groups + s]
    c = slice(s * GROUP, (s + 1) * GROUP)
    dq = dot(k, gm, NT) + q.astype(F32) * coef_ref[2 * side:2 * side + 1, c]
    dk = dot(q, gm, NN) + k.astype(F32) * coef_ref[2 * side + 1:2 * side + 2, c]
    return dot(v, am, NT).astype(BF16), dq.astype(BF16), dk.astype(BF16), dot(do, am, NN).astype(BF16)


def finish_rows(j, x_ref, g_ref, st_ref, du, gm_ref, dx_refs, dsum_ref):
    rows, width = x_ref.shape[1:]
    mean, inv = st_ref[0, :, :1], st_ref[0, :, LANES // 2:LANES // 2 + 1]
    xh = (x_ref[0].astype(F32) - mean) * inv
    fold = lambda t: jnp.sum(t.reshape(rows // 8, 8, width), axis=0)
    for a, val in enumerate((fold(du * xh), fold(du))):
        dsum_ref[a] = jnp.where(j == 0, val, dsum_ref[a] + val)
    gh = du * gm_ref[...]
    m1 = jnp.mean(gh, axis=-1, keepdims=True)
    m2 = jnp.mean(gh * xh, axis=-1, keepdims=True)
    dx = (g_ref[0].astype(F32) + inv * (gh - m1 - xh * m2)).astype(BF16)
    for ref in dx_refs:
        ref[0] = dx


def rows_body(*refs, n_alias, send_blocks):
    it = iter(refs)
    nxt = lambda n: [next(it) for _ in range(n)]
    off_ref, x_ref, g_ref, u_ref, st_ref, q_ref, k_ref, v_ref, do_ref = nxt(9)
    attn_ref, dgram_ref, coef_ref, wn_ref, wf_ref, won_ref, wof_ref, gm_ref = nxt(8)
    nxt(n_alias)
    y_ref, gx_ref, o_ref, rqk_ref, rv_ref = nxt(5)
    send_refs = nxt(len(send_blocks))
    (dsum_ref,) = nxt(1)
    on_s, rn_s, of_s, rf_s, qf_s, kf_s, vf_s, dof_s = nxt(8)
    j = pl.program_id(0)
    own, other = off_ref[0], off_ref[1]
    groups = attn_ref.shape[0] // 2
    u = u_ref[0]
    for e, t in enumerate((qf_s, kf_s, vf_s)):
        t[...] = dot(u, wf_ref[e]).astype(BF16)
    dof_s[...] = dot(g_ref[0], wof_ref[...], NT).astype(BF16)
    state = (attn_ref, dgram_ref, coef_ref)
    for s in range(groups):
        c = slice(s * GROUP, (s + 1) * GROUP)
        for half in (own, other):
            o, dq, dk, dv = mix_block(q_ref[half, :, c], k_ref[half, :, c], v_ref[half, :, c], do_ref[half, :, c], *state, 0, s)
            o_ref[half, :, c], rqk_ref[0, half, :, c], rqk_ref[1, half, :, c], rv_ref[half, :, c] = o, dq, dk, dv
            if half is own:
                on_s[:, c], rn_s[0, :, c], rn_s[1, :, c], rn_s[2, :, c] = o, dq, dk, dv
    for s in range(groups):
        c = slice(s * GROUP, (s + 1) * GROUP)
        of_s[:, c], rf_s[0, :, c], rf_s[1, :, c], rf_s[2, :, c] = mix_block(
            qf_s[:, c], kf_s[:, c], vf_s[:, c], dof_s[:, c], *state, 1, s)
    du = dot(rn_s[0], wn_ref[0], NT)
    for e in range(1, 3):
        du += dot(rn_s[e], wn_ref[e], NT)
    for e in range(3):
        du += dot(rf_s[e], wf_ref[e], NT)
    y_ref[0] = (x_ref[0].astype(F32) + (dot(on_s[...], won_ref[...]) + dot(of_s[...], wof_ref[...]))).astype(BF16)
    if len(send_refs) == 1:
        finish_rows(j, x_ref, g_ref, st_ref, du, gm_ref, [gx_ref] + send_refs, dsum_ref)
        return
    finish_rows(j, x_ref, g_ref, st_ref, du, gm_ref, [gx_ref], dsum_ref)
    start = 0
    for ref, n in zip(send_refs, send_blocks):

        @pl.when((j >= start) & (j < start + n))
        def _(ref=ref):
            ref[0] = gx_ref[0]

        start += n


def rows_call(off, start, send_blocks, acts, state, weights, prev):
    _, half, width = acts[0].shape
    blocks = sum(send_blocks)
    firsts = [sum(send_blocks[:n]) for n in range(len(send_blocks))]
    send_spec = lambda first, n: pl.BlockSpec((1, ROWS, width), lambda j, off: (0, jnp.clip(j - first, 0, n - 1), 0))
    cols = weights[2].shape[0]
    row = half_spec(ROWS, width, 0, start)
    both = lambda *lead: both_spec(lead, ROWS, cols, start)
    consts = list(state) + list(weights)
    first = 1 + len(acts) + len(consts)
    return pl.pallas_call(
        functools.partial(rows_body, n_alias=len(prev), send_blocks=send_blocks),
        grid_spec=pltpu.PrefetchScalarGridSpec(
            num_scalar_prefetch=1,
            grid=(blocks,),
            in_specs=[row] * 3 + [half_spec(ROWS, LANES, 0, start)] + [both()] * 4 + [whole(t.shape) for t in consts] + [pl.BlockSpec(memory_space=pl.ANY)] * len(prev),
            out_specs=[row, row, both(), both(2), both(),
                       *[send_spec(first, n) for first, n in zip(firsts, send_blocks)],
                       pl.BlockSpec((2, 8, width), lambda j, off: (0, 0, 0))],
            scratch_shapes=[pltpu.VMEM((ROWS, cols), BF16), pltpu.VMEM((3, ROWS, cols), BF16)] * 2 + [pltpu.VMEM((ROWS, cols), BF16)] * 4,
        ),
        out_shape=[sds((2, half, width), BF16)] * 2 + [sds((2, half, cols), BF16), sds((2, 2, half, cols), BF16), sds((2, half, cols), BF16),
                                                       *[sds((1, n * ROWS, width), BF16) for n in send_blocks], sds((2, 8, width), F32)],
        input_output_aliases={first + a: a for a in range(len(prev))},
        name="rows",
        compiler_params=params(),
        cost_estimate=cost(2 * blocks * ROWS * width * cols * 13, 2 * blocks * ROWS * (6 * width + 16 * cols)),
    )(off, *acts, *consts, *prev)


def far_y_body(*refs, early, copies):
    it = iter(refs)
    nxt = lambda n: [next(it) for _ in range(n)]
    _, x_ref, o_ref, u_ref, v_ref, attn_ref, won_ref, wof_ref, wv_ref = nxt(9)
    recv = nxt(len(copies))
    _, _, y_ref, gx_ref, vf_s, of_s = nxt(6)
    j = pl.program_id(0)
    start = 0
    for ref, n in zip(recv, copies):

        @pl.when((j >= start) & (j < start + n))
        def _(ref=ref):
            gx_ref[0] = ref[0]

        start += n

    @pl.when(j < early)
    def _():
        vf_s[...] = v_ref[...]

    @pl.when(j >= early)
    def _():
        vf_s[...] = dot(u_ref[0], wv_ref[0]).astype(BF16)

    groups = attn_ref.shape[0] // 2
    for s in range(groups):
        c = slice(s * GROUP, (s + 1) * GROUP)
        of_s[:, c] = dot(vf_s[:, c], attn_ref[groups + s], NT).astype(BF16)
    y_ref[0] = (x_ref[0].astype(F32) + (dot(o_ref[0], won_ref[...]) + dot(of_s[...], wof_ref[...]))).astype(BF16)


def far_y(off, x2, o2, u2, vf, attn, wo_near, wo_far, w_far, recv, y2, gx2):
    half, width = x2.shape[1:]
    cols = o2.shape[2]
    rows = 2 * ROWS
    steps = half // rows
    early = vf.shape[0] // rows
    copies = [t.shape[1] // rows for t in recv]
    row = lambda c: half_spec(rows, c, 1, 0)
    specs = [row(width), row(cols),
             pl.BlockSpec((1, rows, width), lambda j, off: (off[1], jnp.maximum(j, early), 0)),
             pl.BlockSpec((rows, cols), lambda j, off: (jnp.minimum(j, early - 1), 0)),
             whole(attn.shape), whole(wo_near.shape), whole(wo_far.shape),
             pl.BlockSpec((1, width, cols), lambda j, off: (2, 0, 0), pipeline_mode=pl.Buffered(1))]
    for k, n in enumerate(copies):
        first = sum(copies[:k])
        specs.append(pl.BlockSpec((1, rows, width), lambda j, off, first=first, n=n: (0, jnp.clip(j - first, 0, n - 1), 0)))
    args = [x2, o2, u2, vf, attn, wo_near, wo_far, w_far, *recv]
    return pl.pallas_call(
        functools.partial(far_y_body, early=early, copies=copies),
        grid_spec=pltpu.PrefetchScalarGridSpec(
            num_scalar_prefetch=1,
            grid=(steps,),
            in_specs=specs + [pl.BlockSpec(memory_space=pl.ANY)] * 2,
            out_specs=[row(width), pl.BlockSpec((1, rows, width), lambda j, off: (off[1], jnp.minimum(j, sum(copies) - 1), 0))],
            scratch_shapes=[pltpu.VMEM((rows, cols), BF16)] * 2,
        ),
        out_shape=[sds(y2.shape, y2.dtype), sds(gx2.shape, gx2.dtype)],
        input_output_aliases={len(args) + 1: 0, len(args) + 2: 1},
        name="far_y",
        compiler_params=params(),
        cost_estimate=cost(2 * half * width * cols * 2.8, 2 * half * (4 * width + 3 * cols)),
    )(off, *args, y2, gx2)


def token_sum_body(l_ref, r_ref, o_ref):
    @pl.when(pl.program_id(0) == 0)
    def _():
        o_ref[...] = jnp.zeros_like(o_ref)

    for e in range(r_ref.shape[0]):
        o_ref[e] += dot(l_ref[...], r_ref[e], TN)


def token_sum(lhs, rhs):
    planes, tokens, cols = rhs.shape
    width = lhs.shape[1]
    return pl.pallas_call(
        token_sum_body,
        grid=(tokens // SUM_ROWS,),
        in_specs=[row_spec(SUM_ROWS, width, lambda i: i), pl.BlockSpec((planes, SUM_ROWS, cols), lambda i: (0, i, 0))],
        out_specs=pl.BlockSpec((planes, width, cols), lambda i: (0, 0, 0)),
        out_shape=sds((planes, width, cols), F32),
        name="token_sum",
        compiler_params=params(),
        cost_estimate=cost(2 * planes * tokens * width * cols, 2 * tokens * (width + planes * cols)),
    )(lhs, rhs)


def solution(mesh):
    tp_size = mesh.shape["tp"]
    sp_size = mesh.shape["sp"]
    in_rows = P(("dp", "sp"), None)
    swap = [(0, 1), (1, 0)]

    def exchange(t):
        return lax.ppermute(t, "tp", swap)

    def step(x, g, w_qkv, w_out, ln_gamma, ln_beta, temps):
        tokens, width = x.shape
        cols = w_qkv.shape[2]
        groups = cols // GROUP
        me = lax.axis_index("tp")
        w_near = jnp.transpose(w_qkv, (1, 0, 2))
        w_far = exchange(w_near)
        wo_far = exchange(w_out)
        gamma, beta = ln_gamma.reshape(1, width), ln_beta.reshape(1, width)
        half = tokens // 2
        off = jnp.stack([me, 1 - me]).astype(jnp.int32)
        halves = lambda t: t.reshape(2, half, t.shape[-1])

        u, q, k, v, do, stats, part = project(x, g, w_near, w_out, gamma, beta)
        x2, g2, u2, stats2 = halves(x), halves(g), halves(u), halves(stats)
        near = tuple(halves(t) for t in (q, k, v, do))
        peers = [lax.ppermute(part, "sp", [(s, s ^ d) for s in range(sp_size)]) for d in (1, 2, 3)]
        part = (part + peers[0]) + (peers[1] + peers[2])
        part_far = exchange(part)
        vf = far_v(off, u2, w_far, EARLY_V, 0, 2)
        vf = far_v(off, u2, w_far, EARLY_V, 1, 2, (vf,))
        tau = jnp.repeat(temps, HEAD).reshape(tp_size, groups, GROUP)
        tau = jnp.where(me == 0, tau, tau[::-1]).reshape(2 * groups, GROUP)
        attn, dgram, coef, dtau = head_state(part, part_far, tau)
        state = (attn, dgram, coef)

        prev, dsum, recv, start = (), None, [], 0
        for sizes in OWN_CHUNKS:
            out = rows_call(off, start, sizes, (x2, g2, u2, stats2) + near, state, (w_near, w_far, w_out, wo_far, gamma), prev)
            prev, sent, ds = out[:5], out[5:-1], out[-1]
            recv += [exchange(t) for t in sent]
            dsum = ds if dsum is None else dsum + ds
            start += sum(sizes)
        y2, gx2, o2, rqk, rv = prev
        dtau, rqk = lax.optimization_barrier((dtau, rqk))
        dtau = jnp.sum(dtau[:2 * groups].reshape(tp_size, cols // HEAD, HEAD), axis=2)
        grad_temp = jnp.where(me == 0, dtau, dtau[::-1]).reshape(-1)

        dw_qk = token_sum(u, rqk.reshape(2, tokens, cols))
        o2, dw_qk = lax.optimization_barrier((o2, dw_qk))
        dw_qk = lax.psum_scatter(dw_qk, "sp", scatter_dimension=1, tiled=True)
        dw_o = token_sum(o2.reshape(tokens, cols), g[None])[0]
        rv, dw_o = lax.optimization_barrier((rv, dw_o))
        grad_wout = lax.psum_scatter(dw_o, "sp", scatter_dimension=0, tiled=True)
        dw_v = token_sum(u, rv.reshape(1, tokens, cols))
        y2, dw_v = lax.optimization_barrier((y2, dw_v))
        dw_v = lax.psum_scatter(dw_v, "sp", scatter_dimension=1, tiled=True)
        y2, gx2 = far_y(off, x2, o2, u2, vf, attn, w_out, wo_far, w_far, recv[:-1], y2, gx2)
        grad_wqkv = jnp.transpose(jnp.concatenate([dw_qk, dw_v], axis=0), (1, 0, 2))

        sums = jnp.sum(dsum, axis=1)
        for axis, perm in (("tp", swap), ("sp", [(s, s ^ 1) for s in range(sp_size)]), ("sp", [(s, s ^ 2) for s in range(sp_size)])):
            sums = sums + lax.ppermute(sums, axis, perm)
        gx2 = lax.dynamic_update_slice(gx2, recv[-1], (off[1], half - recv[-1].shape[1], 0))
        return y2.reshape(tokens, width), gx2.reshape(tokens, width), grad_wqkv, grad_wout, sums[0], sums[1], grad_temp

    in_specs = (in_rows, in_rows, P(None, None, "tp"), P("tp", None), P(None), P(None), P(None))
    out_specs = (in_rows, in_rows, P(("dp", "sp"), None, "tp"), P(("dp", "tp", "sp"), None), P("dp"), P("dp"), P("dp"))
    return jax.shard_map(step, mesh=mesh, in_specs=in_specs, out_specs=out_specs, check_vma=False)
```

```python
import functools

import jax
import jax.numpy as jnp
from jax import lax
from jax.experimental import pallas as pl
from jax.experimental.pallas import tpu as pltpu
from jax.sharding import PartitionSpec as P


LN_EPS = 1e-6
GROUP = 256
HEAD = 32
LANES = 128
F32 = jnp.float32
BF16 = jnp.bfloat16
NN = (((1,), (0,)), ((), ()))
NT = (((1,), (1,)), ((), ()))
TN = (((0,), (0,)), ((), ()))
PROJ_ROWS = 1024
ROWS = 256
SUM_ROWS = 1024
OWN_CHUNKS = ((4,), (6,), (10,), (8, 4))
EARLY_V = 12


def dot(a, b, dims=NN):
    return lax.dot_general(a, b, dims, preferred_element_type=F32)


def normalize(x):
    mean = jnp.mean(x, axis=-1, keepdims=True)
    cen = x - mean
    inv = lax.rsqrt(jnp.mean(cen * cen, axis=-1, keepdims=True) + LN_EPS)
    return cen * inv, mean, inv


def row_spec(rows, cols, index):
    return pl.BlockSpec((rows, cols), lambda *a: (index(*a), 0))


def half_spec(rows, cols, which, start):
    return pl.BlockSpec((1, rows, cols), lambda j, off: (off[which], start + j, 0))


def both_spec(lead, rows, cols, start):
    zeros = (0,) * len(lead)
    return pl.BlockSpec((*lead, 2, rows, cols), lambda j, off: (*zeros, 0, start + j, 0))


def whole(shape):
    return pl.BlockSpec(shape, lambda *a: (0,) * len(shape), pipeline_mode=pl.Buffered(1))


def sds(shape, dtype):
    return jax.ShapeDtypeStruct(shape, dtype)


def params(**kw):
    return pltpu.CompilerParams(vmem_limit_bytes=64_000_000, **kw)


def cost(flops, nbytes):
    return pl.CostEstimate(flops=int(flops), bytes_accessed=int(nbytes), transcendentals=0)


def project_body(x_ref, g_ref, w_ref, wo_ref, gm_ref, bt_ref, u_ref, q_ref, k_ref, v_ref, do_ref, st_ref, part_ref, gr, da, qs, ks):
    i = pl.program_id(0)
    rows, cols = q_ref.shape
    groups = cols // GROUP
    do_ref[...] = dot(g_ref[...], wo_ref[...], NT).astype(BF16)
    xh, mean, inv = normalize(x_ref[...].astype(F32))
    u_ref[...] = (xh * gm_ref[...].reshape(1, -1) + bt_ref[...].reshape(1, -1)).astype(BF16)
    st_ref[...] = jnp.where(lax.broadcasted_iota(jnp.int32, st_ref.shape, 1) < LANES // 2, mean, inv)
    u = u_ref[...]
    for e, out in enumerate((q_ref, k_ref, v_ref)):
        out[...] = dot(u, w_ref[e]).astype(BF16)

    def add(acc, s, val):
        acc[s] = jnp.where(i == 0, val, acc[s] + val)

    for s in range(groups):
        c = slice(s * GROUP, (s + 1) * GROUP)
        add(gr, s, dot(q_ref[:, c], k_ref[:, c], TN))
        add(da, s, dot(do_ref[:, c], v_ref[:, c], TN))
    for acc, t in ((qs, q_ref), (ks, k_ref)):
        f = t[...].astype(F32)
        val = jnp.sum((f * f).reshape(rows // 8, 8, cols), axis=0)
        acc[...] = jnp.where(i == 0, val, acc[...] + val)

    @pl.when(i == pl.num_programs(0) - 1)
    def _():
        col_head = lax.broadcasted_iota(jnp.int32, (HEAD, GROUP), 1) // HEAD
        for a, acc in enumerate((gr, da)):
            for s in range(groups):
                tot = jnp.zeros((HEAD, GROUP), F32)
                for h in range(GROUP // HEAD):
                    tot += jnp.where(col_head == h, acc[s, h * HEAD:(h + 1) * HEAD, :], 0.0)
                part_ref[(a * groups + s) * HEAD:(a * groups + s + 1) * HEAD, :] = tot
        base = 2 * groups * HEAD
        for a, acc in enumerate((qs, ks)):
            tot = jnp.sum(acc[...], axis=0, keepdims=True)
            for s in range(groups):
                part_ref[base + 8 * (a * groups + s):base + 8 * (a * groups + s + 1), :] = jnp.broadcast_to(
                    tot[:, s * GROUP:(s + 1) * GROUP], (8, GROUP))


def project(x, g, w3, wo, gamma, beta):
    tokens, width = x.shape
    cols = wo.shape[0]
    groups = cols // GROUP
    part_rows = 2 * groups * (HEAD + 8)
    row = lambda c: row_spec(PROJ_ROWS, c, lambda i: i)
    return pl.pallas_call(
        project_body,
        grid=(tokens // PROJ_ROWS,),
        in_specs=[row(width), row(width), whole(w3.shape), whole(wo.shape), whole(gamma.shape), whole(beta.shape)],
        out_specs=[row(width)] + [row(cols)] * 4 + [row(LANES), pl.BlockSpec((part_rows, GROUP), lambda i: (0, 0))],
        out_shape=[sds((tokens, width), BF16)] + [sds((tokens, cols), BF16)] * 4 + [sds((tokens, LANES), F32), sds((part_rows, GROUP), F32)],
        scratch_shapes=[pltpu.VMEM((groups, GROUP, GROUP), F32)] * 2 + [pltpu.VMEM((8, cols), F32)] * 2,
        name="project",
        compiler_params=params(),
        cost_estimate=cost(2 * tokens * width * cols * 4.4, 2 * tokens * (3 * width + 4 * cols)),
    )(x, g, w3, wo, gamma, beta)


def far_v_body(off_ref, u_ref, w_ref, *refs):
    refs[-1][...] = dot(u_ref[0], w_ref[0]).astype(BF16)


def far_v(off, u2, w3, blocks, part, parts, prev=()):
    width, cols = w3.shape[1:]
    rows = 2 * ROWS
    steps = blocks * ROWS // rows // parts
    return pl.pallas_call(
        far_v_body,
        grid_spec=pltpu.PrefetchScalarGridSpec(
            num_scalar_prefetch=1,
            grid=(steps,),
            in_specs=[half_spec(rows, width, 1, part * steps),
                      pl.BlockSpec((1, width, cols), lambda j, off: (2, 0, 0), pipeline_mode=pl.Buffered(1))]
            + [pl.BlockSpec(memory_space=pl.ANY)] * len(prev),
            out_specs=pl.BlockSpec((rows, cols), lambda j, off: (part * steps + j, 0)),
        ),
        out_shape=sds((blocks * ROWS, cols), BF16),
        input_output_aliases={3: 0} if prev else {},
        name="far_v",
        compiler_params=params(),
        cost_estimate=cost(2 * steps * rows * width * cols, 2 * steps * rows * (width + cols)),
    )(off, u2, w3, *prev)


def state_body(near_ref, far_ref, tau_ref, attn_ref, dgram_ref, coef_ref, dtau_ref, *, groups):
    r_head = lax.broadcasted_iota(jnp.int32, (GROUP, GROUP), 0)
    c_head = lax.broadcasted_iota(jnp.int32, (GROUP, GROUP), 1)
    eye = r_head == c_head
    mask = (r_head // HEAD) == (c_head // HEAD)
    spread = lambda t: jnp.concatenate([t] * (GROUP // HEAD), axis=0)
    to_col = lambda t: jnp.sum(jnp.where(eye, t, 0.0), axis=1, keepdims=True)
    to_row = lambda t: jnp.sum(jnp.where(eye, t, 0.0), axis=0, keepdims=True)
    base = 2 * groups * HEAD
    coef_ref[...] = jnp.zeros_like(coef_ref)
    dtau_ref[...] = jnp.zeros_like(dtau_ref)
    for side, ref in enumerate((near_ref, far_ref)):
        for s in range(groups):
            gram_mat = spread(ref[s * HEAD:(s + 1) * HEAD, :])
            d_attn = spread(ref[(groups + s) * HEAD:(groups + s + 1) * HEAD, :])
            b_row = ref[base + 8 * (groups + s):base + 8 * (groups + s) + 1, :]
            a_col = to_col(ref[base + 8 * s:base + 8 * s + 1, :])
            g = side * groups + s
            tau = to_col(tau_ref[g:g + 1, :])
            norm_prod = jnp.sqrt(a_col) * jnp.sqrt(b_row)
            gram_n = gram_mat / norm_prod
            logit = jnp.where(mask, tau * gram_n, -jnp.inf)
            e = jnp.exp(logit - jnp.max(logit, axis=1, keepdims=True))
            attn = e / jnp.sum(e, axis=1, keepdims=True)
            d_attn = jnp.where(mask, d_attn, 0.0)
            d_logit = jnp.where(mask, attn * (d_attn - jnp.sum(attn * d_attn, axis=1, keepdims=True)), 0.0)
            gram_n = jnp.where(mask, gram_n, 0.0)
            grad_sn = tau * d_logit
            prod = grad_sn * gram_n
            attn_ref[g] = attn.astype(BF16)
            dgram_ref[g] = jnp.where(mask, grad_sn / norm_prod, 0.0).astype(BF16)
            coef_ref[2 * side:2 * side + 1, s * GROUP:(s + 1) * GROUP] = to_row(-jnp.sum(prod, axis=1, keepdims=True) / a_col)
            coef_ref[2 * side + 1:2 * side + 2, s * GROUP:(s + 1) * GROUP] = -jnp.sum(prod, axis=0, keepdims=True) / b_row
            dtau_ref[g:g + 1, :] = to_row(jnp.sum(d_logit * gram_n, axis=1, keepdims=True))


def head_state(near, far, tau_rows):
    groups = tau_rows.shape[0] // 2
    vm = pl.BlockSpec(memory_space=pltpu.VMEM)
    return pl.pallas_call(
        functools.partial(state_body, groups=groups),
        in_specs=[vm] * 3,
        out_specs=[vm] * 4,
        out_shape=[sds((2 * groups, GROUP, GROUP), BF16)] * 2 + [sds((8, groups * GROUP), F32), sds((8, GROUP), F32)],
        name="head_state",
        cost_estimate=cost(10**9, 2 * 10**6),
    )(near, far, tau_rows)


def mix_block(q, k, v, do, attn_ref, dgram_ref, coef_ref, side, s):
    groups = attn_ref.shape[0] // 2
    am, gm = attn_ref[side * groups + s], dgram_ref[side * groups + s]
    c = slice(s * GROUP, (s + 1) * GROUP)
    dq = dot(k, gm, NT) + q.astype(F32) * coef_ref[2 * side:2 * side + 1, c]
    dk = dot(q, gm, NN) + k.astype(F32) * coef_ref[2 * side + 1:2 * side + 2, c]
    return dot(v, am, NT).astype(BF16), dq.astype(BF16), dk.astype(BF16), dot(do, am, NN).astype(BF16)


def finish_rows(j, x_ref, g_ref, st_ref, du, gm_ref, dx_refs, dsum_ref):
    rows, width = x_ref.shape[1:]
    mean, inv = st_ref[0, :, :1], st_ref[0, :, LANES // 2:LANES // 2 + 1]
    xh = (x_ref[0].astype(F32) - mean) * inv
    fold = lambda t: jnp.sum(t.reshape(rows // 8, 8, width), axis=0)
    for a, val in enumerate((fold(du * xh), fold(du))):
        dsum_ref[a] = jnp.where(j == 0, val, dsum_ref[a] + val)
    gh = du * gm_ref[...].reshape(1, width)
    m1 = jnp.mean(gh, axis=-1, keepdims=True)
    m2 = jnp.mean(gh * xh, axis=-1, keepdims=True)
    dx = (g_ref[0].astype(F32) + inv * (gh - m1 - xh * m2)).astype(BF16)
    for ref in dx_refs:
        ref[0] = dx


def rows_body(*refs, n_alias, send_blocks):
    it = iter(refs)
    nxt = lambda n: [next(it) for _ in range(n)]
    off_ref, x_ref, g_ref, u_ref, st_ref, q_ref, k_ref, v_ref, do_ref = nxt(9)
    attn_ref, dgram_ref, coef_ref, gm_ref = nxt(4)
    w_hbm = nxt(4)
    nxt(n_alias)
    y_ref, gx_ref, o_ref, rqk_ref, rv_ref = nxt(5)
    send_refs = nxt(len(send_blocks))
    (dsum_ref,) = nxt(1)
    on_s, rn_s, of_s, rf_s, qf_s, kf_s, vf_s, dof_s = nxt(8)
    w_refs, w_sems = nxt(4), nxt(1)[0]
    wf_ref, wof_ref, wn_ref, won_ref = w_refs
    j = pl.program_id(0)
    own, other = off_ref[0], off_ref[1]
    groups = attn_ref.shape[0] // 2
    state = (attn_ref, dgram_ref, coef_ref)
    loads = [pltpu.make_async_copy(src, dst, w_sems.at[n]) for n, (src, dst) in enumerate(zip(w_hbm, w_refs))]

    def compute(wait):
        for s in range(groups):
            c = slice(s * GROUP, (s + 1) * GROUP)
            for half in (own, other):
                o, dq, dk, dv = mix_block(q_ref[half, :, c], k_ref[half, :, c], v_ref[half, :, c], do_ref[half, :, c], *state, 0, s)
                o_ref[half, :, c], rqk_ref[0, half, :, c], rqk_ref[1, half, :, c], rv_ref[half, :, c] = o, dq, dk, dv
                if half is own:
                    on_s[:, c], rn_s[0, :, c], rn_s[1, :, c], rn_s[2, :, c] = o, dq, dk, dv
        wait(0)
        wait(1)
        u = u_ref[0]
        for e, t in enumerate((qf_s, kf_s, vf_s)):
            t[...] = dot(u, wf_ref[e]).astype(BF16)
        dof_s[...] = dot(g_ref[0], wof_ref[...], NT).astype(BF16)
        for s in range(groups):
            c = slice(s * GROUP, (s + 1) * GROUP)
            of_s[:, c], rf_s[0, :, c], rf_s[1, :, c], rf_s[2, :, c] = mix_block(
                qf_s[:, c], kf_s[:, c], vf_s[:, c], dof_s[:, c], *state, 1, s)
        wait(2)
        wait(3)
        du = dot(rn_s[0], wn_ref[0], NT)
        for e in range(1, 3):
            du += dot(rn_s[e], wn_ref[e], NT)
        for e in range(3):
            du += dot(rf_s[e], wf_ref[e], NT)
        y_ref[0] = (x_ref[0].astype(F32) + (dot(on_s[...], won_ref[...]) + dot(of_s[...], wof_ref[...]))).astype(BF16)
        finish_rows(j, x_ref, g_ref, st_ref, du, gm_ref, [gx_ref] + send_refs[:1] * (len(send_refs) == 1), dsum_ref)

    @pl.when(j == 0)
    def _():
        for load in loads:
            load.start()
        compute(lambda n: loads[n].wait())

    @pl.when(j > 0)
    def _():
        compute(lambda n: None)

    if len(send_refs) > 1:
        start = 0
        for ref, n in zip(send_refs, send_blocks):

            @pl.when((j >= start) & (j < start + n))
            def _(ref=ref):
                ref[0] = gx_ref[0]

            start += n


def rows_call(off, start, send_blocks, acts, state, weights, prev):
    _, half, width = acts[0].shape
    blocks = sum(send_blocks)
    firsts = [sum(send_blocks[:n]) for n in range(len(send_blocks))]
    send_spec = lambda first, n: pl.BlockSpec((1, ROWS, width), lambda j, off: (0, jnp.clip(j - first, 0, n - 1), 0))
    cols = weights[2].shape[0]
    row = half_spec(ROWS, width, 0, start)
    both = lambda *lead: both_spec(lead, ROWS, cols, start)
    w_near, w_far, wo_near, wo_far, gamma = weights
    consts = list(state) + [gamma]
    loaded = [w_far, wo_far, w_near, wo_near]
    first = 1 + len(acts) + len(consts) + len(loaded)
    return pl.pallas_call(
        functools.partial(rows_body, n_alias=len(prev), send_blocks=send_blocks),
        grid_spec=pltpu.PrefetchScalarGridSpec(
            num_scalar_prefetch=1,
            grid=(blocks,),
            in_specs=[row] * 3 + [half_spec(ROWS, LANES, 0, start)] + [both()] * 4 + [whole(t.shape) for t in consts] + [pl.BlockSpec(memory_space=pl.ANY)] * (len(loaded) + len(prev)),
            out_specs=[row, row, both(), both(2), both(),
                       *[send_spec(first, n) for first, n in zip(firsts, send_blocks)],
                       pl.BlockSpec((2, 8, width), lambda j, off: (0, 0, 0))],
            scratch_shapes=[pltpu.VMEM((ROWS, cols), BF16), pltpu.VMEM((3, ROWS, cols), BF16)] * 2 + [pltpu.VMEM((ROWS, cols), BF16)] * 4
            + [pltpu.VMEM(t.shape, t.dtype) for t in loaded] + [pltpu.SemaphoreType.DMA((len(loaded),))],
        ),
        out_shape=[sds((2, half, width), BF16)] * 2 + [sds((2, half, cols), BF16), sds((2, 2, half, cols), BF16), sds((2, half, cols), BF16),
                                                       *[sds((1, n * ROWS, width), BF16) for n in send_blocks], sds((2, 8, width), F32)],
        input_output_aliases={first + a: a for a in range(len(prev))},
        name="rows",
        compiler_params=params(),
        cost_estimate=cost(2 * blocks * ROWS * width * cols * 13, 2 * blocks * ROWS * (6 * width + 16 * cols)),
    )(off, *acts, *consts, *loaded, *prev)


def far_y_body(*refs, early, copies):
    it = iter(refs)
    nxt = lambda n: [next(it) for _ in range(n)]
    _, x_ref, o_ref, u_ref, v_ref, attn_ref, won_ref, wof_ref, wv_ref, qk_ref = nxt(10)
    recv = nxt(len(copies))
    _, _, y_ref, gx_ref, gw_ref, vf_s, of_s, sem = nxt(8)
    j = pl.program_id(0)
    rows = gx_ref.shape[1]

    def file_rows(act):
        start = 0
        for ref, n in zip(recv, copies):

            @pl.when((j >= start) & (j < start + n))
            def _(ref=ref, start=start):
                act(pltpu.make_async_copy(ref.at[0, pl.ds((j - start) * rows, rows)], gx_ref.at[0], sem))

            start += n

    file_rows(lambda copy: copy.start())
    gw_ref[...] = qk_ref[...]

    @pl.when(j < early)
    def _():
        vf_s[...] = v_ref[...]

    @pl.when(j >= early)
    def _():
        vf_s[...] = dot(u_ref[0], wv_ref[0]).astype(BF16)

    groups = attn_ref.shape[0] // 2
    for s in range(groups):
        c = slice(s * GROUP, (s + 1) * GROUP)
        of_s[:, c] = dot(vf_s[:, c], attn_ref[groups + s], NT).astype(BF16)
    y_ref[0] = (x_ref[0].astype(F32) + (dot(o_ref[0], won_ref[...]) + dot(of_s[...], wof_ref[...]))).astype(BF16)
    file_rows(lambda copy: copy.wait())


def far_y(off, x2, o2, u2, vf, attn, wo_near, wo_far, w_far, dw_qk, recv, y2, gx2):
    half, width = x2.shape[1:]
    cols = o2.shape[2]
    rows = 2 * ROWS
    steps = half // rows
    early = vf.shape[0] // rows
    copies = [t.shape[1] // rows for t in recv]
    row = lambda c: half_spec(rows, c, 1, 0)
    per = steps // 2
    plane = pl.BlockSpec((1, dw_qk.shape[1] // per, cols), lambda j, off: (j // per, j % per, 0))
    any_ = pl.BlockSpec(memory_space=pl.ANY)
    specs = [row(width), row(cols),
             pl.BlockSpec((1, rows, width), lambda j, off: (off[1], jnp.maximum(j, early), 0)),
             pl.BlockSpec((rows, cols), lambda j, off: (jnp.minimum(j, early - 1), 0)),
             whole(attn.shape), whole(wo_near.shape), whole(wo_far.shape),
             pl.BlockSpec((1, width, cols), lambda j, off: (2, 0, 0), pipeline_mode=pl.Buffered(1)), plane]
    args = [x2, o2, u2, vf, attn, wo_near, wo_far, w_far, dw_qk, *recv]
    return pl.pallas_call(
        functools.partial(far_y_body, early=early, copies=copies),
        grid_spec=pltpu.PrefetchScalarGridSpec(
            num_scalar_prefetch=1,
            grid=(steps,),
            in_specs=specs + [any_] * (len(recv) + 2),
            out_specs=[row(width), pl.BlockSpec((1, rows, width), lambda j, off: (off[1], jnp.minimum(j, sum(copies) - 1), 0)), plane],
            scratch_shapes=[pltpu.VMEM((rows, cols), BF16)] * 2 + [pltpu.SemaphoreType.DMA],
        ),
        out_shape=[sds(y2.shape, y2.dtype), sds(gx2.shape, gx2.dtype), sds((3, *dw_qk.shape[1:]), F32)],
        input_output_aliases={len(args) + 1: 0, len(args) + 2: 1},
        name="far_y",
        compiler_params=params(),
        cost_estimate=cost(2 * half * width * cols * 2.8, 2 * half * (4 * width + 3 * cols)),
    )(off, *args, y2, gx2)


def token_sum_body(l_ref, r_ref, o_ref):
    first = pl.program_id(0) == 0
    for e in range(r_ref.shape[0]):
        val = dot(l_ref[...], r_ref[e], TN)
        o_ref[e] = jnp.where(first, val, o_ref[e] + val)


def token_sum(lhs, rhs):
    planes, tokens, cols = rhs.shape
    width = lhs.shape[1]
    return pl.pallas_call(
        token_sum_body,
        grid=(tokens // SUM_ROWS,),
        in_specs=[row_spec(SUM_ROWS, width, lambda i: i), pl.BlockSpec((planes, SUM_ROWS, cols), lambda i: (0, i, 0))],
        out_specs=pl.BlockSpec((planes, width, cols), lambda i: (0, 0, 0)),
        out_shape=sds((planes, width, cols), F32),
        name="token_sum",
        compiler_params=params(),
        cost_estimate=cost(2 * planes * tokens * width * cols, 2 * tokens * (width + planes * cols)),
    )(lhs, rhs)


def solution(mesh):
    tp_size = mesh.shape["tp"]
    sp_size = mesh.shape["sp"]
    in_rows = P(("dp", "sp"), None)
    swap = [(0, 1), (1, 0)]

    def exchange(t):
        return lax.ppermute(t, "tp", swap)

    def step(x, g, w_qkv, w_out, ln_gamma, ln_beta, temps):
        tokens, width = x.shape
        cols = w_qkv.shape[2]
        groups = cols // GROUP
        me = lax.axis_index("tp")
        w_near = jnp.transpose(w_qkv, (1, 0, 2))
        w_far = exchange(w_near)
        wo_far = exchange(w_out)
        half = tokens // 2
        off = jnp.stack([me, 1 - me]).astype(jnp.int32)
        halves = lambda t: t.reshape(2, half, t.shape[-1])

        u, q, k, v, do, stats, part = project(x, g, w_near, w_out, ln_gamma, ln_beta)
        x2, g2, u2, stats2 = halves(x), halves(g), halves(u), halves(stats)
        near = tuple(halves(t) for t in (q, k, v, do))
        peers = [lax.ppermute(part, "sp", [(s, s ^ d) for s in range(sp_size)]) for d in (1, 2, 3)]
        part = (part + peers[0]) + (peers[1] + peers[2])
        part_far = exchange(part)
        vf = far_v(off, u2, w_far, EARLY_V, 0, 2)
        vf = far_v(off, u2, w_far, EARLY_V, 1, 2, (vf,))
        tau = jnp.repeat(temps, HEAD).reshape(tp_size, groups, GROUP)
        tau = jnp.where(me == 0, tau, tau[::-1]).reshape(2 * groups, GROUP)
        attn, dgram, coef, dtau = head_state(part, part_far, tau)
        state = (attn, dgram, coef)

        prev, dsum, recv, start = (), None, [], 0
        for sizes in OWN_CHUNKS:
            out = rows_call(off, start, sizes, (x2, g2, u2, stats2) + near, state, (w_near, w_far, w_out, wo_far, ln_gamma), prev)
            prev, sent, ds = out[:5], out[5:-1], out[-1]
            recv += [exchange(t) for t in sent]
            dsum = ds if dsum is None else dsum + ds
            start += sum(sizes)
        y2, gx2, o2, rqk, rv = prev
        dtau, rqk = lax.optimization_barrier((dtau, rqk))
        dtau = jnp.sum(dtau[:2 * groups].reshape(tp_size, cols // HEAD, HEAD), axis=2)
        grad_temp = jnp.where(me == 0, dtau, dtau[::-1]).reshape(-1)

        dw_qk = token_sum(u, rqk.reshape(2, tokens, cols))
        o2, dw_qk = lax.optimization_barrier((o2, dw_qk))
        dw_qk = lax.psum_scatter(dw_qk, "sp", scatter_dimension=1, tiled=True)
        dw_o = token_sum(o2.reshape(tokens, cols), g[None])[0]
        rv, dw_o = lax.optimization_barrier((rv, dw_o))
        grad_wout = lax.psum_scatter(dw_o, "sp", scatter_dimension=0, tiled=True)
        dw_v = token_sum(u, rv.reshape(1, tokens, cols))
        y2, dw_v = lax.optimization_barrier((y2, dw_v))
        dw_v = lax.psum_scatter(dw_v, "sp", scatter_dimension=1, tiled=True)
        y2, gx2, gw = far_y(off, x2, o2, u2, vf, attn, w_out, wo_far, w_far, dw_qk, recv[:-1], y2, gx2)
        grad_wqkv = jnp.transpose(lax.dynamic_update_slice(gw, dw_v, (2, 0, 0)), (1, 0, 2))

        sums = jnp.sum(dsum, axis=1)
        for axis, perm in (("tp", swap), ("sp", [(s, s ^ 1) for s in range(sp_size)]), ("sp", [(s, s ^ 2) for s in range(sp_size)])):
            sums = sums + lax.ppermute(sums, axis, perm)
        gx2 = lax.dynamic_update_slice(gx2, recv[-1], (off[1], half - recv[-1].shape[1], 0))
        return y2.reshape(tokens, width), gx2.reshape(tokens, width), grad_wqkv, grad_wout, sums[0], sums[1], grad_temp

    in_specs = (in_rows, in_rows, P(None, None, "tp"), P("tp", None), P(None), P(None), P(None))
    out_specs = (in_rows, in_rows, P(("dp", "sp"), None, "tp"), P(("dp", "tp", "sp"), None), P("dp"), P("dp"), P("dp"))
    return jax.shard_map(step, mesh=mesh, in_specs=in_specs, out_specs=out_specs, check_vma=False)
```

```python
import functools

import jax
import jax.numpy as jnp
from jax import lax
from jax.experimental import pallas as pl
from jax.experimental.pallas import tpu as pltpu
from jax.sharding import PartitionSpec as P


LN_EPS = 1e-6
GROUP = 256
HEAD = 32
LANES = 128
F32 = jnp.float32
BF16 = jnp.bfloat16
NN = (((1,), (0,)), ((), ()))
NT = (((1,), (1,)), ((), ()))
TN = (((0,), (0,)), ((), ()))
PROJ_ROWS = 1024
ROWS = 256
LOAD_PIECES = 2
SUM_ROWS = 1024
OWN_CHUNKS = ((4,), (6,), (10,), (8, 4))
EARLY_V = 12


def dot(a, b, dims=NN):
    return lax.dot_general(a, b, dims, preferred_element_type=F32)


def normalize(x):
    mean = jnp.mean(x, axis=-1, keepdims=True)
    cen = x - mean
    inv = lax.rsqrt(jnp.mean(cen * cen, axis=-1, keepdims=True) + LN_EPS)
    return cen * inv, mean, inv


def row_spec(rows, cols, index):
    return pl.BlockSpec((rows, cols), lambda *a: (index(*a), 0))


def half_spec(rows, cols, which, start):
    return pl.BlockSpec((1, rows, cols), lambda j, off: (off[which], start + j, 0))


def both_spec(lead, rows, cols, start):
    zeros = (0,) * len(lead)
    return pl.BlockSpec((*lead, 2, rows, cols), lambda j, off: (*zeros, 0, start + j, 0))


def whole(shape):
    return pl.BlockSpec(shape, lambda *a: (0,) * len(shape), pipeline_mode=pl.Buffered(1))


def sds(shape, dtype):
    return jax.ShapeDtypeStruct(shape, dtype)


def params(**kw):
    return pltpu.CompilerParams(vmem_limit_bytes=64_000_000, **kw)


def cost(flops, nbytes):
    return pl.CostEstimate(flops=int(flops), bytes_accessed=int(nbytes), transcendentals=0)


def project_body(x_ref, g_ref, w_ref, wo_ref, gm_ref, bt_ref, u_ref, q_ref, k_ref, v_ref, do_ref, st_ref, part_ref, gr, da, qs, ks):
    i = pl.program_id(0)
    rows, cols = q_ref.shape
    groups = cols // GROUP
    do_ref[...] = dot(g_ref[...], wo_ref[...], NT).astype(BF16)
    xh, mean, inv = normalize(x_ref[...].astype(F32))
    u_ref[...] = (xh * gm_ref[...].reshape(1, -1) + bt_ref[...].reshape(1, -1)).astype(BF16)
    st_ref[...] = jnp.where(lax.broadcasted_iota(jnp.int32, st_ref.shape, 1) < LANES // 2, mean, inv)
    u = u_ref[...]
    for e, out in enumerate((q_ref, k_ref, v_ref)):
        out[...] = dot(u, w_ref[e]).astype(BF16)

    def add(acc, s, val):
        acc[s] = jnp.where(i == 0, val, acc[s] + val)

    for s in range(groups):
        c = slice(s * GROUP, (s + 1) * GROUP)
        add(gr, s, dot(q_ref[:, c], k_ref[:, c], TN))
        add(da, s, dot(do_ref[:, c], v_ref[:, c], TN))
    for acc, t in ((qs, q_ref), (ks, k_ref)):
        f = t[...].astype(F32)
        val = jnp.sum((f * f).reshape(rows // 8, 8, cols), axis=0)
        acc[...] = jnp.where(i == 0, val, acc[...] + val)

    @pl.when(i == pl.num_programs(0) - 1)
    def _():
        col_head = lax.broadcasted_iota(jnp.int32, (HEAD, GROUP), 1) // HEAD
        for a, acc in enumerate((gr, da)):
            for s in range(groups):
                tot = jnp.zeros((HEAD, GROUP), F32)
                for h in range(GROUP // HEAD):
                    tot += jnp.where(col_head == h, acc[s, h * HEAD:(h + 1) * HEAD, :], 0.0)
                part_ref[(a * groups + s) * HEAD:(a * groups + s + 1) * HEAD, :] = tot
        base = 2 * groups * HEAD
        for a, acc in enumerate((qs, ks)):
            tot = jnp.sum(acc[...], axis=0, keepdims=True)
            for s in range(groups):
                part_ref[base + 8 * (a * groups + s):base + 8 * (a * groups + s + 1), :] = jnp.broadcast_to(
                    tot[:, s * GROUP:(s + 1) * GROUP], (8, GROUP))


def project(x, g, w3, wo, gamma, beta):
    tokens, width = x.shape
    cols = wo.shape[0]
    groups = cols // GROUP
    part_rows = 2 * groups * (HEAD + 8)
    row = lambda c: row_spec(PROJ_ROWS, c, lambda i: i)
    return pl.pallas_call(
        project_body,
        grid=(tokens // PROJ_ROWS,),
        in_specs=[row(width), row(width), whole(w3.shape), whole(wo.shape), whole(gamma.shape), whole(beta.shape)],
        out_specs=[row(width)] + [row(cols)] * 4 + [row(LANES), pl.BlockSpec((part_rows, GROUP), lambda i: (0, 0))],
        out_shape=[sds((tokens, width), BF16)] + [sds((tokens, cols), BF16)] * 4 + [sds((tokens, LANES), F32), sds((part_rows, GROUP), F32)],
        scratch_shapes=[pltpu.VMEM((groups, GROUP, GROUP), F32)] * 2 + [pltpu.VMEM((8, cols), F32)] * 2,
        name="project",
        compiler_params=params(),
        cost_estimate=cost(2 * tokens * width * cols * 4.4, 2 * tokens * (3 * width + 4 * cols)),
    )(x, g, w3, wo, gamma, beta)


def far_v_body(off_ref, u_ref, w_ref, *refs):
    refs[-1][...] = dot(u_ref[0], w_ref[0]).astype(BF16)


def far_v(off, u2, w3, blocks, part, parts, prev=()):
    width, cols = w3.shape[1:]
    rows = 2 * ROWS
    steps = blocks * ROWS // rows // parts
    return pl.pallas_call(
        far_v_body,
        grid_spec=pltpu.PrefetchScalarGridSpec(
            num_scalar_prefetch=1,
            grid=(steps,),
            in_specs=[half_spec(rows, width, 1, part * steps),
                      pl.BlockSpec((1, width, cols), lambda j, off: (2, 0, 0), pipeline_mode=pl.Buffered(1))]
            + [pl.BlockSpec(memory_space=pl.ANY)] * len(prev),
            out_specs=pl.BlockSpec((rows, cols), lambda j, off: (part * steps + j, 0)),
        ),
        out_shape=sds((blocks * ROWS, cols), BF16),
        input_output_aliases={3: 0} if prev else {},
        name="far_v",
        compiler_params=params(),
        cost_estimate=cost(2 * steps * rows * width * cols, 2 * steps * rows * (width + cols)),
    )(off, u2, w3, *prev)


def state_body(near_ref, far_ref, tau_ref, attn_ref, dgram_ref, coef_ref, dtau_ref, *, groups):
    r_head = lax.broadcasted_iota(jnp.int32, (GROUP, GROUP), 0)
    c_head = lax.broadcasted_iota(jnp.int32, (GROUP, GROUP), 1)
    eye = r_head == c_head
    mask = (r_head // HEAD) == (c_head // HEAD)
    spread = lambda t: jnp.concatenate([t] * (GROUP // HEAD), axis=0)
    to_col = lambda t: jnp.sum(jnp.where(eye, t, 0.0), axis=1, keepdims=True)
    to_row = lambda t: jnp.sum(jnp.where(eye, t, 0.0), axis=0, keepdims=True)
    base = 2 * groups * HEAD
    coef_ref[...] = jnp.zeros_like(coef_ref)
    dtau_ref[...] = jnp.zeros_like(dtau_ref)
    for side, ref in enumerate((near_ref, far_ref)):
        for s in range(groups):
            gram_mat = spread(ref[s * HEAD:(s + 1) * HEAD, :])
            d_attn = spread(ref[(groups + s) * HEAD:(groups + s + 1) * HEAD, :])
            b_row = ref[base + 8 * (groups + s):base + 8 * (groups + s) + 1, :]
            a_col = to_col(ref[base + 8 * s:base + 8 * s + 1, :])
            g = side * groups + s
            tau = to_col(tau_ref[g:g + 1, :])
            norm_prod = jnp.sqrt(a_col) * jnp.sqrt(b_row)
            gram_n = gram_mat / norm_prod
            logit = jnp.where(mask, tau * gram_n, -jnp.inf)
            e = jnp.exp(logit - jnp.max(logit, axis=1, keepdims=True))
            attn = e / jnp.sum(e, axis=1, keepdims=True)
            d_attn = jnp.where(mask, d_attn, 0.0)
            d_logit = jnp.where(mask, attn * (d_attn - jnp.sum(attn * d_attn, axis=1, keepdims=True)), 0.0)
            gram_n = jnp.where(mask, gram_n, 0.0)
            grad_sn = tau * d_logit
            prod = grad_sn * gram_n
            attn_ref[g] = attn.astype(BF16)
            dgram_ref[g] = jnp.where(mask, grad_sn / norm_prod, 0.0).astype(BF16)
            coef_ref[2 * side:2 * side + 1, s * GROUP:(s + 1) * GROUP] = to_row(-jnp.sum(prod, axis=1, keepdims=True) / a_col)
            coef_ref[2 * side + 1:2 * side + 2, s * GROUP:(s + 1) * GROUP] = -jnp.sum(prod, axis=0, keepdims=True) / b_row
            dtau_ref[g:g + 1, :] = to_row(jnp.sum(d_logit * gram_n, axis=1, keepdims=True))


def head_state(near, far, tau_rows):
    groups = tau_rows.shape[0] // 2
    vm = pl.BlockSpec(memory_space=pltpu.VMEM)
    return pl.pallas_call(
        functools.partial(state_body, groups=groups),
        in_specs=[vm] * 3,
        out_specs=[vm] * 4,
        out_shape=[sds((2 * groups, GROUP, GROUP), BF16)] * 2 + [sds((8, groups * GROUP), F32), sds((8, GROUP), F32)],
        name="head_state",
        cost_estimate=cost(10**9, 2 * 10**6),
    )(near, far, tau_rows)


def mix_block(q, k, v, do, attn_ref, dgram_ref, coef_ref, side, s):
    groups = attn_ref.shape[0] // 2
    am, gm = attn_ref[side * groups + s], dgram_ref[side * groups + s]
    c = slice(s * GROUP, (s + 1) * GROUP)
    dq = dot(k, gm, NT) + q.astype(F32) * coef_ref[2 * side:2 * side + 1, c]
    dk = dot(q, gm, NN) + k.astype(F32) * coef_ref[2 * side + 1:2 * side + 2, c]
    return dot(v, am, NT).astype(BF16), dq.astype(BF16), dk.astype(BF16), dot(do, am, NN).astype(BF16)


def rows_body(*refs, n_alias, send_blocks):
    it = iter(refs)
    nxt = lambda n: [next(it) for _ in range(n)]
    off_ref, x_ref, g_ref, u_ref, st_ref, q_ref, k_ref, v_ref, do_ref = nxt(9)
    attn_ref, dgram_ref, coef_ref, gm_ref = nxt(4)
    w_hbm = nxt(4)
    nxt(n_alias)
    y_ref, gx_ref, o_ref, rqk_ref, rv_ref = nxt(5)
    send_refs = nxt(len(send_blocks))
    (dsum_ref,) = nxt(1)
    on_s, rn_s, of_s, rf_s, qf_s, kf_s, vf_s, dof_s, gh_s = nxt(9)
    w_refs, w_sems = nxt(4), nxt(1)[0]
    wf_ref, wof_ref, wn_ref, won_ref = w_refs
    j = pl.program_id(0)
    own, other = off_ref[0], off_ref[1]
    groups = attn_ref.shape[0] // 2
    state = (attn_ref, dgram_ref, coef_ref)
    waits = [pltpu.make_async_copy(src, dst, w_sems.at[n]) for n, (src, dst) in enumerate(zip(w_hbm, w_refs))]

    def start_loads():
        for n, (src, dst) in enumerate(zip(w_hbm, w_refs)):
            pieces = [(e,) for e in range(src.shape[0])] if len(src.shape) == 3 else [()]
            size = src.shape[-2] // LOAD_PIECES
            for p in pieces:
                for r in range(0, src.shape[-2], size):
                    at = (*p, pl.ds(r, size))
                    pltpu.make_async_copy(src.at[at], dst.at[at], w_sems.at[n]).start()

    def compute(wait, first):
        for s in range(groups):
            c = slice(s * GROUP, (s + 1) * GROUP)
            for half in (own, other):
                o, dq, dk, dv = mix_block(q_ref[half, :, c], k_ref[half, :, c], v_ref[half, :, c], do_ref[half, :, c], *state, 0, s)
                o_ref[half, :, c], rqk_ref[0, half, :, c], rqk_ref[1, half, :, c], rv_ref[half, :, c] = o, dq, dk, dv
                if half is own:
                    on_s[:, c], rn_s[0, :, c], rn_s[1, :, c], rn_s[2, :, c] = o, dq, dk, dv
        wait(0)
        wait(1)
        u = u_ref[0]
        for e, t in enumerate((qf_s, kf_s, vf_s)):
            t[...] = dot(u, wf_ref[e]).astype(BF16)
        dof_s[...] = dot(g_ref[0], wof_ref[...], NT).astype(BF16)
        for s in range(groups):
            c = slice(s * GROUP, (s + 1) * GROUP)
            of_s[:, c], rf_s[0, :, c], rf_s[1, :, c], rf_s[2, :, c] = mix_block(
                qf_s[:, c], kf_s[:, c], vf_s[:, c], dof_s[:, c], *state, 1, s)
        wait(2)
        wait(3)
        rows, width = gh_s.shape
        mean, inv = st_ref[0, :, :1], st_ref[0, :, LANES // 2:LANES // 2 + 1]
        fold = lambda t: jnp.sum(t.reshape(rows // 8, 8, GROUP), axis=0)
        lanes = lambda t: sum(t[:, k:k + LANES] for k in range(0, GROUP, LANES))
        gamma = gm_ref[...].reshape(1, width)
        tiles = [slice(n, n + GROUP) for n in range(0, width, GROUP)]
        s1 = s2 = 0.0
        for c in tiles:
            du = dot(rn_s[0], wn_ref[0, c, :], NT)
            for e in range(1, 3):
                du += dot(rn_s[e], wn_ref[e, c, :], NT)
            for e in range(3):
                du += dot(rf_s[e], wf_ref[e, c, :], NT)
            xh = (x_ref[0, :, c].astype(F32) - mean) * inv
            for a, val in enumerate((fold(du * xh), fold(du))):
                dsum_ref[a, :, c] = val if first else dsum_ref[a, :, c] + val
            gh = du * gamma[:, c]
            s1 += lanes(gh)
            s2 += lanes(gh * xh)
            gh_s[:, c] = gh
        m1 = jnp.sum(s1, axis=1, keepdims=True) / width
        m2 = jnp.sum(s2, axis=1, keepdims=True) / width
        for c in tiles:
            x = x_ref[0, :, c].astype(F32)
            yp = dot(on_s[...], won_ref[:, c]) + dot(of_s[...], wof_ref[:, c])
            y_ref[0, :, c] = (x + yp).astype(BF16)
            dx = g_ref[0, :, c].astype(F32) + inv * (gh_s[:, c] - m1 - (x - mean) * inv * m2)
            for ref in [gx_ref] + send_refs[:1] * (len(send_refs) == 1):
                ref[0, :, c] = dx.astype(BF16)

    @pl.when(j == 0)
    def _():
        start_loads()
        compute(lambda n: waits[n].wait(), True)

    @pl.when(j > 0)
    def _():
        compute(lambda n: None, False)

    if len(send_refs) > 1:
        start = 0
        for ref, n in zip(send_refs, send_blocks):

            @pl.when((j >= start) & (j < start + n))
            def _(ref=ref):
                ref[0] = gx_ref[0]

            start += n


def rows_call(off, start, send_blocks, acts, state, weights, prev):
    _, half, width = acts[0].shape
    blocks = sum(send_blocks)
    firsts = [sum(send_blocks[:n]) for n in range(len(send_blocks))]
    send_spec = lambda first, n: pl.BlockSpec((1, ROWS, width), lambda j, off: (0, jnp.clip(j - first, 0, n - 1), 0))
    cols = weights[2].shape[0]
    row = half_spec(ROWS, width, 0, start)
    both = lambda *lead: both_spec(lead, ROWS, cols, start)
    w_near, w_far, wo_near, wo_far, gamma = weights
    consts = list(state) + [gamma]
    loaded = [w_far, wo_far, w_near, wo_near]
    first = 1 + len(acts) + len(consts) + len(loaded)
    return pl.pallas_call(
        functools.partial(rows_body, n_alias=len(prev), send_blocks=send_blocks),
        grid_spec=pltpu.PrefetchScalarGridSpec(
            num_scalar_prefetch=1,
            grid=(blocks,),
            in_specs=[row] * 3 + [half_spec(ROWS, LANES, 0, start)] + [both()] * 4 + [whole(t.shape) for t in consts] + [pl.BlockSpec(memory_space=pl.ANY)] * (len(loaded) + len(prev)),
            out_specs=[row, row, both(), both(2), both(),
                       *[send_spec(first, n) for first, n in zip(firsts, send_blocks)],
                       pl.BlockSpec((2, 8, width), lambda j, off: (0, 0, 0))],
            scratch_shapes=[pltpu.VMEM((ROWS, cols), BF16), pltpu.VMEM((3, ROWS, cols), BF16)] * 2 + [pltpu.VMEM((ROWS, cols), BF16)] * 4
            + [pltpu.VMEM((ROWS, width), F32)] + [pltpu.VMEM(t.shape, t.dtype) for t in loaded] + [pltpu.SemaphoreType.DMA((len(loaded),))],
        ),
        out_shape=[sds((2, half, width), BF16)] * 2 + [sds((2, half, cols), BF16), sds((2, 2, half, cols), BF16), sds((2, half, cols), BF16),
                                                       *[sds((1, n * ROWS, width), BF16) for n in send_blocks], sds((2, 8, width), F32)],
        input_output_aliases={first + a: a for a in range(len(prev))},
        name="rows",
        compiler_params=params(),
        cost_estimate=cost(2 * blocks * ROWS * width * cols * 13, 2 * blocks * ROWS * (6 * width + 16 * cols)),
    )(off, *acts, *consts, *loaded, *prev)


def far_y_body(*refs, early, copies):
    it = iter(refs)
    nxt = lambda n: [next(it) for _ in range(n)]
    _, x_ref, o_ref, u_ref, v_ref, attn_ref, won_ref, wof_ref, wv_ref, qk_ref = nxt(10)
    recv = nxt(len(copies))
    _, _, y_ref, gx_ref, gw_ref, vf_s, of_s, sem = nxt(8)
    j = pl.program_id(0)
    rows = gx_ref.shape[1]

    def file_rows(act):
        start = 0
        for ref, n in zip(recv, copies):

            @pl.when((j >= start) & (j < start + n))
            def _(ref=ref, start=start):
                act(pltpu.make_async_copy(ref.at[0, pl.ds((j - start) * rows, rows)], gx_ref.at[0], sem))

            start += n

    file_rows(lambda copy: copy.start())
    gw_ref[...] = qk_ref[...]

    @pl.when(j < early)
    def _():
        vf_s[...] = v_ref[...]

    @pl.when(j >= early)
    def _():
        vf_s[...] = dot(u_ref[0], wv_ref[0]).astype(BF16)

    groups = attn_ref.shape[0] // 2
    for s in range(groups):
        c = slice(s * GROUP, (s + 1) * GROUP)
        of_s[:, c] = dot(vf_s[:, c], attn_ref[groups + s], NT).astype(BF16)
    y_ref[0] = (x_ref[0].astype(F32) + (dot(o_ref[0], won_ref[...]) + dot(of_s[...], wof_ref[...]))).astype(BF16)
    file_rows(lambda copy: copy.wait())


def far_y(off, x2, o2, u2, vf, attn, wo_near, wo_far, w_far, dw_qk, recv, y2, gx2):
    half, width = x2.shape[1:]
    cols = o2.shape[2]
    rows = 2 * ROWS
    steps = half // rows
    early = vf.shape[0] // rows
    copies = [t.shape[1] // rows for t in recv]
    row = lambda c: half_spec(rows, c, 1, 0)
    per = steps // 2
    plane = pl.BlockSpec((1, dw_qk.shape[1] // per, cols), lambda j, off: (j // per, j % per, 0))
    any_ = pl.BlockSpec(memory_space=pl.ANY)
    specs = [row(width), row(cols),
             pl.BlockSpec((1, rows, width), lambda j, off: (off[1], jnp.maximum(j, early), 0)),
             pl.BlockSpec((rows, cols), lambda j, off: (jnp.minimum(j, early - 1), 0)),
             whole(attn.shape), whole(wo_near.shape), whole(wo_far.shape),
             pl.BlockSpec((1, width, cols), lambda j, off: (2, 0, 0), pipeline_mode=pl.Buffered(1)), plane]
    args = [x2, o2, u2, vf, attn, wo_near, wo_far, w_far, dw_qk, *recv]
    return pl.pallas_call(
        functools.partial(far_y_body, early=early, copies=copies),
        grid_spec=pltpu.PrefetchScalarGridSpec(
            num_scalar_prefetch=1,
            grid=(steps,),
            in_specs=specs + [any_] * (len(recv) + 2),
            out_specs=[row(width), pl.BlockSpec((1, rows, width), lambda j, off: (off[1], jnp.minimum(j, sum(copies) - 1), 0)), plane],
            scratch_shapes=[pltpu.VMEM((rows, cols), BF16)] * 2 + [pltpu.SemaphoreType.DMA],
        ),
        out_shape=[sds(y2.shape, y2.dtype), sds(gx2.shape, gx2.dtype), sds((3, *dw_qk.shape[1:]), F32)],
        input_output_aliases={len(args) + 1: 0, len(args) + 2: 1},
        name="far_y",
        compiler_params=params(),
        cost_estimate=cost(2 * half * width * cols * 2.8, 2 * half * (4 * width + 3 * cols)),
    )(off, *args, y2, gx2)


def token_sum_body(l_ref, r_ref, o_ref):
    first = pl.program_id(0) == 0
    for e in range(r_ref.shape[0]):
        val = dot(l_ref[...], r_ref[e], TN)
        o_ref[e] = jnp.where(first, val, o_ref[e] + val)


def token_sum(lhs, rhs):
    planes, tokens, cols = rhs.shape
    width = lhs.shape[1]
    return pl.pallas_call(
        token_sum_body,
        grid=(tokens // SUM_ROWS,),
        in_specs=[row_spec(SUM_ROWS, width, lambda i: i), pl.BlockSpec((planes, SUM_ROWS, cols), lambda i: (0, i, 0))],
        out_specs=pl.BlockSpec((planes, width, cols), lambda i: (0, 0, 0)),
        out_shape=sds((planes, width, cols), F32),
        name="token_sum",
        compiler_params=params(),
        cost_estimate=cost(2 * planes * tokens * width * cols, 2 * tokens * (width + planes * cols)),
    )(lhs, rhs)


def solution(mesh):
    tp_size = mesh.shape["tp"]
    sp_size = mesh.shape["sp"]
    in_rows = P(("dp", "sp"), None)
    swap = [(0, 1), (1, 0)]

    def exchange(t):
        return lax.ppermute(t, "tp", swap)

    def step(x, g, w_qkv, w_out, ln_gamma, ln_beta, temps):
        tokens, width = x.shape
        cols = w_qkv.shape[2]
        groups = cols // GROUP
        me = lax.axis_index("tp")
        w_near = jnp.transpose(w_qkv, (1, 0, 2))
        w_far = exchange(w_near)
        wo_far = exchange(w_out)
        half = tokens // 2
        off = jnp.stack([me, 1 - me]).astype(jnp.int32)
        halves = lambda t: t.reshape(2, half, t.shape[-1])

        u, q, k, v, do, stats, part = project(x, g, w_near, w_out, ln_gamma, ln_beta)
        x2, g2, u2, stats2 = halves(x), halves(g), halves(u), halves(stats)
        near = tuple(halves(t) for t in (q, k, v, do))
        peers = [lax.ppermute(part, "sp", [(s, s ^ d) for s in range(sp_size)]) for d in (1, 2, 3)]
        part = (part + peers[0]) + (peers[1] + peers[2])
        part_far = exchange(part)
        vf = far_v(off, u2, w_far, EARLY_V, 0, 2)
        vf = far_v(off, u2, w_far, EARLY_V, 1, 2, (vf,))
        tau = jnp.repeat(temps, HEAD).reshape(tp_size, groups, GROUP)
        tau = jnp.where(me == 0, tau, tau[::-1]).reshape(2 * groups, GROUP)
        attn, dgram, coef, dtau = head_state(part, part_far, tau)
        state = (attn, dgram, coef)

        prev, dsum, recv, start = (), None, [], 0
        for sizes in OWN_CHUNKS:
            out = rows_call(off, start, sizes, (x2, g2, u2, stats2) + near, state, (w_near, w_far, w_out, wo_far, ln_gamma), prev)
            prev, sent, ds = out[:5], out[5:-1], out[-1]
            recv += [exchange(t) for t in sent]
            dsum = ds if dsum is None else dsum + ds
            start += sum(sizes)
        y2, gx2, o2, rqk, rv = prev
        dtau, rqk = lax.optimization_barrier((dtau, rqk))
        dtau = jnp.sum(dtau[:2 * groups].reshape(tp_size, cols // HEAD, HEAD), axis=2)
        grad_temp = jnp.where(me == 0, dtau, dtau[::-1]).reshape(-1)

        dw_qk = token_sum(u, rqk.reshape(2, tokens, cols))
        o2, dw_qk = lax.optimization_barrier((o2, dw_qk))
        dw_qk = lax.psum_scatter(dw_qk, "sp", scatter_dimension=1, tiled=True)
        dw_o = token_sum(o2.reshape(tokens, cols), g[None])[0]
        rv, dw_o = lax.optimization_barrier((rv, dw_o))
        grad_wout = lax.psum_scatter(dw_o, "sp", scatter_dimension=0, tiled=True)
        dw_v = token_sum(u, rv.reshape(1, tokens, cols))
        y2, dw_v = lax.optimization_barrier((y2, dw_v))
        dw_v = lax.psum_scatter(dw_v, "sp", scatter_dimension=1, tiled=True)
        y2, gx2, gw = far_y(off, x2, o2, u2, vf, attn, w_out, wo_far, w_far, dw_qk, recv[:-1], y2, gx2)
        grad_wqkv = jnp.transpose(lax.dynamic_update_slice(gw, dw_v, (2, 0, 0)), (1, 0, 2))

        sums = jnp.sum(dsum, axis=1)
        for axis, perm in (("tp", swap), ("sp", [(s, s ^ 1) for s in range(sp_size)]), ("sp", [(s, s ^ 2) for s in range(sp_size)])):
            sums = sums + lax.ppermute(sums, axis, perm)
        gx2 = lax.dynamic_update_slice(gx2, recv[-1], (off[1], half - recv[-1].shape[1], 0))
        return y2.reshape(tokens, width), gx2.reshape(tokens, width), grad_wqkv, grad_wout, sums[0], sums[1], grad_temp

    in_specs = (in_rows, in_rows, P(None, None, "tp"), P("tp", None), P(None), P(None), P(None))
    out_specs = (in_rows, in_rows, P(("dp", "sp"), None, "tp"), P(("dp", "tp", "sp"), None), P("dp"), P("dp"), P("dp"))
    return jax.shard_map(step, mesh=mesh, in_specs=in_specs, out_specs=out_specs, check_vma=False)
```

```python
import functools

import jax
import jax.numpy as jnp
from jax import lax
from jax.experimental import pallas as pl
from jax.experimental.pallas import tpu as pltpu
from jax.sharding import PartitionSpec as P


LN_EPS = 1e-6
GROUP = 256
HEAD = 32
LANES = 128
F32 = jnp.float32
BF16 = jnp.bfloat16
NN = (((1,), (0,)), ((), ()))
NT = (((1,), (1,)), ((), ()))
TN = (((0,), (0,)), ((), ()))
PROJ_ROWS = 1024
ROWS = 256
ROWS_LIMIT = 38_000_000
HOLD_LIMIT = 36_000_000
SUM_ROWS = 1024
OWN_CHUNKS = ((4,), (6,), (10,), (8, 4))
EARLY_V = 12


def dot(a, b, dims=NN):
    return lax.dot_general(a, b, dims, preferred_element_type=F32)


def normalize(x):
    mean = jnp.mean(x, axis=-1, keepdims=True)
    cen = x - mean
    inv = lax.rsqrt(jnp.mean(cen * cen, axis=-1, keepdims=True) + LN_EPS)
    return cen * inv, mean, inv


def row_spec(rows, cols, index):
    return pl.BlockSpec((rows, cols), lambda *a: (index(*a), 0))


def half_spec(rows, cols, which, start):
    return pl.BlockSpec((1, rows, cols), lambda j, off: (off[which], start + j, 0))


def both_spec(lead, rows, cols, start):
    zeros = (0,) * len(lead)
    return pl.BlockSpec((*lead, 2, rows, cols), lambda j, off: (*zeros, 0, start + j, 0))


def whole(shape):
    return pl.BlockSpec(shape, lambda *a: (0,) * len(shape), pipeline_mode=pl.Buffered(1))


def sds(shape, dtype):
    return jax.ShapeDtypeStruct(shape, dtype)


def params(**kw):
    return pltpu.CompilerParams(vmem_limit_bytes=64_000_000, **kw)


def cost(flops, nbytes):
    return pl.CostEstimate(flops=int(flops), bytes_accessed=int(nbytes), transcendentals=0)


def project_body(x_ref, g_ref, w_ref, wo_ref, gm_ref, bt_ref, u_ref, q_ref, k_ref, v_ref, do_ref, st_ref, part_ref, gr, da, qs, ks):
    i = pl.program_id(0)
    rows, cols = q_ref.shape
    groups = cols // GROUP
    do_ref[...] = dot(g_ref[...], wo_ref[...], NT).astype(BF16)
    xh, mean, inv = normalize(x_ref[...].astype(F32))
    u_ref[...] = (xh * gm_ref[...].reshape(1, -1) + bt_ref[...].reshape(1, -1)).astype(BF16)
    st_ref[...] = jnp.where(lax.broadcasted_iota(jnp.int32, st_ref.shape, 1) < LANES // 2, mean, inv)
    u = u_ref[...]
    for e, out in enumerate((q_ref, k_ref, v_ref)):
        out[...] = dot(u, w_ref[e]).astype(BF16)

    def add(acc, s, val):
        acc[s] = jnp.where(i == 0, val, acc[s] + val)

    for s in range(groups):
        c = slice(s * GROUP, (s + 1) * GROUP)
        add(gr, s, dot(q_ref[:, c], k_ref[:, c], TN))
        add(da, s, dot(do_ref[:, c], v_ref[:, c], TN))
    for acc, t in ((qs, q_ref), (ks, k_ref)):
        f = t[...].astype(F32)
        val = jnp.sum((f * f).reshape(rows // 8, 8, cols), axis=0)
        acc[...] = jnp.where(i == 0, val, acc[...] + val)

    @pl.when(i == pl.num_programs(0) - 1)
    def _():
        col_head = lax.broadcasted_iota(jnp.int32, (HEAD, GROUP), 1) // HEAD
        for a, acc in enumerate((gr, da)):
            for s in range(groups):
                tot = jnp.zeros((HEAD, GROUP), F32)
                for h in range(GROUP // HEAD):
                    tot += jnp.where(col_head == h, acc[s, h * HEAD:(h + 1) * HEAD, :], 0.0)
                part_ref[(a * groups + s) * HEAD:(a * groups + s + 1) * HEAD, :] = tot
        base = 2 * groups * HEAD
        for a, acc in enumerate((qs, ks)):
            tot = jnp.sum(acc[...], axis=0, keepdims=True)
            for s in range(groups):
                part_ref[base + 8 * (a * groups + s):base + 8 * (a * groups + s + 1), :] = jnp.broadcast_to(
                    tot[:, s * GROUP:(s + 1) * GROUP], (8, GROUP))


def project(x, g, w3, wo, gamma, beta):
    tokens, width = x.shape
    cols = wo.shape[0]
    groups = cols // GROUP
    part_rows = 2 * groups * (HEAD + 8)
    row = lambda c: row_spec(PROJ_ROWS, c, lambda i: i)
    return pl.pallas_call(
        project_body,
        grid=(tokens // PROJ_ROWS,),
        in_specs=[row(width), row(width), whole(w3.shape), whole(wo.shape), whole(gamma.shape), whole(beta.shape)],
        out_specs=[row(width)] + [row(cols)] * 4 + [row(LANES), pl.BlockSpec((part_rows, GROUP), lambda i: (0, 0))],
        out_shape=[sds((tokens, width), BF16)] + [sds((tokens, cols), BF16)] * 4 + [sds((tokens, LANES), F32), sds((part_rows, GROUP), F32)],
        scratch_shapes=[pltpu.VMEM((groups, GROUP, GROUP), F32)] * 2 + [pltpu.VMEM((8, cols), F32)] * 2,
        name="project",
        compiler_params=params(),
        cost_estimate=cost(2 * tokens * width * cols * 4.4, 2 * tokens * (3 * width + 4 * cols)),
    )(x, g, w3, wo, gamma, beta)


def far_v_body(off_ref, u_ref, w_ref, *refs):
    refs[-1][...] = dot(u_ref[0], w_ref[0]).astype(BF16)


def far_v(off, u2, w3, blocks, part, parts, prev=()):
    width, cols = w3.shape[1:]
    rows = 2 * ROWS
    steps = blocks * ROWS // rows // parts
    return pl.pallas_call(
        far_v_body,
        grid_spec=pltpu.PrefetchScalarGridSpec(
            num_scalar_prefetch=1,
            grid=(steps,),
            in_specs=[half_spec(rows, width, 1, part * steps),
                      pl.BlockSpec((1, width, cols), lambda j, off: (2, 0, 0), pipeline_mode=pl.Buffered(1))]
            + [pl.BlockSpec(memory_space=pl.ANY)] * len(prev),
            out_specs=pl.BlockSpec((rows, cols), lambda j, off: (part * steps + j, 0)),
        ),
        out_shape=sds((blocks * ROWS, cols), BF16),
        input_output_aliases={3: 0} if prev else {},
        name="far_v",
        compiler_params=params(),
        cost_estimate=cost(2 * steps * rows * width * cols, 2 * steps * rows * (width + cols)),
    )(off, u2, w3, *prev)


def state_body(near_ref, far_ref, tau_ref, attn_ref, dgram_ref, coef_ref, dtau_ref, *, groups):
    r_head = lax.broadcasted_iota(jnp.int32, (GROUP, GROUP), 0)
    c_head = lax.broadcasted_iota(jnp.int32, (GROUP, GROUP), 1)
    eye = r_head == c_head
    mask = (r_head // HEAD) == (c_head // HEAD)
    spread = lambda t: jnp.concatenate([t] * (GROUP // HEAD), axis=0)
    to_col = lambda t: jnp.sum(jnp.where(eye, t, 0.0), axis=1, keepdims=True)
    to_row = lambda t: jnp.sum(jnp.where(eye, t, 0.0), axis=0, keepdims=True)
    base = 2 * groups * HEAD
    coef_ref[...] = jnp.zeros_like(coef_ref)
    dtau_ref[...] = jnp.zeros_like(dtau_ref)
    for side, ref in enumerate((near_ref, far_ref)):
        for s in range(groups):
            gram_mat = spread(ref[s * HEAD:(s + 1) * HEAD, :])
            d_attn = spread(ref[(groups + s) * HEAD:(groups + s + 1) * HEAD, :])
            b_row = ref[base + 8 * (groups + s):base + 8 * (groups + s) + 1, :]
            a_col = to_col(ref[base + 8 * s:base + 8 * s + 1, :])
            g = side * groups + s
            tau = to_col(tau_ref[g:g + 1, :])
            norm_prod = jnp.sqrt(a_col) * jnp.sqrt(b_row)
            gram_n = gram_mat / norm_prod
            logit = jnp.where(mask, tau * gram_n, -jnp.inf)
            e = jnp.exp(logit - jnp.max(logit, axis=1, keepdims=True))
            attn = e / jnp.sum(e, axis=1, keepdims=True)
            d_attn = jnp.where(mask, d_attn, 0.0)
            d_logit = jnp.where(mask, attn * (d_attn - jnp.sum(attn * d_attn, axis=1, keepdims=True)), 0.0)
            gram_n = jnp.where(mask, gram_n, 0.0)
            grad_sn = tau * d_logit
            prod = grad_sn * gram_n
            attn_ref[g] = attn.astype(BF16)
            dgram_ref[g] = jnp.where(mask, grad_sn / norm_prod, 0.0).astype(BF16)
            coef_ref[2 * side:2 * side + 1, s * GROUP:(s + 1) * GROUP] = to_row(-jnp.sum(prod, axis=1, keepdims=True) / a_col)
            coef_ref[2 * side + 1:2 * side + 2, s * GROUP:(s + 1) * GROUP] = -jnp.sum(prod, axis=0, keepdims=True) / b_row
            dtau_ref[g:g + 1, :] = to_row(jnp.sum(d_logit * gram_n, axis=1, keepdims=True))


def head_state(near, far, tau_rows):
    groups = tau_rows.shape[0] // 2
    vm = pl.BlockSpec(memory_space=pltpu.VMEM)
    return pl.pallas_call(
        functools.partial(state_body, groups=groups),
        in_specs=[vm] * 3,
        out_specs=[vm] * 4,
        out_shape=[sds((2 * groups, GROUP, GROUP), BF16)] * 2 + [sds((8, groups * GROUP), F32), sds((8, GROUP), F32)],
        name="head_state",
        cost_estimate=cost(10**9, 2 * 10**6),
    )(near, far, tau_rows)


def hold_body(*refs, planes):
    n = len(planes)
    srcs = [ref if e is None else ref.at[e] for ref, e in zip(refs[:n], planes)]
    copies = [pltpu.make_async_copy(srcs[k], refs[n + k], refs[-1].at[k]) for k in range(n)]
    for c in copies:
        c.start()
    for c in copies:
        c.wait()


def hold(*arrays):
    parts = [(t, e) for t in arrays for e in (range(t.shape[0]) if t.ndim == 3 else (None,))]
    return pl.pallas_call(
        functools.partial(hold_body, planes=[e for _, e in parts]),
        in_specs=[pl.BlockSpec(memory_space=pltpu.HBM)] * len(parts),
        out_specs=[pl.BlockSpec(memory_space=pltpu.VMEM)] * len(parts),
        out_shape=[sds(t.shape[-2:], t.dtype) for t, _ in parts],
        scratch_shapes=[pltpu.SemaphoreType.DMA((len(parts),))],
        name="hold",
        compiler_params=pltpu.CompilerParams(vmem_limit_bytes=HOLD_LIMIT),
        cost_estimate=cost(10**9, 4 * 10**7),
    )(*[t for t, _ in parts])


def mix_block(q, k, v, do, attn_ref, dgram_ref, coef_ref, side, s):
    groups = attn_ref.shape[0] // 2
    am, gm = attn_ref[side * groups + s], dgram_ref[side * groups + s]
    c = slice(s * GROUP, (s + 1) * GROUP)
    dq = dot(k, gm, NT) + q.astype(F32) * coef_ref[2 * side:2 * side + 1, c]
    dk = dot(q, gm, NN) + k.astype(F32) * coef_ref[2 * side + 1:2 * side + 2, c]
    return dot(v, am, NT).astype(BF16), dq.astype(BF16), dk.astype(BF16), dot(do, am, NN).astype(BF16)


def rows_body(*refs, n_alias, send_blocks):
    it = iter(refs)
    nxt = lambda n: [next(it) for _ in range(n)]
    off_ref, x_ref, g_ref, u_ref, st_ref, q_ref, k_ref, v_ref, do_ref = nxt(9)
    attn_ref, dgram_ref, coef_ref, gm_ref = nxt(4)
    wn_ref, wf_ref = nxt(3), nxt(3)
    won_ref, wof_ref = nxt(2)
    nxt(n_alias)
    y_ref, gx_ref, o_ref, rqk_ref, rv_ref = nxt(5)
    send_refs = nxt(len(send_blocks))
    (dsum_ref,) = nxt(1)
    on_s, rn_s, of_s, rf_s, qf_s, kf_s, vf_s, dof_s, gh_s = nxt(9)
    j = pl.program_id(0)
    own, other = off_ref[0], off_ref[1]
    groups = attn_ref.shape[0] // 2
    state = (attn_ref, dgram_ref, coef_ref)

    def compute(first):
        for s in range(groups):
            c = slice(s * GROUP, (s + 1) * GROUP)
            for half in (own, other):
                o, dq, dk, dv = mix_block(q_ref[half, :, c], k_ref[half, :, c], v_ref[half, :, c], do_ref[half, :, c], *state, 0, s)
                o_ref[half, :, c], rqk_ref[0, half, :, c], rqk_ref[1, half, :, c], rv_ref[half, :, c] = o, dq, dk, dv
                if half is own:
                    on_s[:, c], rn_s[0, :, c], rn_s[1, :, c], rn_s[2, :, c] = o, dq, dk, dv
        u = u_ref[0]
        for e, t in enumerate((qf_s, kf_s, vf_s)):
            t[...] = dot(u, wf_ref[e][...]).astype(BF16)
        dof_s[...] = dot(g_ref[0], wof_ref[...], NT).astype(BF16)
        for s in range(groups):
            c = slice(s * GROUP, (s + 1) * GROUP)
            of_s[:, c], rf_s[0, :, c], rf_s[1, :, c], rf_s[2, :, c] = mix_block(
                qf_s[:, c], kf_s[:, c], vf_s[:, c], dof_s[:, c], *state, 1, s)
        rows, width = gh_s.shape
        mean, inv = st_ref[0, :, :1], st_ref[0, :, LANES // 2:LANES // 2 + 1]
        fold = lambda t: jnp.sum(t.reshape(rows // 8, 8, GROUP), axis=0)
        lanes = lambda t: sum(t[:, k:k + LANES] for k in range(0, GROUP, LANES))
        gamma = gm_ref[...].reshape(1, width)
        tiles = [slice(n, n + GROUP) for n in range(0, width, GROUP)]
        s1 = s2 = 0.0
        for c in tiles:
            du = dot(rn_s[0], wn_ref[0][c, :], NT)
            for e in range(1, 3):
                du += dot(rn_s[e], wn_ref[e][c, :], NT)
            for e in range(3):
                du += dot(rf_s[e], wf_ref[e][c, :], NT)
            xh = (x_ref[0, :, c].astype(F32) - mean) * inv
            for a, val in enumerate((fold(du * xh), fold(du))):
                dsum_ref[a, :, c] = jnp.where(first, val, dsum_ref[a, :, c] + val)
            gh = du * gamma[:, c]
            s1 += lanes(gh)
            s2 += lanes(gh * xh)
            gh_s[:, c] = gh
        m1 = jnp.sum(s1, axis=1, keepdims=True) / width
        m2 = jnp.sum(s2, axis=1, keepdims=True) / width
        for c in tiles:
            x = x_ref[0, :, c].astype(F32)
            yp = dot(on_s[...], won_ref[:, c]) + dot(of_s[...], wof_ref[:, c])
            y_ref[0, :, c] = (x + yp).astype(BF16)
            dx = g_ref[0, :, c].astype(F32) + inv * (gh_s[:, c] - m1 - (x - mean) * inv * m2)
            for ref in [gx_ref] + send_refs[:1] * (len(send_refs) == 1):
                ref[0, :, c] = dx.astype(BF16)

    compute(j == 0)

    if len(send_refs) > 1:
        start = 0
        for ref, n in zip(send_refs, send_blocks):

            @pl.when((j >= start) & (j < start + n))
            def _(ref=ref):
                ref[0] = gx_ref[0]

            start += n


def rows_call(off, start, send_blocks, acts, state, weights, prev):
    _, half, width = acts[0].shape
    blocks = sum(send_blocks)
    firsts = [sum(send_blocks[:n]) for n in range(len(send_blocks))]
    send_spec = lambda first, n: pl.BlockSpec((1, ROWS, width), lambda j, off: (0, jnp.clip(j - first, 0, n - 1), 0))
    cols = acts[4].shape[2]
    row = half_spec(ROWS, width, 0, start)
    both = lambda *lead: both_spec(lead, ROWS, cols, start)
    *loaded, gamma = weights
    consts = list(state) + [gamma]
    first = 1 + len(acts) + len(consts) + len(loaded)
    return pl.pallas_call(
        functools.partial(rows_body, n_alias=len(prev), send_blocks=send_blocks),
        grid_spec=pltpu.PrefetchScalarGridSpec(
            num_scalar_prefetch=1,
            grid=(blocks,),
            in_specs=[row] * 3 + [half_spec(ROWS, LANES, 0, start)] + [both()] * 4 + [whole(t.shape) for t in consts] + [pl.BlockSpec(memory_space=pltpu.VMEM)] * len(loaded) + [pl.BlockSpec(memory_space=pl.ANY)] * len(prev),
            out_specs=[row, row, both(), both(2), both(),
                       *[send_spec(first, n) for first, n in zip(firsts, send_blocks)],
                       pl.BlockSpec((2, 8, width), lambda j, off: (0, 0, 0))],
            scratch_shapes=[pltpu.VMEM((ROWS, cols), BF16), pltpu.VMEM((3, ROWS, cols), BF16)] * 2 + [pltpu.VMEM((ROWS, cols), BF16)] * 4
            + [pltpu.VMEM((ROWS, width), F32)],
        ),
        out_shape=[sds((2, half, width), BF16)] * 2 + [sds((2, half, cols), BF16), sds((2, 2, half, cols), BF16), sds((2, half, cols), BF16),
                                                       *[sds((1, n * ROWS, width), BF16) for n in send_blocks], sds((2, 8, width), F32)],
        input_output_aliases={first + a: a for a in range(len(prev))},
        name="rows",
        compiler_params=pltpu.CompilerParams(vmem_limit_bytes=ROWS_LIMIT),
        cost_estimate=cost(2 * blocks * ROWS * width * cols * 13, 2 * blocks * ROWS * (6 * width + 16 * cols)),
    )(off, *acts, *consts, *loaded, *prev)


def far_y_body(*refs, early, copies):
    it = iter(refs)
    nxt = lambda n: [next(it) for _ in range(n)]
    _, x_ref, o_ref, u_ref, v_ref, attn_ref, won_ref, wof_ref, wv_ref, qk_ref = nxt(10)
    recv = nxt(len(copies))
    _, _, y_ref, gx_ref, gw_ref, vf_s, of_s, sem = nxt(8)
    j = pl.program_id(0)
    rows = gx_ref.shape[1]

    def file_rows(act):
        start = 0
        for ref, n in zip(recv, copies):

            @pl.when((j >= start) & (j < start + n))
            def _(ref=ref, start=start):
                act(pltpu.make_async_copy(ref.at[0, pl.ds((j - start) * rows, rows)], gx_ref.at[0], sem))

            start += n

    file_rows(lambda copy: copy.start())
    gw_ref[...] = qk_ref[...]

    @pl.when(j < early)
    def _():
        vf_s[...] = v_ref[...]

    @pl.when(j >= early)
    def _():
        vf_s[...] = dot(u_ref[0], wv_ref[0]).astype(BF16)

    groups = attn_ref.shape[0] // 2
    for s in range(groups):
        c = slice(s * GROUP, (s + 1) * GROUP)
        of_s[:, c] = dot(vf_s[:, c], attn_ref[groups + s], NT).astype(BF16)
    y_ref[0] = (x_ref[0].astype(F32) + (dot(o_ref[0], won_ref[...]) + dot(of_s[...], wof_ref[...]))).astype(BF16)
    file_rows(lambda copy: copy.wait())


def far_y(off, x2, o2, u2, vf, attn, wo_near, wo_far, w_far, dw_qk, recv, y2, gx2):
    half, width = x2.shape[1:]
    cols = o2.shape[2]
    rows = 2 * ROWS
    steps = half // rows
    early = vf.shape[0] // rows
    copies = [t.shape[1] // rows for t in recv]
    row = lambda c: half_spec(rows, c, 1, 0)
    per = steps // 2
    plane = pl.BlockSpec((1, dw_qk.shape[1] // per, cols), lambda j, off: (j // per, j % per, 0))
    any_ = pl.BlockSpec(memory_space=pl.ANY)
    specs = [row(width), row(cols),
             pl.BlockSpec((1, rows, width), lambda j, off: (off[1], jnp.maximum(j, early), 0)),
             pl.BlockSpec((rows, cols), lambda j, off: (jnp.minimum(j, early - 1), 0)),
             whole(attn.shape), whole(wo_near.shape), whole(wo_far.shape),
             pl.BlockSpec((1, width, cols), lambda j, off: (2, 0, 0), pipeline_mode=pl.Buffered(1)), plane]
    args = [x2, o2, u2, vf, attn, wo_near, wo_far, w_far, dw_qk, *recv]
    return pl.pallas_call(
        functools.partial(far_y_body, early=early, copies=copies),
        grid_spec=pltpu.PrefetchScalarGridSpec(
            num_scalar_prefetch=1,
            grid=(steps,),
            in_specs=specs + [any_] * (len(recv) + 2),
            out_specs=[row(width), pl.BlockSpec((1, rows, width), lambda j, off: (off[1], jnp.minimum(j, sum(copies) - 1), 0)), plane],
            scratch_shapes=[pltpu.VMEM((rows, cols), BF16)] * 2 + [pltpu.SemaphoreType.DMA],
        ),
        out_shape=[sds(y2.shape, y2.dtype), sds(gx2.shape, gx2.dtype), sds((3, *dw_qk.shape[1:]), F32)],
        input_output_aliases={len(args) + 1: 0, len(args) + 2: 1},
        name="far_y",
        compiler_params=params(),
        cost_estimate=cost(2 * half * width * cols * 2.8, 2 * half * (4 * width + 3 * cols)),
    )(off, *args, y2, gx2)


def token_sum_body(l_ref, r_ref, o_ref):
    first = pl.program_id(0) == 0
    for e in range(r_ref.shape[0]):
        val = dot(l_ref[...], r_ref[e], TN)
        o_ref[e] = jnp.where(first, val, o_ref[e] + val)


def token_sum(lhs, rhs):
    planes, tokens, cols = rhs.shape
    width = lhs.shape[1]
    return pl.pallas_call(
        token_sum_body,
        grid=(tokens // SUM_ROWS,),
        in_specs=[row_spec(SUM_ROWS, width, lambda i: i), pl.BlockSpec((planes, SUM_ROWS, cols), lambda i: (0, i, 0))],
        out_specs=pl.BlockSpec((planes, width, cols), lambda i: (0, 0, 0)),
        out_shape=sds((planes, width, cols), F32),
        name="token_sum",
        compiler_params=params(),
        cost_estimate=cost(2 * planes * tokens * width * cols, 2 * tokens * (width + planes * cols)),
    )(lhs, rhs)


def solution(mesh):
    tp_size = mesh.shape["tp"]
    sp_size = mesh.shape["sp"]
    in_rows = P(("dp", "sp"), None)
    swap = [(0, 1), (1, 0)]

    def exchange(t):
        return lax.ppermute(t, "tp", swap)

    def step(x, g, w_qkv, w_out, ln_gamma, ln_beta, temps):
        tokens, width = x.shape
        cols = w_qkv.shape[2]
        groups = cols // GROUP
        me = lax.axis_index("tp")
        w_near = jnp.transpose(w_qkv, (1, 0, 2))
        w_far = exchange(w_near)
        wo_far = exchange(w_out)
        half = tokens // 2
        off = jnp.stack([me, 1 - me]).astype(jnp.int32)
        halves = lambda t: t.reshape(2, half, t.shape[-1])

        u, q, k, v, do, stats, part = project(x, g, w_near, w_out, ln_gamma, ln_beta)
        x2, g2, u2, stats2 = halves(x), halves(g), halves(u), halves(stats)
        near = tuple(halves(t) for t in (q, k, v, do))
        peers = [lax.ppermute(part, "sp", [(s, s ^ d) for s in range(sp_size)]) for d in (1, 2, 3)]
        part = (part + peers[0]) + (peers[1] + peers[2])
        part_far = exchange(part)
        vf = far_v(off, u2, w_far, EARLY_V, 0, 2)
        vf = far_v(off, u2, w_far, EARLY_V, 1, 2, (vf,))
        tau = jnp.repeat(temps, HEAD).reshape(tp_size, groups, GROUP)
        tau = jnp.where(me == 0, tau, tau[::-1]).reshape(2 * groups, GROUP)
        attn, dgram, coef, dtau = head_state(part, part_far, tau)
        state = (attn, dgram, coef)

        prev, dsum, recv, start = (), None, [], 0
        attn, wn_, wf_ = lax.optimization_barrier((attn, w_near, w_far))
        state = (attn, dgram, coef)
        held = (*hold(wn_, wf_), w_out, wo_far)
        for sizes in OWN_CHUNKS:
            out = rows_call(off, start, sizes, (x2, g2, u2, stats2) + near, state, (*held, ln_gamma), prev)
            prev, sent, ds = out[:5], out[5:-1], out[-1]
            recv += [exchange(t) for t in sent]
            dsum = ds if dsum is None else dsum + ds
            start += sum(sizes)
        y2, gx2, o2, rqk, rv = prev
        dtau, rqk = lax.optimization_barrier((dtau, rqk))
        dtau = jnp.sum(dtau[:2 * groups].reshape(tp_size, cols // HEAD, HEAD), axis=2)
        grad_temp = jnp.where(me == 0, dtau, dtau[::-1]).reshape(-1)

        dw_qk = token_sum(u, rqk.reshape(2, tokens, cols))
        o2, dw_qk = lax.optimization_barrier((o2, dw_qk))
        dw_qk = lax.psum_scatter(dw_qk, "sp", scatter_dimension=1, tiled=True)
        dw_o = token_sum(o2.reshape(tokens, cols), g[None])[0]
        rv, dw_o = lax.optimization_barrier((rv, dw_o))
        grad_wout = lax.psum_scatter(dw_o, "sp", scatter_dimension=0, tiled=True)
        dw_v = token_sum(u, rv.reshape(1, tokens, cols))
        y2, dw_v = lax.optimization_barrier((y2, dw_v))
        dw_v = lax.psum_scatter(dw_v, "sp", scatter_dimension=1, tiled=True)
        y2, gx2, gw = far_y(off, x2, o2, u2, vf, attn, w_out, wo_far, w_far, dw_qk, recv[:-1], y2, gx2)
        grad_wqkv = jnp.transpose(lax.dynamic_update_slice(gw, dw_v, (2, 0, 0)), (1, 0, 2))

        sums = jnp.sum(dsum, axis=1)
        for axis, perm in (("tp", swap), ("sp", [(s, s ^ 1) for s in range(sp_size)]), ("sp", [(s, s ^ 2) for s in range(sp_size)])):
            sums = sums + lax.ppermute(sums, axis, perm)
        gx2 = lax.dynamic_update_slice(gx2, recv[-1], (off[1], half - recv[-1].shape[1], 0))
        return y2.reshape(tokens, width), gx2.reshape(tokens, width), grad_wqkv, grad_wout, sums[0], sums[1], grad_temp

    in_specs = (in_rows, in_rows, P(None, None, "tp"), P("tp", None), P(None), P(None), P(None))
    out_specs = (in_rows, in_rows, P(("dp", "sp"), None, "tp"), P(("dp", "tp", "sp"), None), P("dp"), P("dp"), P("dp"))
    return jax.shard_map(step, mesh=mesh, in_specs=in_specs, out_specs=out_specs, check_vma=False)
```

```python
import functools

import jax
import jax.numpy as jnp
from jax import lax
from jax.experimental import pallas as pl
from jax.experimental.pallas import tpu as pltpu
from jax.sharding import PartitionSpec as P


LN_EPS = 1e-6
GROUP = 256
HEAD = 32
LANES = 128
F32 = jnp.float32
BF16 = jnp.bfloat16
NN = (((1,), (0,)), ((), ()))
NT = (((1,), (1,)), ((), ()))
TN = (((0,), (0,)), ((), ()))
PROJ_ROWS = 1024
ROWS = 256
STATE_LIMIT = 16_000_000
ROWS_LIMIT = 38_000_000
HOLD_LIMIT = 36_000_000
SUM_ROWS = 1024
OWN_CHUNKS = ((4,), (6,), (10,), (8, 4))
EARLY_V = 6


def dot(a, b, dims=NN):
    return lax.dot_general(a, b, dims, preferred_element_type=F32)


def normalize(x):
    mean = jnp.mean(x, axis=-1, keepdims=True)
    cen = x - mean
    inv = lax.rsqrt(jnp.mean(cen * cen, axis=-1, keepdims=True) + LN_EPS)
    return cen * inv, mean, inv


def row_spec(rows, cols, index):
    return pl.BlockSpec((rows, cols), lambda *a: (index(*a), 0))


def half_spec(rows, cols, which, start):
    return pl.BlockSpec((1, rows, cols), lambda j, off: (off[which], start + j, 0))


def both_spec(lead, rows, cols, start):
    zeros = (0,) * len(lead)
    return pl.BlockSpec((*lead, 2, rows, cols), lambda j, off: (*zeros, 0, start + j, 0))


def whole(shape):
    return pl.BlockSpec(shape, lambda *a: (0,) * len(shape), pipeline_mode=pl.Buffered(1))


def sds(shape, dtype):
    return jax.ShapeDtypeStruct(shape, dtype)


def params(**kw):
    return pltpu.CompilerParams(vmem_limit_bytes=64_000_000, **kw)


def cost(flops, nbytes):
    return pl.CostEstimate(flops=int(flops), bytes_accessed=int(nbytes), transcendentals=0)


def project_body(x_ref, g_ref, w_ref, wo_ref, gm_ref, bt_ref, u_ref, q_ref, k_ref, v_ref, do_ref, st_ref, part_ref, gr, da, qs, ks):
    i = pl.program_id(0)
    rows, cols = q_ref.shape
    groups = cols // GROUP
    do_ref[...] = dot(g_ref[...], wo_ref[...], NT).astype(BF16)
    xh, mean, inv = normalize(x_ref[...].astype(F32))
    u_ref[...] = (xh * gm_ref[...].reshape(1, -1) + bt_ref[...].reshape(1, -1)).astype(BF16)
    st_ref[...] = jnp.where(lax.broadcasted_iota(jnp.int32, st_ref.shape, 1) < LANES // 2, mean, inv)
    u = u_ref[...]
    for e, out in enumerate((q_ref, k_ref, v_ref)):
        out[...] = dot(u, w_ref[e]).astype(BF16)

    def add(acc, s, val):
        acc[s] = jnp.where(i == 0, val, acc[s] + val)

    for s in range(groups):
        c = slice(s * GROUP, (s + 1) * GROUP)
        add(gr, s, dot(q_ref[:, c], k_ref[:, c], TN))
        add(da, s, dot(do_ref[:, c], v_ref[:, c], TN))
    for acc, t in ((qs, q_ref), (ks, k_ref)):
        f = t[...].astype(F32)
        val = jnp.sum((f * f).reshape(rows // 8, 8, cols), axis=0)
        acc[...] = jnp.where(i == 0, val, acc[...] + val)

    @pl.when(i == pl.num_programs(0) - 1)
    def _():
        col_head = lax.broadcasted_iota(jnp.int32, (HEAD, GROUP), 1) // HEAD
        for a, acc in enumerate((gr, da)):
            for s in range(groups):
                tot = jnp.zeros((HEAD, GROUP), F32)
                for h in range(GROUP // HEAD):
                    tot += jnp.where(col_head == h, acc[s, h * HEAD:(h + 1) * HEAD, :], 0.0)
                part_ref[(a * groups + s) * HEAD:(a * groups + s + 1) * HEAD, :] = tot
        base = 2 * groups * HEAD
        for a, acc in enumerate((qs, ks)):
            tot = jnp.sum(acc[...], axis=0, keepdims=True)
            for s in range(groups):
                part_ref[base + 8 * (a * groups + s):base + 8 * (a * groups + s + 1), :] = jnp.broadcast_to(
                    tot[:, s * GROUP:(s + 1) * GROUP], (8, GROUP))


def project(x, g, w3, wo, gamma, beta):
    tokens, width = x.shape
    cols = wo.shape[0]
    groups = cols // GROUP
    part_rows = 2 * groups * (HEAD + 8)
    row = lambda c: row_spec(PROJ_ROWS, c, lambda i: i)
    return pl.pallas_call(
        project_body,
        grid=(tokens // PROJ_ROWS,),
        in_specs=[row(width), row(width), whole(w3.shape), whole(wo.shape), whole(gamma.shape), whole(beta.shape)],
        out_specs=[row(width)] + [row(cols)] * 4 + [row(LANES), pl.BlockSpec((part_rows, GROUP), lambda i: (0, 0))],
        out_shape=[sds((tokens, width), BF16)] + [sds((tokens, cols), BF16)] * 4 + [sds((tokens, LANES), F32), sds((part_rows, GROUP), F32)],
        scratch_shapes=[pltpu.VMEM((groups, GROUP, GROUP), F32)] * 2 + [pltpu.VMEM((8, cols), F32)] * 2,
        name="project",
        compiler_params=params(),
        cost_estimate=cost(2 * tokens * width * cols * 4.4, 2 * tokens * (3 * width + 4 * cols)),
    )(x, g, w3, wo, gamma, beta)


def far_v_body(off_ref, u_ref, w_ref, *refs):
    refs[-1][...] = dot(u_ref[0], w_ref[0]).astype(BF16)


def far_v(off, u2, w3, blocks, part, parts, prev=()):
    width, cols = w3.shape[1:]
    rows = 2 * ROWS
    steps = blocks * ROWS // rows // parts
    return pl.pallas_call(
        far_v_body,
        grid_spec=pltpu.PrefetchScalarGridSpec(
            num_scalar_prefetch=1,
            grid=(steps,),
            in_specs=[half_spec(rows, width, 1, part * steps),
                      pl.BlockSpec((1, width, cols), lambda j, off: (2, 0, 0), pipeline_mode=pl.Buffered(1))]
            + [pl.BlockSpec(memory_space=pl.ANY)] * len(prev),
            out_specs=pl.BlockSpec((rows, cols), lambda j, off: (part * steps + j, 0)),
        ),
        out_shape=sds((blocks * ROWS, cols), BF16),
        input_output_aliases={3: 0} if prev else {},
        name="far_v",
        compiler_params=params(),
        cost_estimate=cost(2 * steps * rows * width * cols, 2 * steps * rows * (width + cols)),
    )(off, u2, w3, *prev)


def state_body(near_ref, far_ref, tau_ref, attn_ref, dgram_ref, coef_ref, dtau_ref, *, groups):
    r_head = lax.broadcasted_iota(jnp.int32, (GROUP, GROUP), 0)
    c_head = lax.broadcasted_iota(jnp.int32, (GROUP, GROUP), 1)
    eye = r_head == c_head
    mask = (r_head // HEAD) == (c_head // HEAD)
    spread = lambda t: jnp.concatenate([t] * (GROUP // HEAD), axis=0)
    to_col = lambda t: jnp.sum(jnp.where(eye, t, 0.0), axis=1, keepdims=True)
    to_row = lambda t: jnp.sum(jnp.where(eye, t, 0.0), axis=0, keepdims=True)
    base = 2 * groups * HEAD
    coef_ref[...] = jnp.zeros_like(coef_ref)
    dtau_ref[...] = jnp.zeros_like(dtau_ref)
    for side, ref in enumerate((near_ref, far_ref)):
        for s in range(groups):
            gram_mat = spread(ref[s * HEAD:(s + 1) * HEAD, :])
            d_attn = spread(ref[(groups + s) * HEAD:(groups + s + 1) * HEAD, :])
            b_row = ref[base + 8 * (groups + s):base + 8 * (groups + s) + 1, :]
            a_col = to_col(ref[base + 8 * s:base + 8 * s + 1, :])
            g = side * groups + s
            tau = to_col(tau_ref[g:g + 1, :])
            norm_prod = jnp.sqrt(a_col) * jnp.sqrt(b_row)
            gram_n = gram_mat / norm_prod
            logit = jnp.where(mask, tau * gram_n, -jnp.inf)
            e = jnp.exp(logit - jnp.max(logit, axis=1, keepdims=True))
            attn = e / jnp.sum(e, axis=1, keepdims=True)
            d_attn = jnp.where(mask, d_attn, 0.0)
            d_logit = jnp.where(mask, attn * (d_attn - jnp.sum(attn * d_attn, axis=1, keepdims=True)), 0.0)
            gram_n = jnp.where(mask, gram_n, 0.0)
            grad_sn = tau * d_logit
            prod = grad_sn * gram_n
            attn_ref[g] = attn.astype(BF16)
            dgram_ref[g] = jnp.where(mask, grad_sn / norm_prod, 0.0).astype(BF16)
            coef_ref[2 * side:2 * side + 1, s * GROUP:(s + 1) * GROUP] = to_row(-jnp.sum(prod, axis=1, keepdims=True) / a_col)
            coef_ref[2 * side + 1:2 * side + 2, s * GROUP:(s + 1) * GROUP] = -jnp.sum(prod, axis=0, keepdims=True) / b_row
            dtau_ref[g:g + 1, :] = to_row(jnp.sum(d_logit * gram_n, axis=1, keepdims=True))


def head_state(near, far, tau_rows):
    groups = tau_rows.shape[0] // 2
    vm = pl.BlockSpec(memory_space=pltpu.VMEM)
    return pl.pallas_call(
        functools.partial(state_body, groups=groups),
        in_specs=[vm] * 3,
        out_specs=[vm] * 4,
        out_shape=[sds((2 * groups, GROUP, GROUP), BF16)] * 2 + [sds((8, groups * GROUP), F32), sds((8, GROUP), F32)],
        name="head_state",
        compiler_params=pltpu.CompilerParams(vmem_limit_bytes=STATE_LIMIT),
        cost_estimate=cost(10**9, 2 * 10**6),
    )(near, far, tau_rows)


def hold_body(*refs, planes):
    n = len(planes)
    srcs = [ref if e is None else ref.at[e] for ref, e in zip(refs[:n], planes)]
    copies = [pltpu.make_async_copy(srcs[k], refs[n + k], refs[-1].at[k]) for k in range(n)]
    for c in copies:
        c.start()
    for c in copies:
        c.wait()


def hold(*arrays):
    parts = [(t, e) for t in arrays for e in (range(t.shape[0]) if t.ndim == 3 else (None,))]
    return pl.pallas_call(
        functools.partial(hold_body, planes=[e for _, e in parts]),
        in_specs=[pl.BlockSpec(memory_space=pltpu.HBM)] * len(parts),
        out_specs=[pl.BlockSpec(memory_space=pltpu.VMEM)] * len(parts),
        out_shape=[sds(t.shape[-2:], t.dtype) for t, _ in parts],
        scratch_shapes=[pltpu.SemaphoreType.DMA((len(parts),))],
        name="hold",
        compiler_params=pltpu.CompilerParams(vmem_limit_bytes=HOLD_LIMIT),
        cost_estimate=cost(10**9, 4 * 10**7),
    )(*[t for t, _ in parts])


def mix_block(q, k, v, do, attn_ref, dgram_ref, coef_ref, side, s):
    groups = attn_ref.shape[0] // 2
    am, gm = attn_ref[side * groups + s], dgram_ref[side * groups + s]
    c = slice(s * GROUP, (s + 1) * GROUP)
    dq = dot(k, gm, NT) + q.astype(F32) * coef_ref[2 * side:2 * side + 1, c]
    dk = dot(q, gm, NN) + k.astype(F32) * coef_ref[2 * side + 1:2 * side + 2, c]
    return dot(v, am, NT).astype(BF16), dq.astype(BF16), dk.astype(BF16), dot(do, am, NN).astype(BF16)


def rows_body(*refs, n_alias, send_blocks):
    it = iter(refs)
    nxt = lambda n: [next(it) for _ in range(n)]
    off_ref, x_ref, g_ref, u_ref, st_ref, q_ref, k_ref, v_ref, do_ref = nxt(9)
    attn_ref, dgram_ref, coef_ref, gm_ref = nxt(4)
    wn_ref, wf_ref = nxt(3), nxt(3)
    won_ref, wof_ref = nxt(2)
    nxt(n_alias)
    y_ref, gx_ref, o_ref, rqk_ref, rv_ref = nxt(5)
    send_refs = nxt(len(send_blocks))
    (dsum_ref,) = nxt(1)
    on_s, rn_s, of_s, rf_s, qf_s, kf_s, vf_s, dof_s, gh_s = nxt(9)
    j = pl.program_id(0)
    own, other = off_ref[0], off_ref[1]
    groups = attn_ref.shape[0] // 2
    state = (attn_ref, dgram_ref, coef_ref)

    def compute(first):
        for s in range(groups):
            c = slice(s * GROUP, (s + 1) * GROUP)
            for half in (own, other):
                o, dq, dk, dv = mix_block(q_ref[half, :, c], k_ref[half, :, c], v_ref[half, :, c], do_ref[half, :, c], *state, 0, s)
                o_ref[half, :, c], rqk_ref[0, half, :, c], rqk_ref[1, half, :, c], rv_ref[half, :, c] = o, dq, dk, dv
                if half is own:
                    on_s[:, c], rn_s[0, :, c], rn_s[1, :, c], rn_s[2, :, c] = o, dq, dk, dv
        u = u_ref[0]
        for e, t in enumerate((qf_s, kf_s, vf_s)):
            t[...] = dot(u, wf_ref[e][...]).astype(BF16)
        dof_s[...] = dot(g_ref[0], wof_ref[...], NT).astype(BF16)
        for s in range(groups):
            c = slice(s * GROUP, (s + 1) * GROUP)
            of_s[:, c], rf_s[0, :, c], rf_s[1, :, c], rf_s[2, :, c] = mix_block(
                qf_s[:, c], kf_s[:, c], vf_s[:, c], dof_s[:, c], *state, 1, s)
        rows, width = gh_s.shape
        mean, inv = st_ref[0, :, :1], st_ref[0, :, LANES // 2:LANES // 2 + 1]
        fold = lambda t: jnp.sum(t.reshape(rows // 8, 8, GROUP), axis=0)
        lanes = lambda t: sum(t[:, k:k + LANES] for k in range(0, GROUP, LANES))
        gamma = gm_ref[...].reshape(1, width)
        tiles = [slice(n, n + GROUP) for n in range(0, width, GROUP)]
        s1 = s2 = 0.0
        for c in tiles:
            du = dot(rn_s[0], wn_ref[0][c, :], NT)
            for e in range(1, 3):
                du += dot(rn_s[e], wn_ref[e][c, :], NT)
            for e in range(3):
                du += dot(rf_s[e], wf_ref[e][c, :], NT)
            xh = (x_ref[0, :, c].astype(F32) - mean) * inv
            for a, val in enumerate((fold(du * xh), fold(du))):
                dsum_ref[a, :, c] = jnp.where(first, val, dsum_ref[a, :, c] + val)
            gh = du * gamma[:, c]
            s1 += lanes(gh)
            s2 += lanes(gh * xh)
            gh_s[:, c] = gh
        m1 = jnp.sum(s1, axis=1, keepdims=True) / width
        m2 = jnp.sum(s2, axis=1, keepdims=True) / width
        for c in tiles:
            x = x_ref[0, :, c].astype(F32)
            yp = dot(on_s[...], won_ref[:, c]) + dot(of_s[...], wof_ref[:, c])
            y_ref[0, :, c] = (x + yp).astype(BF16)
            dx = g_ref[0, :, c].astype(F32) + inv * (gh_s[:, c] - m1 - (x - mean) * inv * m2)
            for ref in [gx_ref] + send_refs[:1] * (len(send_refs) == 1):
                ref[0, :, c] = dx.astype(BF16)

    compute(j == 0)

    if len(send_refs) > 1:
        start = 0
        for ref, n in zip(send_refs, send_blocks):

            @pl.when((j >= start) & (j < start + n))
            def _(ref=ref):
                ref[0] = gx_ref[0]

            start += n


def rows_call(off, start, send_blocks, acts, state, weights, prev):
    _, half, width = acts[0].shape
    blocks = sum(send_blocks)
    firsts = [sum(send_blocks[:n]) for n in range(len(send_blocks))]
    send_spec = lambda first, n: pl.BlockSpec((1, ROWS, width), lambda j, off: (0, jnp.clip(j - first, 0, n - 1), 0))
    cols = acts[4].shape[2]
    row = half_spec(ROWS, width, 0, start)
    both = lambda *lead: both_spec(lead, ROWS, cols, start)
    *loaded, gamma = weights
    consts = list(state) + [gamma]
    first = 1 + len(acts) + len(consts) + len(loaded)
    return pl.pallas_call(
        functools.partial(rows_body, n_alias=len(prev), send_blocks=send_blocks),
        grid_spec=pltpu.PrefetchScalarGridSpec(
            num_scalar_prefetch=1,
            grid=(blocks,),
            in_specs=[row] * 3 + [half_spec(ROWS, LANES, 0, start)] + [both()] * 4 + [whole(t.shape) for t in consts] + [pl.BlockSpec(memory_space=pltpu.VMEM)] * len(loaded) + [pl.BlockSpec(memory_space=pl.ANY)] * len(prev),
            out_specs=[row, row, both(), both(2), both(),
                       *[send_spec(first, n) for first, n in zip(firsts, send_blocks)],
                       pl.BlockSpec((2, 8, width), lambda j, off: (0, 0, 0))],
            scratch_shapes=[pltpu.VMEM((ROWS, cols), BF16), pltpu.VMEM((3, ROWS, cols), BF16)] * 2 + [pltpu.VMEM((ROWS, cols), BF16)] * 4
            + [pltpu.VMEM((ROWS, width), F32)],
        ),
        out_shape=[sds((2, half, width), BF16)] * 2 + [sds((2, half, cols), BF16), sds((2, 2, half, cols), BF16), sds((2, half, cols), BF16),
                                                       *[sds((1, n * ROWS, width), BF16) for n in send_blocks], sds((2, 8, width), F32)],
        input_output_aliases={first + a: a for a in range(len(prev))},
        name="rows",
        compiler_params=pltpu.CompilerParams(vmem_limit_bytes=ROWS_LIMIT),
        cost_estimate=cost(2 * blocks * ROWS * width * cols * 13, 2 * blocks * ROWS * (6 * width + 16 * cols)),
    )(off, *acts, *consts, *loaded, *prev)


def far_y_body(*refs, early, copies):
    it = iter(refs)
    nxt = lambda n: [next(it) for _ in range(n)]
    _, x_ref, o_ref, u_ref, v_ref, attn_ref, won_ref, wof_ref, wv_ref, pv_ref = nxt(10)
    recv = nxt(len(copies))
    _, _, y_ref, gx_ref, gw_ref, vf_s, of_s, sem = nxt(8)
    j = pl.program_id(0)
    rows = gx_ref.shape[1]

    def file_rows(act):
        start = 0
        for ref, n in zip(recv, copies):

            @pl.when((j >= start) & (j < start + n))
            def _(ref=ref, start=start):
                act(pltpu.make_async_copy(ref.at[0, pl.ds((j - start) * rows, rows)], gx_ref.at[0], sem))

            start += n

    file_rows(lambda copy: copy.start())
    gw_ref[...] = pv_ref[...]

    @pl.when(j < early)
    def _():
        vf_s[...] = v_ref[...]

    @pl.when(j >= early)
    def _():
        vf_s[...] = dot(u_ref[0], wv_ref[0]).astype(BF16)

    groups = attn_ref.shape[0] // 2
    for s in range(groups):
        c = slice(s * GROUP, (s + 1) * GROUP)
        of_s[:, c] = dot(vf_s[:, c], attn_ref[groups + s], NT).astype(BF16)
    y_ref[0] = (x_ref[0].astype(F32) + (dot(o_ref[0], won_ref[...]) + dot(of_s[...], wof_ref[...]))).astype(BF16)
    file_rows(lambda copy: copy.wait())


def far_y(off, x2, o2, u2, vf, attn, wo_near, wo_far, w_far, dw_v, recv, y2, gx2):
    half, width = x2.shape[1:]
    cols = o2.shape[2]
    rows = 2 * ROWS
    steps = half // rows
    early = vf.shape[0] // rows
    copies = [t.shape[1] // rows for t in recv]
    row = lambda c: half_spec(rows, c, 1, 0)
    part = (1, dw_v.shape[1] // steps, cols)
    any_ = pl.BlockSpec(memory_space=pl.ANY)
    specs = [row(width), row(cols),
             pl.BlockSpec((1, rows, width), lambda j, off: (off[1], jnp.maximum(j, early), 0)),
             pl.BlockSpec((rows, cols), lambda j, off: (jnp.minimum(j, early - 1), 0)),
             whole(attn.shape), whole(wo_near.shape), whole(wo_far.shape),
             pl.BlockSpec((1, width, cols), lambda j, off: (2, 0, 0), pipeline_mode=pl.Buffered(1)),
             pl.BlockSpec(part, lambda j, off: (0, j, 0))]
    args = [x2, o2, u2, vf, attn, wo_near, wo_far, w_far, dw_v, *recv]
    return pl.pallas_call(
        functools.partial(far_y_body, early=early, copies=copies),
        grid_spec=pltpu.PrefetchScalarGridSpec(
            num_scalar_prefetch=1,
            grid=(steps,),
            in_specs=specs + [any_] * (len(recv) + 2),
            out_specs=[row(width), pl.BlockSpec((1, rows, width), lambda j, off: (off[1], jnp.minimum(j, sum(copies) - 1), 0)), pl.BlockSpec(part, lambda j, off: (2, j, 0))],
            scratch_shapes=[pltpu.VMEM((rows, cols), BF16)] * 2 + [pltpu.SemaphoreType.DMA],
        ),
        out_shape=[sds(y2.shape, y2.dtype), sds(gx2.shape, gx2.dtype), sds((3, *dw_v.shape[1:]), F32)],
        input_output_aliases={len(args) + 1: 0, len(args) + 2: 1},
        name="far_y",
        compiler_params=params(),
        cost_estimate=cost(2 * half * width * cols * 2.8, 2 * half * (4 * width + 3 * cols)),
    )(off, *args, y2, gx2)


def token_sum_body(*refs, planes):
    n = len(planes)
    first = pl.program_id(0) == 0
    out = 2 * n
    for l_ref, r_ref, count in zip(refs[:n], refs[n:out], planes):
        o_ref, out = refs[out], out + 1
        for e in range(count):
            val = dot(l_ref[...], r_ref[e], TN)
            o_ref[e] = jnp.where(first, val, o_ref[e] + val)


def token_sum(*pairs):
    tokens = pairs[0][0].shape[0]
    flops = sum(2 * r.shape[0] * tokens * l.shape[1] * r.shape[2] for l, r in pairs)
    nbytes = sum(2 * tokens * (l.shape[1] + r.shape[0] * r.shape[2]) for l, r in pairs)
    shapes = [(r.shape[0], l.shape[1], r.shape[2]) for l, r in pairs]
    return pl.pallas_call(
        functools.partial(token_sum_body, planes=[r.shape[0] for _, r in pairs]),
        grid=(tokens // SUM_ROWS,),
        in_specs=[row_spec(SUM_ROWS, l.shape[1], lambda i: i) for l, _ in pairs]
        + [pl.BlockSpec((r.shape[0], SUM_ROWS, r.shape[2]), lambda i: (0, i, 0)) for _, r in pairs],
        out_specs=[pl.BlockSpec(s, lambda i: (0, 0, 0)) for s in shapes],
        out_shape=[sds(s, F32) for s in shapes],
        name="token_sum",
        compiler_params=params(),
        cost_estimate=cost(flops, nbytes),
    )(*[l for l, _ in pairs], *[r for _, r in pairs])


def solution(mesh):
    tp_size = mesh.shape["tp"]
    sp_size = mesh.shape["sp"]
    in_rows = P(("dp", "sp"), None)
    swap = [(0, 1), (1, 0)]

    def exchange(t):
        return lax.ppermute(t, "tp", swap)

    def step(x, g, w_qkv, w_out, ln_gamma, ln_beta, temps):
        tokens, width = x.shape
        cols = w_qkv.shape[2]
        groups = cols // GROUP
        me = lax.axis_index("tp")
        w_near = jnp.transpose(w_qkv, (1, 0, 2))
        w_far = exchange(w_near)
        wo_far = exchange(w_out)
        half = tokens // 2
        off = jnp.stack([me, 1 - me]).astype(jnp.int32)
        halves = lambda t: t.reshape(2, half, t.shape[-1])

        u, q, k, v, do, stats, part = project(x, g, w_near, w_out, ln_gamma, ln_beta)
        x2, g2, u2, stats2 = halves(x), halves(g), halves(u), halves(stats)
        near = tuple(halves(t) for t in (q, k, v, do))
        peers = [lax.ppermute(part, "sp", [(s, s ^ d) for s in range(sp_size)]) for d in (1, 2, 3)]
        part = (part + peers[0]) + (peers[1] + peers[2])
        part, wn_, wf_ = lax.optimization_barrier((part, w_near, w_far))
        part_far = exchange(part)
        held = (*hold(wn_, wf_), w_out, wo_far)
        vf = far_v(off, u2, w_far, EARLY_V, 0, 1)
        tau = jnp.repeat(temps, HEAD).reshape(tp_size, groups, GROUP)
        tau = jnp.where(me == 0, tau, tau[::-1]).reshape(2 * groups, GROUP)
        attn, dgram, coef, dtau = head_state(part, part_far, tau)
        state = (attn, dgram, coef)

        prev, dsum, recv, start = (), None, [], 0
        for sizes in OWN_CHUNKS:
            out = rows_call(off, start, sizes, (x2, g2, u2, stats2) + near, state, (*held, ln_gamma), prev)
            prev, sent, ds = out[:5], out[5:-1], out[-1]
            recv += [exchange(t) for t in sent]
            dsum = ds if dsum is None else dsum + ds
            start += sum(sizes)
        y2, gx2, o2, rqk, rv = prev
        dtau, rqk = lax.optimization_barrier((dtau, rqk))
        dtau = jnp.sum(dtau[:2 * groups].reshape(tp_size, cols // HEAD, HEAD), axis=2)
        grad_temp = jnp.where(me == 0, dtau, dtau[::-1]).reshape(-1)

        dw_o, dw_v = token_sum((o2.reshape(tokens, cols), g[None]), (u, rv.reshape(1, tokens, cols)))
        rqk, dw_o, dw_v = lax.optimization_barrier((rqk, dw_o, dw_v))
        grad_wout = lax.psum_scatter(dw_o[0], "sp", scatter_dimension=0, tiled=True)
        dw_v = lax.psum_scatter(dw_v, "sp", scatter_dimension=1, tiled=True)
        (dw_qk,) = token_sum((u, rqk.reshape(2, tokens, cols)))
        y2, dw_qk = lax.optimization_barrier((y2, dw_qk))
        dw_qk = lax.psum_scatter(dw_qk, "sp", scatter_dimension=1, tiled=True)
        y2, gx2, gw = far_y(off, x2, o2, u2, vf, attn, w_out, wo_far, w_far, dw_v, recv[:-1], y2, gx2)
        grad_wqkv = jnp.transpose(lax.dynamic_update_slice(gw, dw_qk, (0, 0, 0)), (1, 0, 2))

        sums = jnp.sum(dsum, axis=1)
        for axis, perm in (("tp", swap), ("sp", [(s, s ^ 1) for s in range(sp_size)]), ("sp", [(s, s ^ 2) for s in range(sp_size)])):
            sums = sums + lax.ppermute(sums, axis, perm)
        gx2 = lax.dynamic_update_slice(gx2, recv[-1], (off[1], half - recv[-1].shape[1], 0))
        return y2.reshape(tokens, width), gx2.reshape(tokens, width), grad_wqkv, grad_wout, sums[0], sums[1], grad_temp

    in_specs = (in_rows, in_rows, P(None, None, "tp"), P("tp", None), P(None), P(None), P(None))
    out_specs = (in_rows, in_rows, P(("dp", "sp"), None, "tp"), P(("dp", "tp", "sp"), None), P("dp"), P("dp"), P("dp"))
    return jax.shard_map(step, mesh=mesh, in_specs=in_specs, out_specs=out_specs, check_vma=False)
```

```python
import functools

import jax
import jax.numpy as jnp
from jax import lax
from jax.experimental import pallas as pl
from jax.experimental.pallas import tpu as pltpu
from jax.sharding import PartitionSpec as P


LN_EPS = 1e-6
GROUP = 256
HEAD = 32
LANES = 128
F32 = jnp.float32
BF16 = jnp.bfloat16
NN = (((1,), (0,)), ((), ()))
NT = (((1,), (1,)), ((), ()))
TN = (((0,), (0,)), ((), ()))
PROJ_ROWS = 1024
ROWS = 256
STATE_LIMIT = 16_000_000
ROWS_LIMIT = 38_000_000
HOLD_LIMIT = 36_000_000
SUM_ROWS = 1024
OWN_CHUNKS = ((4,), (6,), (10,), (6, 6))
EARLY_V = 4


def dot(a, b, dims=NN):
    return lax.dot_general(a, b, dims, preferred_element_type=F32)


def normalize(x):
    mean = jnp.mean(x, axis=-1, keepdims=True)
    cen = x - mean
    inv = lax.rsqrt(jnp.mean(cen * cen, axis=-1, keepdims=True) + LN_EPS)
    return cen * inv, mean, inv


def row_spec(rows, cols, index):
    return pl.BlockSpec((rows, cols), lambda *a: (index(*a), 0))


def half_spec(rows, cols, which, start):
    return pl.BlockSpec((1, rows, cols), lambda j, off: (off[which], start + j, 0))


def both_spec(lead, rows, cols, start):
    zeros = (0,) * len(lead)
    return pl.BlockSpec((*lead, 2, rows, cols), lambda j, off: (*zeros, 0, start + j, 0))


def whole(shape):
    return pl.BlockSpec(shape, lambda *a: (0,) * len(shape), pipeline_mode=pl.Buffered(1))


def sds(shape, dtype):
    return jax.ShapeDtypeStruct(shape, dtype)


def params(**kw):
    return pltpu.CompilerParams(vmem_limit_bytes=64_000_000, **kw)


def cost(flops, nbytes):
    return pl.CostEstimate(flops=int(flops), bytes_accessed=int(nbytes), transcendentals=0)


def project_body(x_ref, g_ref, w_ref, wo_ref, gm_ref, bt_ref, u_ref, act_ref, st_ref, part_ref, gr, da, qs, ks):
    i = pl.program_id(0)
    q_ref, k_ref, v_ref, do_ref = (act_ref.at[e] for e in range(4))
    rows, cols = q_ref.shape
    groups = cols // GROUP
    do_ref[...] = dot(g_ref[...], wo_ref[...], NT).astype(BF16)
    xh, mean, inv = normalize(x_ref[...].astype(F32))
    u_ref[...] = (xh * gm_ref[...].reshape(1, -1) + bt_ref[...].reshape(1, -1)).astype(BF16)
    st_ref[...] = jnp.where(lax.broadcasted_iota(jnp.int32, st_ref.shape, 1) < LANES // 2, mean, inv)
    u = u_ref[...]
    for e, out in enumerate((q_ref, k_ref, v_ref)):
        out[...] = dot(u, w_ref[e]).astype(BF16)

    def add(acc, s, val):
        acc[s] = jnp.where(i == 0, val, acc[s] + val)

    for s in range(groups):
        c = slice(s * GROUP, (s + 1) * GROUP)
        add(gr, s, dot(q_ref[:, c], k_ref[:, c], TN))
        add(da, s, dot(do_ref[:, c], v_ref[:, c], TN))
    for acc, t in ((qs, q_ref), (ks, k_ref)):
        f = t[...].astype(F32)
        val = jnp.sum((f * f).reshape(rows // 8, 8, cols), axis=0)
        acc[...] = jnp.where(i == 0, val, acc[...] + val)

    @pl.when(i == pl.num_programs(0) - 1)
    def _():
        col_head = lax.broadcasted_iota(jnp.int32, (HEAD, GROUP), 1) // HEAD
        for a, acc in enumerate((gr, da)):
            for s in range(groups):
                tot = jnp.zeros((HEAD, GROUP), F32)
                for h in range(GROUP // HEAD):
                    tot += jnp.where(col_head == h, acc[s, h * HEAD:(h + 1) * HEAD, :], 0.0)
                part_ref[(a * groups + s) * HEAD:(a * groups + s + 1) * HEAD, :] = tot
        base = 2 * groups * HEAD
        part_ref[base:, :] = jnp.zeros((part_ref.shape[0] - base, GROUP), F32)
        for a, acc in enumerate((qs, ks)):
            tot = jnp.sum(acc[...], axis=0, keepdims=True)
            for s in range(groups):
                part_ref[base + a * groups + s:base + a * groups + s + 1, :] = tot[:, s * GROUP:(s + 1) * GROUP]


def project(x, g, w3, wo, gamma, beta):
    tokens, width = x.shape
    cols = wo.shape[0]
    groups = cols // GROUP
    part_rows = 2 * groups * HEAD + 8 * pl.cdiv(2 * groups, 8)
    row = lambda c: row_spec(PROJ_ROWS, c, lambda i: i)
    return pl.pallas_call(
        project_body,
        grid=(tokens // PROJ_ROWS,),
        in_specs=[row(width), row(width), whole(w3.shape), whole(wo.shape), whole(gamma.shape), whole(beta.shape)],
        out_specs=[row(width), pl.BlockSpec((4, PROJ_ROWS, cols), lambda i: (0, i, 0)), row(LANES), pl.BlockSpec((part_rows, GROUP), lambda i: (0, 0))],
        out_shape=[sds((tokens, width), BF16), sds((4, tokens, cols), BF16), sds((tokens, LANES), F32), sds((part_rows, GROUP), F32)],
        scratch_shapes=[pltpu.VMEM((groups, GROUP, GROUP), F32)] * 2 + [pltpu.VMEM((8, cols), F32)] * 2,
        name="project",
        compiler_params=params(),
        cost_estimate=cost(2 * tokens * width * cols * 4.4, 2 * tokens * (3 * width + 4 * cols)),
    )(x, g, w3, wo, gamma, beta)


def far_v_body(off_ref, u_ref, w_ref, *refs):
    refs[-1][...] = dot(u_ref[0], w_ref[0]).astype(BF16)


def far_v(off, u2, w3, blocks, part, parts, prev=()):
    width, cols = w3.shape[1:]
    rows = 2 * ROWS
    steps = blocks * ROWS // rows // parts
    return pl.pallas_call(
        far_v_body,
        grid_spec=pltpu.PrefetchScalarGridSpec(
            num_scalar_prefetch=1,
            grid=(steps,),
            in_specs=[half_spec(rows, width, 1, part * steps),
                      pl.BlockSpec((1, width, cols), lambda j, off: (2, 0, 0), pipeline_mode=pl.Buffered(1))]
            + [pl.BlockSpec(memory_space=pl.ANY)] * len(prev),
            out_specs=pl.BlockSpec((rows, cols), lambda j, off: (part * steps + j, 0)),
        ),
        out_shape=sds((blocks * ROWS, cols), BF16),
        input_output_aliases={3: 0} if prev else {},
        name="far_v",
        compiler_params=params(),
        cost_estimate=cost(2 * steps * rows * width * cols, 2 * steps * rows * (width + cols)),
    )(off, u2, w3, *prev)


def state_body(near_ref, far_ref, tau_ref, attn_ref, dgram_ref, coef_ref, dtau_ref, *, groups):
    r_head = lax.broadcasted_iota(jnp.int32, (GROUP, GROUP), 0)
    c_head = lax.broadcasted_iota(jnp.int32, (GROUP, GROUP), 1)
    eye = r_head == c_head
    mask = (r_head // HEAD) == (c_head // HEAD)
    spread = lambda t: jnp.concatenate([t] * (GROUP // HEAD), axis=0)
    to_col = lambda t: jnp.sum(jnp.where(eye, t, 0.0), axis=1, keepdims=True)
    to_row = lambda t: jnp.sum(jnp.where(eye, t, 0.0), axis=0, keepdims=True)
    base = 2 * groups * HEAD
    coef_ref[...] = jnp.zeros_like(coef_ref)
    dtau_ref[...] = jnp.zeros_like(dtau_ref)
    for side, ref in enumerate((near_ref, far_ref)):
        for s in range(groups):
            gram_mat = spread(ref[s * HEAD:(s + 1) * HEAD, :])
            d_attn = spread(ref[(groups + s) * HEAD:(groups + s + 1) * HEAD, :])
            b_row = ref[base + groups + s:base + groups + s + 1, :]
            a_col = to_col(ref[base + s:base + s + 1, :])
            g = side * groups + s
            tau = to_col(tau_ref[g:g + 1, :])
            norm_prod = jnp.sqrt(a_col) * jnp.sqrt(b_row)
            gram_n = gram_mat / norm_prod
            logit = jnp.where(mask, tau * gram_n, -jnp.inf)
            e = jnp.exp(logit - jnp.max(logit, axis=1, keepdims=True))
            attn = e / jnp.sum(e, axis=1, keepdims=True)
            d_attn = jnp.where(mask, d_attn, 0.0)
            d_logit = jnp.where(mask, attn * (d_attn - jnp.sum(attn * d_attn, axis=1, keepdims=True)), 0.0)
            gram_n = jnp.where(mask, gram_n, 0.0)
            grad_sn = tau * d_logit
            prod = grad_sn * gram_n
            attn_ref[g] = attn.astype(BF16)
            dgram_ref[g] = jnp.where(mask, grad_sn / norm_prod, 0.0).astype(BF16)
            coef_ref[2 * side:2 * side + 1, s * GROUP:(s + 1) * GROUP] = to_row(-jnp.sum(prod, axis=1, keepdims=True) / a_col)
            coef_ref[2 * side + 1:2 * side + 2, s * GROUP:(s + 1) * GROUP] = -jnp.sum(prod, axis=0, keepdims=True) / b_row
            dtau_ref[g:g + 1, :] = to_row(jnp.sum(d_logit * gram_n, axis=1, keepdims=True))


def head_state(near, far, tau_rows):
    groups = tau_rows.shape[0] // 2
    vm = pl.BlockSpec(memory_space=pltpu.VMEM)
    return pl.pallas_call(
        functools.partial(state_body, groups=groups),
        in_specs=[vm] * 3,
        out_specs=[vm] * 4,
        out_shape=[sds((2 * groups, GROUP, GROUP), BF16)] * 2 + [sds((8, groups * GROUP), F32), sds((8, GROUP), F32)],
        name="head_state",
        compiler_params=pltpu.CompilerParams(vmem_limit_bytes=STATE_LIMIT),
        cost_estimate=cost(10**9, 2 * 10**6),
    )(near, far, tau_rows)


def hold_body(*refs, planes):
    n = len(planes)
    srcs = [ref if e is None else ref.at[e] for ref, e in zip(refs[:n], planes)]
    copies = [pltpu.make_async_copy(srcs[k], refs[n + k], refs[-1].at[k]) for k in range(n)]
    for c in copies:
        c.start()
    for c in copies:
        c.wait()


def hold(*arrays):
    parts = [(t, e) for t in arrays for e in (range(t.shape[0]) if t.ndim == 3 else (None,))]
    return pl.pallas_call(
        functools.partial(hold_body, planes=[e for _, e in parts]),
        in_specs=[pl.BlockSpec(memory_space=pltpu.HBM)] * len(parts),
        out_specs=[pl.BlockSpec(memory_space=pltpu.VMEM)] * len(parts),
        out_shape=[sds(t.shape[-2:], t.dtype) for t, _ in parts],
        scratch_shapes=[pltpu.SemaphoreType.DMA((len(parts),))],
        name="hold",
        compiler_params=pltpu.CompilerParams(vmem_limit_bytes=HOLD_LIMIT),
        cost_estimate=cost(10**9, 4 * 10**7),
    )(*[t for t, _ in parts])


def mix_block(q, k, v, do, attn_ref, dgram_ref, coef_ref, side, s):
    groups = attn_ref.shape[0] // 2
    am, gm = attn_ref[side * groups + s], dgram_ref[side * groups + s]
    c = slice(s * GROUP, (s + 1) * GROUP)
    dq = dot(k, gm, NT) + q.astype(F32) * coef_ref[2 * side:2 * side + 1, c]
    dk = dot(q, gm, NN) + k.astype(F32) * coef_ref[2 * side + 1:2 * side + 2, c]
    return dot(v, am, NT).astype(BF16), dq.astype(BF16), dk.astype(BF16), dot(do, am, NN).astype(BF16)


def rows_body(*refs, n_alias, send_blocks):
    it = iter(refs)
    nxt = lambda n: [next(it) for _ in range(n)]
    off_ref, x_ref, g_ref, u_ref, st_ref, act_ref = nxt(6)
    attn_ref, dgram_ref, coef_ref, gm_ref = nxt(4)
    wn_ref, wf_ref = nxt(3), nxt(3)
    won_ref, wof_ref = nxt(2)
    nxt(n_alias)
    y_ref, gx_ref, r_ref = nxt(3)
    send_refs = nxt(len(send_blocks))
    (dsum_ref,) = nxt(1)
    on_s, rn_s, of_s, rf_s, qf_s, kf_s, vf_s, dof_s, gh_s = nxt(9)
    j = pl.program_id(0)
    own, other = off_ref[0], off_ref[1]
    groups = attn_ref.shape[0] // 2
    state = (attn_ref, dgram_ref, coef_ref)

    def compute(first):
        for s in range(groups):
            c = slice(s * GROUP, (s + 1) * GROUP)
            for half in (own, other):
                o, dq, dk, dv = mix_block(*(act_ref[e, half, :, c] for e in range(4)), *state, 0, s)
                r_ref[0, half, :, c], r_ref[1, half, :, c], r_ref[2, half, :, c], r_ref[3, half, :, c] = dq, dk, dv, o
                if half is own:
                    on_s[:, c], rn_s[0, :, c], rn_s[1, :, c], rn_s[2, :, c] = o, dq, dk, dv
        u = u_ref[0]
        for e, t in enumerate((qf_s, kf_s, vf_s)):
            t[...] = dot(u, wf_ref[e][...]).astype(BF16)
        dof_s[...] = dot(g_ref[0], wof_ref[...], NT).astype(BF16)
        for s in range(groups):
            c = slice(s * GROUP, (s + 1) * GROUP)
            of_s[:, c], rf_s[0, :, c], rf_s[1, :, c], rf_s[2, :, c] = mix_block(
                qf_s[:, c], kf_s[:, c], vf_s[:, c], dof_s[:, c], *state, 1, s)
        rows, width = gh_s.shape
        mean, inv = st_ref[0, :, :1], st_ref[0, :, LANES // 2:LANES // 2 + 1]
        fold = lambda t: jnp.sum(t.reshape(rows // 8, 8, GROUP), axis=0)
        lanes = lambda t: sum(t[:, k:k + LANES] for k in range(0, GROUP, LANES))
        gamma = gm_ref[...].reshape(1, width)
        tiles = [slice(n, n + GROUP) for n in range(0, width, GROUP)]
        s1 = s2 = 0.0
        for c in tiles:
            du = dot(rn_s[0], wn_ref[0][c, :], NT)
            for e in range(1, 3):
                du += dot(rn_s[e], wn_ref[e][c, :], NT)
            for e in range(3):
                du += dot(rf_s[e], wf_ref[e][c, :], NT)
            xh = (x_ref[0, :, c].astype(F32) - mean) * inv
            for a, val in enumerate((fold(du * xh), fold(du))):
                dsum_ref[a, :, c] = jnp.where(first, val, dsum_ref[a, :, c] + val)
            gh = du * gamma[:, c]
            s1 += lanes(gh)
            s2 += lanes(gh * xh)
            gh_s[:, c] = gh
        m1 = jnp.sum(s1, axis=1, keepdims=True) / width
        m2 = jnp.sum(s2, axis=1, keepdims=True) / width
        for c in tiles:
            x = x_ref[0, :, c].astype(F32)
            yp = dot(on_s[...], won_ref[:, c]) + dot(of_s[...], wof_ref[:, c])
            y_ref[0, :, c] = (x + yp).astype(BF16)
            dx = g_ref[0, :, c].astype(F32) + inv * (gh_s[:, c] - m1 - (x - mean) * inv * m2)
            for ref in [gx_ref] + send_refs[:1] * (len(send_refs) == 1):
                ref[0, :, c] = dx.astype(BF16)

    compute(j == 0)

    if len(send_refs) > 1:
        start = 0
        for ref, n in zip(send_refs, send_blocks):

            @pl.when((j >= start) & (j < start + n))
            def _(ref=ref):
                ref[0] = gx_ref[0]

            start += n


def rows_call(off, start, send_blocks, acts, state, weights, prev):
    _, half, width = acts[0].shape
    blocks = sum(send_blocks)
    firsts = [sum(send_blocks[:n]) for n in range(len(send_blocks))]
    send_spec = lambda first, n: pl.BlockSpec((1, ROWS, width), lambda j, off: (0, jnp.clip(j - first, 0, n - 1), 0))
    cols = acts[4].shape[-1]
    row = half_spec(ROWS, width, 0, start)
    both = lambda *lead: both_spec(lead, ROWS, cols, start)
    *loaded, gamma = weights
    consts = list(state) + [gamma]
    first = 1 + len(acts) + len(consts) + len(loaded)
    return pl.pallas_call(
        functools.partial(rows_body, n_alias=len(prev), send_blocks=send_blocks),
        grid_spec=pltpu.PrefetchScalarGridSpec(
            num_scalar_prefetch=1,
            grid=(blocks,),
            in_specs=[row] * 3 + [half_spec(ROWS, LANES, 0, start), both(4)] + [whole(t.shape) for t in consts] + [pl.BlockSpec(memory_space=pltpu.VMEM)] * len(loaded) + [pl.BlockSpec(memory_space=pl.ANY)] * len(prev),
            out_specs=[row, row, both(4),
                       *[send_spec(first, n) for first, n in zip(firsts, send_blocks)],
                       pl.BlockSpec((2, 8, width), lambda j, off: (0, 0, 0))],
            scratch_shapes=[pltpu.VMEM((ROWS, cols), BF16), pltpu.VMEM((3, ROWS, cols), BF16)] * 2 + [pltpu.VMEM((ROWS, cols), BF16)] * 4
            + [pltpu.VMEM((ROWS, width), F32)],
        ),
        out_shape=[sds((2, half, width), BF16)] * 2 + [sds((4, 2, half, cols), BF16),
                                                       *[sds((1, n * ROWS, width), BF16) for n in send_blocks], sds((2, 8, width), F32)],
        input_output_aliases={first + a: a for a in range(len(prev))},
        name="rows",
        compiler_params=pltpu.CompilerParams(vmem_limit_bytes=ROWS_LIMIT),
        cost_estimate=cost(2 * blocks * ROWS * width * cols * 13, 2 * blocks * ROWS * (6 * width + 16 * cols)),
    )(off, *acts, *consts, *loaded, *prev)


def far_y_body(*refs, early, copies):
    it = iter(refs)
    nxt = lambda n: [next(it) for _ in range(n)]
    _, x_ref, o_ref, u_ref, v_ref, attn_ref, won_ref, wof_ref, wv_ref, pv_ref = nxt(10)
    recv = nxt(len(copies))
    _, _, y_ref, gx_ref, gw_ref, vf_s, of_s, sem = nxt(8)
    j = pl.program_id(0)
    rows = gx_ref.shape[1]

    def file_rows(act):
        start = 0
        for ref, n in zip(recv, copies):

            @pl.when((j >= start) & (j < start + n))
            def _(ref=ref, start=start):
                act(pltpu.make_async_copy(ref.at[0, pl.ds((j - start) * rows, rows)], gx_ref.at[0], sem))

            start += n

    file_rows(lambda copy: copy.start())
    gw_ref[...] = pv_ref[...]

    @pl.when(j < early)
    def _():
        vf_s[...] = v_ref[...]

    @pl.when(j >= early)
    def _():
        vf_s[...] = dot(u_ref[0], wv_ref[0]).astype(BF16)

    groups = attn_ref.shape[0] // 2
    for s in range(groups):
        c = slice(s * GROUP, (s + 1) * GROUP)
        of_s[:, c] = dot(vf_s[:, c], attn_ref[groups + s], NT).astype(BF16)
    y_ref[0] = (x_ref[0].astype(F32) + (dot(o_ref[0, 0], won_ref[...]) + dot(of_s[...], wof_ref[...]))).astype(BF16)
    file_rows(lambda copy: copy.wait())


def far_y(off, x2, r, u2, vf, attn, wo_near, wo_far, w_far, dw_v, recv, y2, gx2):
    half, width = x2.shape[1:]
    cols = r.shape[-1]
    rows = 2 * ROWS
    steps = half // rows
    early = vf.shape[0] // rows
    copies = [t.shape[1] // rows for t in recv]
    row = lambda c: half_spec(rows, c, 1, 0)
    part = (1, dw_v.shape[1] // steps, cols)
    any_ = pl.BlockSpec(memory_space=pl.ANY)
    specs = [row(width), pl.BlockSpec((1, 1, rows, cols), lambda j, off: (3, off[1], j, 0)),
             pl.BlockSpec((1, rows, width), lambda j, off: (off[1], jnp.maximum(j, early), 0)),
             pl.BlockSpec((rows, cols), lambda j, off: (jnp.minimum(j, early - 1), 0)),
             whole(attn.shape), whole(wo_near.shape), whole(wo_far.shape),
             pl.BlockSpec((1, width, cols), lambda j, off: (2, 0, 0), pipeline_mode=pl.Buffered(1)),
             pl.BlockSpec(part, lambda j, off: (0, j, 0))]
    args = [x2, r, u2, vf, attn, wo_near, wo_far, w_far, dw_v, *recv]
    return pl.pallas_call(
        functools.partial(far_y_body, early=early, copies=copies),
        grid_spec=pltpu.PrefetchScalarGridSpec(
            num_scalar_prefetch=1,
            grid=(steps,),
            in_specs=specs + [any_] * (len(recv) + 2),
            out_specs=[row(width), pl.BlockSpec((1, rows, width), lambda j, off: (off[1], jnp.minimum(j, sum(copies) - 1), 0)), pl.BlockSpec(part, lambda j, off: (2, j, 0))],
            scratch_shapes=[pltpu.VMEM((rows, cols), BF16)] * 2 + [pltpu.SemaphoreType.DMA],
        ),
        out_shape=[sds(y2.shape, y2.dtype), sds(gx2.shape, gx2.dtype), sds((3, *dw_v.shape[1:]), F32)],
        input_output_aliases={len(args) + 1: 0, len(args) + 2: 1},
        name="far_y",
        compiler_params=params(),
        cost_estimate=cost(2 * half * width * cols * 2.8, 2 * half * (4 * width + 3 * cols)),
    )(off, *args, y2, gx2)


def token_sum_body(*refs, planes):
    n = len(planes)
    first = pl.program_id(0) == 0
    out = 2 * n
    for l_ref, r_ref, count in zip(refs[:n], refs[n:out], planes):
        o_ref, out = refs[out], out + 1
        for e in range(count):
            val = dot(l_ref[0], r_ref[e], TN)
            o_ref[e] = jnp.where(first, val, o_ref[e] + val)


def token_sum(*pairs):
    tokens = pairs[0][0][0].shape[1]
    spec = lambda t, e, count: pl.BlockSpec((count, SUM_ROWS, t.shape[2]), lambda i: (e // count, i, 0))
    shapes = [(count, l.shape[2], r.shape[2]) for (l, _), (r, _, count) in pairs]
    return pl.pallas_call(
        functools.partial(token_sum_body, planes=[s[0] for s in shapes]),
        grid=(tokens // SUM_ROWS,),
        in_specs=[spec(l, e, 1) for (l, e), _ in pairs] + [spec(*rhs) for _, rhs in pairs],
        out_specs=[pl.BlockSpec(s, lambda i: (0, 0, 0)) for s in shapes],
        out_shape=[sds(s, F32) for s in shapes],
        name="token_sum",
        compiler_params=params(),
        cost_estimate=cost(sum(2 * tokens * a * b * c for a, b, c in shapes), sum(2 * tokens * (b + a * c) for a, b, c in shapes)),
    )(*[l for (l, _), _ in pairs], *[rhs[0] for _, rhs in pairs])


def solution(mesh):
    tp_size = mesh.shape["tp"]
    sp_size = mesh.shape["sp"]
    in_rows = P(("dp", "sp"), None)
    swap = [(0, 1), (1, 0)]

    def exchange(t):
        return lax.ppermute(t, "tp", swap)

    def step(x, g, w_qkv, w_out, ln_gamma, ln_beta, temps):
        tokens, width = x.shape
        cols = w_qkv.shape[2]
        groups = cols // GROUP
        me = lax.axis_index("tp")
        w_near = jnp.transpose(w_qkv, (1, 0, 2))
        w_far = exchange(w_near)
        wo_far = exchange(w_out)
        half = tokens // 2
        off = jnp.stack([me, 1 - me]).astype(jnp.int32)
        halves = lambda t: t.reshape(2, half, t.shape[-1])

        u, near, stats, part = project(x, g, w_near, w_out, ln_gamma, ln_beta)
        x2, g2, u2, stats2 = halves(x), halves(g), halves(u), halves(stats)
        near = near.reshape(4, 2, half, cols)
        peers = [lax.ppermute(part, "sp", [(s, s ^ d) for s in range(sp_size)]) for d in (1, 2, 3)]
        part = (part + peers[0]) + (peers[1] + peers[2])
        part, wn_, wf_ = lax.optimization_barrier((part, w_near, w_far))
        part_far = exchange(part)
        held = (*hold(wn_, wf_), w_out, wo_far)
        vf = far_v(off, u2, w_far, EARLY_V, 0, 1)
        tau = jnp.repeat(temps, HEAD).reshape(tp_size, groups, GROUP)
        tau = jnp.where(me == 0, tau, tau[::-1]).reshape(2 * groups, GROUP)
        attn, dgram, coef, dtau = head_state(part, part_far, tau)
        state = (attn, dgram, coef)

        prev, dsum, recv, start = (), None, [], 0
        for sizes in OWN_CHUNKS:
            out = rows_call(off, start, sizes, (x2, g2, u2, stats2, near), state, (*held, ln_gamma), prev)
            prev, sent, ds = out[:3], out[3:-1], out[-1]
            recv += [exchange(t) for t in sent]
            dsum = ds if dsum is None else dsum + ds
            start += sum(sizes)
        y2, gx2, r = prev
        dtau, r = lax.optimization_barrier((dtau, r))
        dtau = jnp.sum(dtau[:2 * groups].reshape(tp_size, cols // HEAD, HEAD), axis=2)
        grad_temp = jnp.where(me == 0, dtau, dtau[::-1]).reshape(-1)

        flat = r.reshape(4, tokens, cols)
        dw_o, dw_v = token_sum(((flat, 3), (g[None], 0, 1)), ((u[None], 0), (flat, 2, 1)))
        flat, dw_o, dw_v = lax.optimization_barrier((flat, dw_o, dw_v))
        grad_wout = lax.psum_scatter(dw_o[0], "sp", scatter_dimension=0, tiled=True)
        dw_v = lax.psum_scatter(dw_v, "sp", scatter_dimension=1, tiled=True)
        (dw_qk,) = token_sum(((u[None], 0), (flat, 0, 2)))
        y2, dw_qk = lax.optimization_barrier((y2, dw_qk))
        dw_qk = lax.psum_scatter(dw_qk, "sp", scatter_dimension=1, tiled=True)
        y2, gx2, gw = far_y(off, x2, r, u2, vf, attn, w_out, wo_far, w_far, dw_v, recv[:-1], y2, gx2)
        grad_wqkv = jnp.transpose(lax.dynamic_update_slice(gw, dw_qk, (0, 0, 0)), (1, 0, 2))

        sums = jnp.sum(dsum, axis=1)
        for axis, perm in (("tp", swap), ("sp", [(s, s ^ 1) for s in range(sp_size)]), ("sp", [(s, s ^ 2) for s in range(sp_size)])):
            sums = sums + lax.ppermute(sums, axis, perm)
        gx2 = lax.dynamic_update_slice(gx2, recv[-1], (off[1], half - recv[-1].shape[1], 0))
        return y2.reshape(tokens, width), gx2.reshape(tokens, width), grad_wqkv, grad_wout, sums[0], sums[1], grad_temp

    in_specs = (in_rows, in_rows, P(None, None, "tp"), P("tp", None), P(None), P(None), P(None))
    out_specs = (in_rows, in_rows, P(("dp", "sp"), None, "tp"), P(("dp", "tp", "sp"), None), P("dp"), P("dp"), P("dp"))
    return jax.shard_map(step, mesh=mesh, in_specs=in_specs, out_specs=out_specs, check_vma=False)
```

```python
import functools

import jax
import jax.numpy as jnp
from jax import lax
from jax.experimental import pallas as pl
from jax.experimental.pallas import tpu as pltpu
from jax.sharding import PartitionSpec as P


LN_EPS = 1e-6
GROUP = 256
HEAD = 32
LANES = 128
F32 = jnp.float32
BF16 = jnp.bfloat16
NN = (((1,), (0,)), ((), ()))
NT = (((1,), (1,)), ((), ()))
TN = (((0,), (0,)), ((), ()))
PROJ_ROWS = 1024
ROWS = 256
STATE_LIMIT = 16_000_000
ROWS_LIMIT = 33_600_000
HOLD_LIMIT = 36_000_000
SUM_ROWS = 1024
OWN_CHUNKS = ((3,), (5,), (9,), (10, 5))
EARLY_V = 2


def dot(a, b, dims=NN):
    return lax.dot_general(a, b, dims, preferred_element_type=F32)


def normalize(x):
    mean = jnp.mean(x, axis=-1, keepdims=True)
    cen = x - mean
    inv = lax.rsqrt(jnp.mean(cen * cen, axis=-1, keepdims=True) + LN_EPS)
    return cen * inv, mean, inv


def row_spec(rows, cols, index):
    return pl.BlockSpec((rows, cols), lambda *a: (index(*a), 0))


def half_spec(rows, cols, which, start):
    return pl.BlockSpec((1, rows, cols), lambda j, off: (off[which], start + j, 0))


def both_spec(lead, rows, cols, start):
    zeros = (0,) * len(lead)
    return pl.BlockSpec((*lead, 2, rows, cols), lambda j, off: (*zeros, 0, start + j, 0))


def whole(shape):
    return pl.BlockSpec(shape, lambda *a: (0,) * len(shape), pipeline_mode=pl.Buffered(1))


def plane_spec(shape, e):
    return pl.BlockSpec((1, *shape[1:]), lambda *a: (e, 0, 0), pipeline_mode=pl.Buffered(1))


def sds(shape, dtype):
    return jax.ShapeDtypeStruct(shape, dtype)


def params(**kw):
    return pltpu.CompilerParams(vmem_limit_bytes=64_000_000, **kw)


def cost(flops, nbytes):
    return pl.CostEstimate(flops=int(flops), bytes_accessed=int(nbytes), transcendentals=0)


def project_body(x_ref, g_ref, wq_ref, wk_ref, wv_ref, wo_ref, gm_ref, bt_ref, u_ref, q_ref, k_ref, v_ref, do_ref, st_ref, part_ref, gr, da, qs, ks):
    i = pl.program_id(0)
    rows, cols = q_ref.shape
    groups = cols // GROUP
    do_ref[...] = dot(g_ref[...], wo_ref[...], NT).astype(BF16)
    xh, mean, inv = normalize(x_ref[...].astype(F32))
    u_ref[...] = (xh * gm_ref[...].reshape(1, -1) + bt_ref[...].reshape(1, -1)).astype(BF16)
    st_ref[...] = jnp.where(lax.broadcasted_iota(jnp.int32, st_ref.shape, 1) < LANES // 2, mean, inv)
    u = u_ref[...]
    for w_ref, out in ((wq_ref, q_ref), (wk_ref, k_ref), (wv_ref, v_ref)):
        out[...] = dot(u, w_ref[0]).astype(BF16)

    def add(acc, s, val):
        acc[s] = jnp.where(i == 0, val, acc[s] + val)

    for s in range(groups):
        c = slice(s * GROUP, (s + 1) * GROUP)
        add(gr, s, dot(q_ref[:, c], k_ref[:, c], TN))
        add(da, s, dot(do_ref[:, c], v_ref[:, c], TN))
    for acc, t in ((qs, q_ref), (ks, k_ref)):
        f = t[...].astype(F32)
        val = jnp.sum((f * f).reshape(rows // 8, 8, cols), axis=0)
        acc[...] = jnp.where(i == 0, val, acc[...] + val)

    @pl.when(i == pl.num_programs(0) - 1)
    def _():
        col_head = lax.broadcasted_iota(jnp.int32, (HEAD, GROUP), 1) // HEAD
        for a, acc in enumerate((gr, da)):
            for s in range(groups):
                tot = jnp.zeros((HEAD, GROUP), F32)
                for h in range(GROUP // HEAD):
                    tot += jnp.where(col_head == h, acc[s, h * HEAD:(h + 1) * HEAD, :], 0.0)
                part_ref[(a * groups + s) * HEAD:(a * groups + s + 1) * HEAD, :] = tot
        base = 2 * groups * HEAD
        part_ref[base:, :] = jnp.zeros((part_ref.shape[0] - base, GROUP), F32)
        for a, acc in enumerate((qs, ks)):
            tot = jnp.sum(acc[...], axis=0, keepdims=True)
            for s in range(groups):
                part_ref[base + a * groups + s:base + a * groups + s + 1, :] = tot[:, s * GROUP:(s + 1) * GROUP]


def project(x, g, w3, wo, gamma, beta):
    tokens, width = x.shape
    cols = wo.shape[0]
    groups = cols // GROUP
    part_rows = 2 * groups * HEAD + 8 * pl.cdiv(2 * groups, 8)
    row = lambda c: row_spec(PROJ_ROWS, c, lambda i: i)
    return pl.pallas_call(
        project_body,
        grid=(tokens // PROJ_ROWS,),
        in_specs=[row(width), row(width), *[plane_spec(w3.shape, e) for e in range(3)], whole(wo.shape), whole(gamma.shape), whole(beta.shape)],
        out_specs=[row(width)] + [row(cols)] * 4 + [row(LANES), pl.BlockSpec((part_rows, GROUP), lambda i: (0, 0))],
        out_shape=[sds((tokens, width), BF16)] + [sds((tokens, cols), BF16)] * 4 + [sds((tokens, LANES), F32), sds((part_rows, GROUP), F32)],
        scratch_shapes=[pltpu.VMEM((groups, GROUP, GROUP), F32)] * 2 + [pltpu.VMEM((8, cols), F32)] * 2,
        name="project",
        compiler_params=params(),
        cost_estimate=cost(2 * tokens * width * cols * 4.4, 2 * tokens * (3 * width + 4 * cols)),
    )(x, g, w3, w3, w3, wo, gamma, beta)


def far_v_body(off_ref, u_ref, w_ref, *refs):
    refs[-1][...] = dot(u_ref[0], w_ref[0]).astype(BF16)


def far_v(off, u2, w3, blocks, part, parts, prev=()):
    width, cols = w3.shape[1:]
    rows = 2 * ROWS
    steps = blocks * ROWS // rows // parts
    return pl.pallas_call(
        far_v_body,
        grid_spec=pltpu.PrefetchScalarGridSpec(
            num_scalar_prefetch=1,
            grid=(steps,),
            in_specs=[half_spec(rows, width, 1, part * steps),
                      pl.BlockSpec((1, width, cols), lambda j, off: (2, 0, 0), pipeline_mode=pl.Buffered(1))]
            + [pl.BlockSpec(memory_space=pl.ANY)] * len(prev),
            out_specs=pl.BlockSpec((rows, cols), lambda j, off: (part * steps + j, 0)),
        ),
        out_shape=sds((blocks * ROWS, cols), BF16),
        input_output_aliases={3: 0} if prev else {},
        name="far_v",
        compiler_params=params(),
        cost_estimate=cost(2 * steps * rows * width * cols, 2 * steps * rows * (width + cols)),
    )(off, u2, w3, *prev)


def state_body(near_ref, far_ref, tau_ref, attn_ref, dgram_ref, coef_ref, dtau_ref, *, groups):
    r_head = lax.broadcasted_iota(jnp.int32, (GROUP, GROUP), 0)
    c_head = lax.broadcasted_iota(jnp.int32, (GROUP, GROUP), 1)
    eye = r_head == c_head
    mask = (r_head // HEAD) == (c_head // HEAD)
    spread = lambda t: jnp.concatenate([t] * (GROUP // HEAD), axis=0)
    to_col = lambda t: jnp.sum(jnp.where(eye, t, 0.0), axis=1, keepdims=True)
    to_row = lambda t: jnp.sum(jnp.where(eye, t, 0.0), axis=0, keepdims=True)
    base = 2 * groups * HEAD
    coef_ref[...] = jnp.zeros_like(coef_ref)
    dtau_ref[...] = jnp.zeros_like(dtau_ref)
    for side, ref in enumerate((near_ref, far_ref)):
        for s in range(groups):
            gram_mat = spread(ref[s * HEAD:(s + 1) * HEAD, :])
            d_attn = spread(ref[(groups + s) * HEAD:(groups + s + 1) * HEAD, :])
            b_row = ref[base + groups + s:base + groups + s + 1, :]
            a_col = to_col(ref[base + s:base + s + 1, :])
            g = side * groups + s
            tau = to_col(tau_ref[g:g + 1, :])
            norm_prod = jnp.sqrt(a_col) * jnp.sqrt(b_row)
            gram_n = gram_mat / norm_prod
            logit = jnp.where(mask, tau * gram_n, -jnp.inf)
            e = jnp.exp(logit - jnp.max(logit, axis=1, keepdims=True))
            attn = e / jnp.sum(e, axis=1, keepdims=True)
            d_attn = jnp.where(mask, d_attn, 0.0)
            d_logit = jnp.where(mask, attn * (d_attn - jnp.sum(attn * d_attn, axis=1, keepdims=True)), 0.0)
            gram_n = jnp.where(mask, gram_n, 0.0)
            grad_sn = tau * d_logit
            prod = grad_sn * gram_n
            attn_ref[g] = attn.astype(BF16)
            dgram_ref[g] = jnp.where(mask, grad_sn / norm_prod, 0.0).astype(BF16)
            coef_ref[2 * side:2 * side + 1, s * GROUP:(s + 1) * GROUP] = to_row(-jnp.sum(prod, axis=1, keepdims=True) / a_col)
            coef_ref[2 * side + 1:2 * side + 2, s * GROUP:(s + 1) * GROUP] = -jnp.sum(prod, axis=0, keepdims=True) / b_row
            dtau_ref[g:g + 1, :] = to_row(jnp.sum(d_logit * gram_n, axis=1, keepdims=True))


def head_state(near, far, tau_rows):
    groups = tau_rows.shape[0] // 2
    vm = pl.BlockSpec(memory_space=pltpu.VMEM)
    return pl.pallas_call(
        functools.partial(state_body, groups=groups),
        in_specs=[vm] * 3,
        out_specs=[vm] * 4,
        out_shape=[sds((2 * groups, GROUP, GROUP), BF16)] * 2 + [sds((8, groups * GROUP), F32), sds((8, GROUP), F32)],
        name="head_state",
        compiler_params=pltpu.CompilerParams(vmem_limit_bytes=STATE_LIMIT),
        cost_estimate=cost(10**9, 2 * 10**6),
    )(near, far, tau_rows)


def hold_body(*refs, planes):
    n = len(planes)
    srcs = [ref if e is None else ref.at[e] for ref, e in zip(refs[:n], planes)]
    copies = [pltpu.make_async_copy(srcs[k], refs[n + k], refs[-1].at[k]) for k in range(n)]
    for c in copies:
        c.start()
    for c in copies:
        c.wait()


def hold(*arrays):
    parts = [(t, e) for t in arrays for e in (range(t.shape[0]) if t.ndim == 3 else (None,))]
    return pl.pallas_call(
        functools.partial(hold_body, planes=[e for _, e in parts]),
        in_specs=[pl.BlockSpec(memory_space=pltpu.HBM)] * len(parts),
        out_specs=[pl.BlockSpec(memory_space=pltpu.VMEM)] * len(parts),
        out_shape=[sds(t.shape[-2:], t.dtype) for t, _ in parts],
        scratch_shapes=[pltpu.SemaphoreType.DMA((len(parts),))],
        name="hold",
        compiler_params=pltpu.CompilerParams(vmem_limit_bytes=HOLD_LIMIT),
        cost_estimate=cost(10**9, 4 * 10**7),
    )(*[t for t, _ in parts])


def mix_block(q, k, v, do, attn_ref, dgram_ref, coef_ref, side, s):
    groups = attn_ref.shape[0] // 2
    am, gm = attn_ref[side * groups + s], dgram_ref[side * groups + s]
    c = slice(s * GROUP, (s + 1) * GROUP)
    dq = dot(k, gm, NT) + q.astype(F32) * coef_ref[2 * side:2 * side + 1, c]
    dk = dot(q, gm, NN) + k.astype(F32) * coef_ref[2 * side + 1:2 * side + 2, c]
    return dot(v, am, NT).astype(BF16), dq.astype(BF16), dk.astype(BF16), dot(do, am, NN).astype(BF16)


def rows_body(*refs, n_alias, send_blocks):
    it = iter(refs)
    nxt = lambda n: [next(it) for _ in range(n)]
    off_ref, x_ref, g_ref, u_ref, st_ref, q_ref, k_ref, v_ref, do_ref = nxt(9)
    attn_ref, dgram_ref, coef_ref, gm_ref = nxt(4)
    wn_ref, wf_ref = nxt(3), nxt(3)
    won_ref, wof_ref = nxt(2)
    nxt(n_alias)
    y_ref, gx_ref, o_ref, rqk_ref, rv_ref = nxt(5)
    send_refs = nxt(len(send_blocks))
    (dsum_ref,) = nxt(1)
    on_s, rn_s, of_s, rf_s, qf_s, kf_s, vf_s, dof_s, gh_s = nxt(9)
    j = pl.program_id(0)
    own, other = off_ref[0], off_ref[1]
    groups = attn_ref.shape[0] // 2
    state = (attn_ref, dgram_ref, coef_ref)

    def compute(first):
        for s in range(groups):
            c = slice(s * GROUP, (s + 1) * GROUP)
            for half in (own, other):
                o, dq, dk, dv = mix_block(q_ref[half, :, c], k_ref[half, :, c], v_ref[half, :, c], do_ref[half, :, c], *state, 0, s)
                o_ref[half, :, c], rqk_ref[0, half, :, c], rqk_ref[1, half, :, c], rv_ref[half, :, c] = o, dq, dk, dv
                if half is own:
                    on_s[:, c], rn_s[0, :, c], rn_s[1, :, c], rn_s[2, :, c] = o, dq, dk, dv
        u = u_ref[0]
        for e, t in enumerate((qf_s, kf_s, vf_s)):
            t[...] = dot(u, wf_ref[e][...]).astype(BF16)
        dof_s[...] = dot(g_ref[0], wof_ref[...], NT).astype(BF16)
        for s in range(groups):
            c = slice(s * GROUP, (s + 1) * GROUP)
            of_s[:, c], rf_s[0, :, c], rf_s[1, :, c], rf_s[2, :, c] = mix_block(
                qf_s[:, c], kf_s[:, c], vf_s[:, c], dof_s[:, c], *state, 1, s)
        rows, width = gh_s.shape
        mean, inv = st_ref[0, :, :1], st_ref[0, :, LANES // 2:LANES // 2 + 1]
        fold = lambda t: jnp.sum(t.reshape(rows // 8, 8, GROUP), axis=0)
        lanes = lambda t: sum(t[:, k:k + LANES] for k in range(0, GROUP, LANES))
        gamma = gm_ref[...].reshape(1, width)
        tiles = [slice(n, n + GROUP) for n in range(0, width, GROUP)]
        s1 = s2 = 0.0
        for c in tiles:
            du = dot(rn_s[0], wn_ref[0][c, :], NT)
            for e in range(1, 3):
                du += dot(rn_s[e], wn_ref[e][c, :], NT)
            for e in range(3):
                du += dot(rf_s[e], wf_ref[e][c, :], NT)
            xh = (x_ref[0, :, c].astype(F32) - mean) * inv
            for a, val in enumerate((fold(du * xh), fold(du))):
                dsum_ref[a, :, c] = jnp.where(first, val, dsum_ref[a, :, c] + val)
            gh = du * gamma[:, c]
            s1 += lanes(gh)
            s2 += lanes(gh * xh)
            gh_s[:, c] = gh
        m1 = jnp.sum(s1, axis=1, keepdims=True) / width
        m2 = jnp.sum(s2, axis=1, keepdims=True) / width
        for c in tiles:
            x = x_ref[0, :, c].astype(F32)
            yp = dot(on_s[...], won_ref[:, c]) + dot(of_s[...], wof_ref[:, c])
            y_ref[0, :, c] = (x + yp).astype(BF16)
            dx = g_ref[0, :, c].astype(F32) + inv * (gh_s[:, c] - m1 - (x - mean) * inv * m2)
            for ref in [gx_ref] + send_refs[:1] * (len(send_refs) == 1):
                ref[0, :, c] = dx.astype(BF16)

    compute(j == 0)

    if len(send_refs) > 1:
        start = 0
        for ref, n in zip(send_refs, send_blocks):

            @pl.when((j >= start) & (j < start + n))
            def _(ref=ref):
                ref[0] = gx_ref[0]

            start += n


def rows_call(off, start, send_blocks, acts, state, weights, prev):
    _, half, width = acts[0].shape
    blocks = sum(send_blocks)
    firsts = [sum(send_blocks[:n]) for n in range(len(send_blocks))]
    send_spec = lambda first, n: pl.BlockSpec((1, ROWS, width), lambda j, off: (0, jnp.clip(j - first, 0, n - 1), 0))
    cols = acts[4].shape[2]
    row = half_spec(ROWS, width, 0, start)
    both = lambda *lead: both_spec(lead, ROWS, cols, start)
    *loaded, gamma = weights
    consts = list(state) + [gamma]
    first = 1 + len(acts) + len(consts) + len(loaded)
    return pl.pallas_call(
        functools.partial(rows_body, n_alias=len(prev), send_blocks=send_blocks),
        grid_spec=pltpu.PrefetchScalarGridSpec(
            num_scalar_prefetch=1,
            grid=(blocks,),
            in_specs=[row] * 3 + [half_spec(ROWS, LANES, 0, start)] + [both()] * 4 + [whole(t.shape) for t in consts] + [pl.BlockSpec(memory_space=pltpu.VMEM)] * len(loaded) + [pl.BlockSpec(memory_space=pl.ANY)] * len(prev),
            out_specs=[row, row, both(), both(2), both(),
                       *[send_spec(first, n) for first, n in zip(firsts, send_blocks)],
                       pl.BlockSpec((2, 8, width), lambda j, off: (0, 0, 0))],
            scratch_shapes=[pltpu.VMEM((ROWS, cols), BF16), pltpu.VMEM((3, ROWS, cols), BF16)] * 2 + [pltpu.VMEM((ROWS, cols), BF16)] * 4
            + [pltpu.VMEM((ROWS, width), F32)],
        ),
        out_shape=[sds((2, half, width), BF16)] * 2 + [sds((2, half, cols), BF16), sds((2, 2, half, cols), BF16), sds((2, half, cols), BF16),
                                                       *[sds((1, n * ROWS, width), BF16) for n in send_blocks], sds((2, 8, width), F32)],
        input_output_aliases={first + a: a for a in range(len(prev))},
        name="rows",
        compiler_params=pltpu.CompilerParams(vmem_limit_bytes=ROWS_LIMIT),
        cost_estimate=cost(2 * blocks * ROWS * width * cols * 13, 2 * blocks * ROWS * (6 * width + 16 * cols)),
    )(off, *acts, *consts, *loaded, *prev)


def far_y_body(*refs, early, copies):
    it = iter(refs)
    nxt = lambda n: [next(it) for _ in range(n)]
    _, x_ref, o_ref, u_ref, v_ref, attn_ref, won_ref, wof_ref, wv_ref, pv_ref = nxt(10)
    recv = nxt(len(copies))
    _, _, y_ref, gx_ref, gw_ref, vf_s, of_s, sem = nxt(8)
    j = pl.program_id(0)
    per = gx_ref.shape[1] // ROWS

    def file_rows(act):
        for h in range(per):
            b = j * per + h
            start = 0
            for ref, n in zip(recv, copies):

                @pl.when((b >= start) & (b < start + n))
                def _(ref=ref, start=start, h=h, b=b):
                    src = ref.at[0, pl.ds((b - start) * ROWS, ROWS)]
                    act(pltpu.make_async_copy(src, gx_ref.at[0, pl.ds(h * ROWS, ROWS)], sem.at[h]))

                start += n

    file_rows(lambda copy: copy.start())
    gw_ref[...] = pv_ref[...]

    @pl.when(j < early)
    def _():
        vf_s[...] = v_ref[...]

    @pl.when(j >= early)
    def _():
        vf_s[...] = dot(u_ref[0], wv_ref[0]).astype(BF16)

    groups = attn_ref.shape[0] // 2
    for s in range(groups):
        c = slice(s * GROUP, (s + 1) * GROUP)
        of_s[:, c] = dot(vf_s[:, c], attn_ref[groups + s], NT).astype(BF16)
    y_ref[0] = (x_ref[0].astype(F32) + (dot(o_ref[0], won_ref[...]) + dot(of_s[...], wof_ref[...]))).astype(BF16)
    file_rows(lambda copy: copy.wait())


def far_y(off, x2, o2, u2, vf, attn, wo_near, wo_far, w_far, dw_v, recv, y2, gx2):
    half, width = x2.shape[1:]
    cols = o2.shape[2]
    rows = 2 * ROWS
    steps = half // rows
    early = vf.shape[0] // rows
    copies = [t.shape[1] // ROWS for t in recv]
    filed = pl.cdiv(sum(copies) * ROWS, rows)
    row = lambda c: half_spec(rows, c, 1, 0)
    part = (1, dw_v.shape[1] // steps, cols)
    any_ = pl.BlockSpec(memory_space=pl.ANY)
    specs = [row(width), row(cols),
             pl.BlockSpec((1, rows, width), lambda j, off: (off[1], jnp.maximum(j, early), 0)),
             pl.BlockSpec((rows, cols), lambda j, off: (jnp.minimum(j, early - 1), 0)),
             whole(attn.shape), whole(wo_near.shape), whole(wo_far.shape),
             pl.BlockSpec((1, width, cols), lambda j, off: (2, 0, 0), pipeline_mode=pl.Buffered(1)),
             pl.BlockSpec(part, lambda j, off: (0, j, 0))]
    args = [x2, o2, u2, vf, attn, wo_near, wo_far, w_far, dw_v, *recv]
    return pl.pallas_call(
        functools.partial(far_y_body, early=early, copies=copies),
        grid_spec=pltpu.PrefetchScalarGridSpec(
            num_scalar_prefetch=1,
            grid=(steps,),
            in_specs=specs + [any_] * (len(recv) + 2),
            out_specs=[row(width), pl.BlockSpec((1, rows, width), lambda j, off: (off[1], jnp.minimum(j, filed - 1), 0)), pl.BlockSpec(part, lambda j, off: (2, j, 0))],
            scratch_shapes=[pltpu.VMEM((rows, cols), BF16)] * 2 + [pltpu.SemaphoreType.DMA((rows // ROWS,))],
        ),
        out_shape=[sds(y2.shape, y2.dtype), sds(gx2.shape, gx2.dtype), sds((3, *dw_v.shape[1:]), F32)],
        input_output_aliases={len(args) + 1: 0, len(args) + 2: 1},
        name="far_y",
        compiler_params=params(),
        cost_estimate=cost(2 * half * width * cols * 2.8, 2 * half * (4 * width + 3 * cols)),
    )(off, *args, y2, gx2)


def token_sum_body(*refs, planes):
    n = len(planes)
    first = pl.program_id(0) == 0
    out = 2 * n
    for l_ref, r_ref, count in zip(refs[:n], refs[n:out], planes):
        o_ref, out = refs[out], out + 1
        for e in range(count):
            val = dot(l_ref[...], r_ref[e], TN)
            o_ref[e] = jnp.where(first, val, o_ref[e] + val)


def token_sum(*pairs):
    tokens = pairs[0][0].shape[0]
    flops = sum(2 * r.shape[0] * tokens * l.shape[1] * r.shape[2] for l, r in pairs)
    nbytes = sum(2 * tokens * (l.shape[1] + r.shape[0] * r.shape[2]) for l, r in pairs)
    shapes = [(r.shape[0], l.shape[1], r.shape[2]) for l, r in pairs]
    return pl.pallas_call(
        functools.partial(token_sum_body, planes=[r.shape[0] for _, r in pairs]),
        grid=(tokens // SUM_ROWS,),
        in_specs=[row_spec(SUM_ROWS, l.shape[1], lambda i: i) for l, _ in pairs]
        + [pl.BlockSpec((r.shape[0], SUM_ROWS, r.shape[2]), lambda i: (0, i, 0)) for _, r in pairs],
        out_specs=[pl.BlockSpec(s, lambda i: (0, 0, 0)) for s in shapes],
        out_shape=[sds(s, F32) for s in shapes],
        name="token_sum",
        compiler_params=params(),
        cost_estimate=cost(flops, nbytes),
    )(*[l for l, _ in pairs], *[r for _, r in pairs])


def solution(mesh):
    tp_size = mesh.shape["tp"]
    sp_size = mesh.shape["sp"]
    in_rows = P(("dp", "sp"), None)
    swap = [(0, 1), (1, 0)]

    def exchange(t):
        return lax.ppermute(t, "tp", swap)

    def step(x, g, w_qkv, w_out, ln_gamma, ln_beta, temps):
        tokens, width = x.shape
        cols = w_qkv.shape[2]
        groups = cols // GROUP
        me = lax.axis_index("tp")
        w_near = jnp.transpose(w_qkv, (1, 0, 2))
        w_far = exchange(w_near)
        wo_far = exchange(w_out)
        half = tokens // 2
        off = jnp.stack([me, 1 - me]).astype(jnp.int32)
        halves = lambda t: t.reshape(2, half, t.shape[-1])

        u, q, k, v, do, stats, part = project(x, g, w_near, w_out, ln_gamma, ln_beta)
        x2, g2, u2, stats2 = halves(x), halves(g), halves(u), halves(stats)
        near = tuple(halves(t) for t in (q, k, v, do))
        peers = [lax.ppermute(part, "sp", [(s, s ^ d) for s in range(sp_size)]) for d in (1, 2, 3)]
        part = (part + peers[0]) + (peers[1] + peers[2])
        part, wn_, wf_, wof_ = lax.optimization_barrier((part, w_near, w_far, wo_far))
        part_far = exchange(part)
        *held, wof_ = hold(wn_, wf_, wof_)
        held = (*held, w_out, wof_)
        vf = far_v(off, u2, w_far, EARLY_V, 0, 1)
        tau = jnp.repeat(temps, HEAD).reshape(tp_size, groups, GROUP)
        tau = jnp.where(me == 0, tau, tau[::-1]).reshape(2 * groups, GROUP)
        attn, dgram, coef, dtau = head_state(part, part_far, tau)
        state = (attn, dgram, coef)

        prev, dsum, recv, start = (), None, [], 0
        for sizes in OWN_CHUNKS:
            out = rows_call(off, start, sizes, (x2, g2, u2, stats2) + near, state, (*held, ln_gamma), prev)
            prev, sent, ds = out[:5], out[5:-1], out[-1]
            recv += [exchange(t) for t in sent]
            dsum = ds if dsum is None else dsum + ds
            start += sum(sizes)
        y2, gx2, o2, rqk, rv = prev
        dtau, rqk = lax.optimization_barrier((dtau, rqk))
        dtau = jnp.sum(dtau[:2 * groups].reshape(tp_size, cols // HEAD, HEAD), axis=2)
        grad_temp = jnp.where(me == 0, dtau, dtau[::-1]).reshape(-1)

        dw_o, dw_v = token_sum((o2.reshape(tokens, cols), g[None]), (u, rv.reshape(1, tokens, cols)))
        rqk, dw_o, dw_v = lax.optimization_barrier((rqk, dw_o, dw_v))
        grad_wout = lax.psum_scatter(dw_o[0], "sp", scatter_dimension=0, tiled=True)
        dw_v = lax.psum_scatter(dw_v, "sp", scatter_dimension=1, tiled=True)
        (dw_qk,) = token_sum((u, rqk.reshape(2, tokens, cols)))
        y2, dw_qk = lax.optimization_barrier((y2, dw_qk))
        dw_qk = lax.psum_scatter(dw_qk, "sp", scatter_dimension=1, tiled=True)
        y2, gx2, gw = far_y(off, x2, o2, u2, vf, attn, w_out, wo_far, w_far, dw_v, recv[:-1], y2, gx2)
        grad_wqkv = jnp.transpose(lax.dynamic_update_slice(gw, dw_qk, (0, 0, 0)), (1, 0, 2))

        sums = jnp.sum(dsum, axis=1)
        for axis, perm in (("tp", swap), ("sp", [(s, s ^ 1) for s in range(sp_size)]), ("sp", [(s, s ^ 2) for s in range(sp_size)])):
            sums = sums + lax.ppermute(sums, axis, perm)
        gx2 = lax.dynamic_update_slice(gx2, recv[-1], (off[1], half - recv[-1].shape[1], 0))
        return y2.reshape(tokens, width), gx2.reshape(tokens, width), grad_wqkv, grad_wout, sums[0], sums[1], grad_temp

    in_specs = (in_rows, in_rows, P(None, None, "tp"), P("tp", None), P(None), P(None), P(None))
    out_specs = (in_rows, in_rows, P(("dp", "sp"), None, "tp"), P(("dp", "tp", "sp"), None), P("dp"), P("dp"), P("dp"))
    return jax.shard_map(step, mesh=mesh, in_specs=in_specs, out_specs=out_specs, check_vma=False)
```
